8 devices in a mesh: data: 2 (over z, y), model: 4 (over x, core).
Axes of the slice: x: 2, y: 2, z: 1, core: 2. Of those that a mesh axis runs over, the one named last changes fastest.
Arguments:
- hidden_in: bfloat16 [2, 1024, 2048], P('data', 'model'), parts along dimension 0
- seg_ids: int32 [2, 1024], P('data'), parts along dimension 0
- gain_attn: bfloat16 [2048], replicated
- w_qkv: bfloat16 [2048, 32, 3, 64], P(None, 'model')
- w_out: bfloat16 [32, 64, 2048], P('model')
- gain_mlp: bfloat16 [2048], replicated
- w_up: bfloat16 [2048, 8192], P(None, 'model')
- w_down: bfloat16 [8192, 2048], P('model')
- grad_out: bfloat16 [2, 1024, 2048], P('data', 'model'), parts along dimension 0
Outputs:
- output 1: bfloat16 [2, 1024, 2048], P('data', 'model'), parts along dimension 0
- output 2: bfloat16 [2, 1024, 2048], P('data', 'model'), parts along dimension 0
- output 3: bfloat16 [4096, 32, 3, 64], P('data', 'model'), parts along dimension 0
- output 4: bfloat16 [64, 64, 2048], P(('data', 'model')), parts along dimension 0
- output 5: bfloat16 [4096, 8192], P('data', 'model'), parts along dimension 0
- output 6: bfloat16 [16384, 2048], P(('data', 'model')), parts along dimension 0
- output 7: bfloat16 [4096], P('data'), parts along dimension 0
- output 8: bfloat16 [4096], P('data'), parts along dimension 0
There are 2 independent parts. The reference program is written for one: setup_inputs(seed, part) draws one part's arguments, and reference() takes and returns one part's arrays. A program takes and returns all parts, laid end to end along the dimension named above; an argument that names none is the same for every part.
All inputs are finite; a program needn't handle non-finite values.
Results may differ from the reference program's by a relative error of at most 0.0189308.
Values are sent between devices in bfloat16 or wider.
A program may use at most 1 GiB of HBM per device.

```python
import jax
import jax.numpy as jnp
from jax import lax

BATCH = 1
SEQ_LEN = 1024
HIDDEN = 2048
HEADS = 32
HEAD_DIM = 64
FFN_DIM = 8192

LN_EPS = 1e-5
TOKENS = BATCH * SEQ_LEN
QKV_WIDTH = 3 * HEADS * HEAD_DIM
ATTN_WIDTH = HEADS * HEAD_DIM


def draw_segments(seg_key):
    cut_points = jax.random.randint(seg_key, (BATCH, 3), 1, SEQ_LEN)
    positions = jnp.arange(SEQ_LEN)
    return jnp.sum(positions[None, :, None] >= cut_points[:, None, :], axis=-1).astype(jnp.int32)


def normal_array(rand_key, shape, scale):
    return (scale * jax.random.normal(rand_key, shape, jnp.float32)).astype(jnp.bfloat16)


def setup_inputs(seed: int = 0, part: int = 0) -> dict:
    root_key = jax.random.key(seed)
    shared = jax.random.split(root_key, 6)
    part_keys = jax.random.split(jax.random.fold_in(root_key, part), 3)
    return {
        'hidden_in': normal_array(part_keys[0], (BATCH, SEQ_LEN, HIDDEN), 1.0),
        'seg_ids': draw_segments(part_keys[2]),
        'gain_attn': (1.0 + 0.3 * jax.random.normal(shared[0], (HIDDEN,), jnp.float32)).astype(jnp.bfloat16),
        'w_qkv': normal_array(shared[2], (HIDDEN, HEADS, 3, HEAD_DIM), 1.5 * HIDDEN ** -0.5),
        'w_out': normal_array(shared[3], (HEADS, HEAD_DIM, HIDDEN), 1.5 * ATTN_WIDTH ** -0.5),
        'gain_mlp': (1.0 + 0.3 * jax.random.normal(shared[1], (HIDDEN,), jnp.float32)).astype(jnp.bfloat16),
        'w_up': normal_array(shared[4], (HIDDEN, FFN_DIM), HIDDEN ** -0.5),
        'w_down': normal_array(shared[5], (FFN_DIM, HIDDEN), FFN_DIM ** -0.5),
        'grad_out': normal_array(part_keys[1], (BATCH, SEQ_LEN, HIDDEN), 1.0),
    }


def layer_norm(x_f32, gain_f32):
    mean_val = jnp.mean(x_f32, axis=-1, keepdims=True)
    centered = x_f32 - mean_val
    variance = jnp.mean(centered * centered, axis=-1, keepdims=True)
    return centered * lax.rsqrt(variance + LN_EPS) * gain_f32


def gelu_tanh(pre_act):
    return jax.nn.gelu(pre_act, approximate=True)


def head_probs(q_head, k_head, attn_mask):
    scores = jnp.einsum('bqd,bkd->bqk', q_head.astype(jnp.float32), k_head.astype(jnp.float32)) * HEAD_DIM ** -0.5
    return jax.nn.softmax(jnp.where(attn_mask, scores, -1e30), axis=-1)


def head_forward(head_qkv, attn_mask):
    attn_prob = head_probs(head_qkv[0], head_qkv[1], attn_mask)
    prob_lo = attn_prob.astype(jnp.bfloat16).astype(jnp.float32)
    return jnp.einsum('bqk,bkd->bqd', prob_lo, head_qkv[2].astype(jnp.float32)).astype(jnp.bfloat16)


def head_backward(head_qkv, head_out, d_head, attn_mask):
    q_head = head_qkv[0].astype(jnp.float32)
    k_head = head_qkv[1].astype(jnp.float32)
    v_head = head_qkv[2].astype(jnp.float32)
    attn_prob = head_probs(head_qkv[0], head_qkv[1], attn_mask)
    d_out = d_head.astype(jnp.float32)
    d_prob = jnp.einsum('bqd,bkd->bqk', d_out, v_head)
    row_delta = jnp.sum(d_out * head_out.astype(jnp.float32), axis=-1, keepdims=True)
    d_scores = (attn_prob * (d_prob - row_delta) * HEAD_DIM ** -0.5).astype(jnp.bfloat16).astype(jnp.float32)
    d_q = jnp.einsum('bqk,bkd->bqd', d_scores, k_head).astype(jnp.bfloat16)
    d_k = jnp.einsum('bqk,bqd->bkd', d_scores, q_head).astype(jnp.bfloat16)
    prob_lo = attn_prob.astype(jnp.bfloat16).astype(jnp.float32)
    d_v = jnp.einsum('bqk,bqd->bkd', prob_lo, d_out).astype(jnp.bfloat16)
    return jnp.stack([d_q, d_k, d_v])


def reference(hidden_in, seg_ids, gain_attn, w_qkv, w_out, gain_mlp, w_up, w_down, grad_out):
    x_rows = hidden_in.reshape(TOKENS, HIDDEN).astype(jnp.float32)
    ln1_out, ln1_vjp = jax.vjp(layer_norm, x_rows, gain_attn.astype(jnp.float32))
    attn_in = ln1_out.astype(jnp.bfloat16)
    w_qkv_flat = w_qkv.reshape(HIDDEN, QKV_WIDTH)
    qkv_flat = jnp.dot(attn_in, w_qkv_flat, preferred_element_type=jnp.float32).astype(jnp.bfloat16)
    qkv_heads = jnp.transpose(qkv_flat.reshape(BATCH, SEQ_LEN, HEADS, 3, HEAD_DIM), (2, 3, 0, 1, 4))
    positions = jnp.arange(SEQ_LEN)
    attn_mask = (positions[None, :, None] >= positions[None, None, :]) & (seg_ids[:, :, None] == seg_ids[:, None, :])
    attn_heads = lax.map(lambda head_qkv: head_forward(head_qkv, attn_mask), qkv_heads)
    attn_cat = jnp.transpose(attn_heads, (1, 2, 0, 3)).reshape(TOKENS, ATTN_WIDTH)
    w_out_flat = w_out.reshape(ATTN_WIDTH, HIDDEN)
    attn_sum = jnp.dot(attn_cat, w_out_flat, preferred_element_type=jnp.float32).astype(jnp.bfloat16)
    mid_rows = (x_rows + attn_sum.astype(jnp.float32)).astype(jnp.bfloat16)
    ln2_out, ln2_vjp = jax.vjp(layer_norm, mid_rows.astype(jnp.float32), gain_mlp.astype(jnp.float32))
    mlp_in = ln2_out.astype(jnp.bfloat16)
    pre_act = jnp.dot(mlp_in, w_up, preferred_element_type=jnp.float32)
    act_f32, gelu_vjp = jax.vjp(gelu_tanh, pre_act)
    act_lo = act_f32.astype(jnp.bfloat16)
    mlp_sum = jnp.dot(act_lo, w_down, preferred_element_type=jnp.float32).astype(jnp.bfloat16)
    out_rows = (mid_rows.astype(jnp.float32) + mlp_sum.astype(jnp.float32)).astype(jnp.bfloat16)
    dy_rows = grad_out.reshape(TOKENS, HIDDEN)
    d_act = jnp.dot(dy_rows, w_down.T, preferred_element_type=jnp.float32)
    d_pre = gelu_vjp(d_act)[0].astype(jnp.bfloat16)
    g_down = jnp.dot(act_lo.T, dy_rows, preferred_element_type=jnp.float32).astype(jnp.bfloat16)
    d_mlp_in = jnp.dot(d_pre, w_up.T, preferred_element_type=jnp.float32).astype(jnp.bfloat16)
    g_up = jnp.dot(mlp_in.T, d_pre, preferred_element_type=jnp.float32).astype(jnp.bfloat16)
    d_mid_ln, d_gain_mlp = ln2_vjp(d_mlp_in.astype(jnp.float32))
    d_mid = (dy_rows.astype(jnp.float32) + d_mid_ln).astype(jnp.bfloat16)
    d_attn_cat = jnp.dot(d_mid, w_out_flat.T, preferred_element_type=jnp.float32).astype(jnp.bfloat16)
    g_out = jnp.dot(attn_cat.T, d_mid, preferred_element_type=jnp.float32).astype(jnp.bfloat16)
    d_heads = jnp.transpose(d_attn_cat.reshape(BATCH, SEQ_LEN, HEADS, HEAD_DIM), (2, 0, 1, 3))
    d_qkv_heads = lax.map(lambda head_args: head_backward(head_args[0], head_args[1], head_args[2], attn_mask), (qkv_heads, attn_heads, d_heads))
    d_qkv = jnp.transpose(d_qkv_heads, (2, 3, 0, 1, 4)).reshape(TOKENS, QKV_WIDTH)
    d_attn_in = jnp.dot(d_qkv, w_qkv_flat.T, preferred_element_type=jnp.float32).astype(jnp.bfloat16)
    g_qkv = jnp.dot(attn_in.T, d_qkv, preferred_element_type=jnp.float32).astype(jnp.bfloat16)
    d_x_ln, d_gain_attn = ln1_vjp(d_attn_in.astype(jnp.float32))
    grad_in = (d_mid.astype(jnp.float32) + d_x_ln).astype(jnp.bfloat16)
    return (out_rows.reshape(BATCH, SEQ_LEN, HIDDEN), grad_in.reshape(BATCH, SEQ_LEN, HIDDEN), g_qkv.reshape(HIDDEN, HEADS, 3, HEAD_DIM), g_out.reshape(HEADS, HEAD_DIM, HIDDEN), g_up, g_down, d_gain_attn.astype(jnp.bfloat16), d_gain_mlp.astype(jnp.bfloat16))
```

```python
import functools
import jax, jax.numpy as jnp
from jax import lax
from jax.experimental import pallas as pl
from jax.experimental.pallas import tpu as pltpu
from jax.sharding import PartitionSpec as P
BF=jnp.bfloat16; F32=jnp.float32
BLK=256

def dotf(a,b,ca,cb):
    return lax.dot_general(a,b,(((ca,),(cb,)),((),())),preferred_element_type=F32)

def gather_abs(dst, own, oth, me):
    for r in range(4):
        src = own if r < 2 else oth
        off = pl.multiple_of(jnp.bitwise_xor(me, r)*BLK, BLK)
        dst[:, pl.ds(off, BLK)] = src[:, (r%2)*BLK:(r%2+1)*BLK]

def scatter_rel(own, oth, src, me):
    for r in range(4):
        dst = own if r < 2 else oth
        off = pl.multiple_of(jnp.bitwise_xor(me, r)*BLK, BLK)
        dst[:, (r%2)*BLK:(r%2+1)*BLK] = src[:, pl.ds(off, BLK)].astype(dst.dtype)

def vis_tile(segc, segr, b, a):
    vis = segc[b*BLK:(b+1)*BLK, :] == segr[:, a*BLK:(a+1)*BLK]
    if a == b:
        kp = lax.broadcasted_iota(jnp.int32, (BLK, BLK), 0)
        qp = lax.broadcasted_iota(jnp.int32, (BLK, BLK), 1)
        vis = vis & (kp <= qp)
    return vis

def fwd_kernel(dh, me_ref, own_ref, oth_ref, segr_ref, segc_ref, oo_ref, ot_ref, lse_ref, qkv, osc):
    me = me_ref[0]
    gather_abs(qkv, own_ref, oth_ref, me)
    k = (qkv[dh:2*dh, :].astype(F32)*dh**-0.5).T.astype(BF)
    for a in range(4):
        q = qkv[0:dh, a*BLK:(a+1)*BLK]
        s = [jnp.where(vis_tile(segc_ref, segr_ref, b, a), dotf(k[b*BLK:(b+1)*BLK], q, 1, 0), -1e30) for b in range(a+1)]
        m = functools.reduce(jnp.maximum, [jnp.max(t, axis=0, keepdims=True) for t in s])
        p = [jnp.exp(t - m) for t in s]
        l = functools.reduce(jnp.add, [jnp.sum(t, axis=0, keepdims=True) for t in p])
        inv = 1.0/l
        o = functools.reduce(jnp.add, [dotf(qkv[2*dh:3*dh, b*BLK:(b+1)*BLK], (p[b]*inv).astype(BF), 1, 0) for b in range(a+1)])
        osc[:, a*BLK:(a+1)*BLK] = o.astype(BF)
        lse_ref[0, :, a*BLK:(a+1)*BLK] = m + jnp.log(l)
    scatter_rel(oo_ref, ot_ref, osc, me)

def bwd_kernel(dh, me_ref, own_ref, oth_ref, oo_ref, ot_ref, do_ref, dt_ref, segr_ref, segc_ref, lse_ref, gown_ref, goth_ref, qkv, osc, dsc, gsc):
    me = me_ref[0]
    gather_abs(qkv, own_ref, oth_ref, me)
    gather_abs(osc, oo_ref, ot_ref, me)
    gather_abs(dsc, do_ref, dt_ref, me)
    sc = dh**-0.5
    k = (qkv[dh:2*dh, :].astype(F32)*sc).T.astype(BF)
    v = qkv[2*dh:3*dh, :].astype(F32).T.astype(BF)
    for a in range(4):
        ca = slice(a*BLK, (a+1)*BLK)
        q = qkv[0:dh, ca]
        do = dsc[:, ca]
        delta = jnp.sum(do.astype(F32)*osc[:, ca].astype(F32), axis=0, keepdims=True)
        lse = lse_ref[0, :, ca]
        dq = None
        for b in range(a+1):
            cb = slice(b*BLK, (b+1)*BLK)
            s = dotf(k[cb], q, 1, 0)
            p = jnp.exp(jnp.where(vis_tile(segc_ref, segr_ref, b, a), s - lse, -1e30))
            dp = dotf(v[cb], do, 1, 0)
            ds = (p*(dp-delta)*sc).astype(BF)
            t = dotf(qkv[dh:2*dh, cb], ds, 1, 0)
            dq = t if dq is None else dq + t
            dk = dotf(q, ds, 1, 1)
            dv = dotf(do, p.astype(BF), 1, 1)
            if a == b:
                gsc[dh:2*dh, cb] = dk
                gsc[2*dh:3*dh, cb] = dv
            else:
                gsc[dh:2*dh, cb] += dk
                gsc[2*dh:3*dh, cb] += dv
        gsc[0:dh, ca] = dq
    scatter_rel(gown_ref, goth_ref, gsc, me)

def attn_fwd(me, qo, qt, segr, segc, dh=64):
    nh = qo.shape[0]//(3*dh); half = qo.shape[1]; S = 2*half
    blk = lambda r: pl.BlockSpec((r, half), lambda h, *_: (h, 0))
    return pl.pallas_call(
        functools.partial(fwd_kernel, dh),
        grid_spec=pltpu.PrefetchScalarGridSpec(num_scalar_prefetch=1, grid=(nh,),
            in_specs=[blk(3*dh), blk(3*dh), pl.BlockSpec((1,S), lambda h,*_:(0,0)), pl.BlockSpec((S,1), lambda h,*_:(0,0))],
            out_specs=[blk(dh), blk(dh), pl.BlockSpec((1,1,S), lambda h,*_:(h,0,0))],
            scratch_shapes=[pltpu.VMEM((3*dh,S),BF), pltpu.VMEM((dh,S),BF)]),
        out_shape=[jax.ShapeDtypeStruct((nh*dh,half),BF)]*2+[jax.ShapeDtypeStruct((nh,1,S),F32)],
        name="attn_fwd",
        cost_estimate=pl.CostEstimate(flops=int(10e9), bytes_accessed=8<<20, transcendentals=nh*S*S//2),
        compiler_params=pltpu.CompilerParams(dimension_semantics=("arbitrary",)),
    )(me, qo, qt, segr, segc)

def attn_bwd(me, qo, qt, oo, ot, do, dt, segr, segc, lse, dh=64):
    nh = qo.shape[0]//(3*dh); half = qo.shape[1]; S = 2*half
    blk = lambda r: pl.BlockSpec((r, half), lambda h, *_: (h, 0))
    return pl.pallas_call(
        functools.partial(bwd_kernel, dh),
        grid_spec=pltpu.PrefetchScalarGridSpec(num_scalar_prefetch=1, grid=(nh,),
            in_specs=[blk(3*dh), blk(3*dh)]+[blk(dh)]*4+[pl.BlockSpec((1,S), lambda h,*_:(0,0)), pl.BlockSpec((S,1), lambda h,*_:(0,0)), pl.BlockSpec((1,1,S), lambda h,*_:(h,0,0))],
            out_specs=[blk(3*dh), blk(3*dh)],
            scratch_shapes=[pltpu.VMEM((3*dh,S),BF), pltpu.VMEM((dh,S),BF), pltpu.VMEM((dh,S),BF), pltpu.VMEM((3*dh,S),F32)]),
        out_shape=[jax.ShapeDtypeStruct((nh*3*dh,half),BF)]*2,
        name="attn_bwd",
        cost_estimate=pl.CostEstimate(flops=int(20e9), bytes_accessed=8<<20, transcendentals=nh*S*S//2),
        compiler_params=pltpu.CompilerParams(dimension_semantics=("arbitrary",)),
    )(me, qo, qt, oo, ot, do, dt, segr, segc, lse)

LN_EPS = 1e-5
PC = [(i, i ^ 1) for i in range(4)]
PX = [(i, i ^ 2) for i in range(4)]


def swap_core(v):
    return lax.ppermute(v, 'model', PC)


def swap_chip(v):
    return lax.ppermute(v, 'model', PX)


def layer_norm(x_f32, gain_f32):
    mean_val = jnp.mean(x_f32, axis=-1, keepdims=True)
    centered = x_f32 - mean_val
    variance = jnp.mean(centered * centered, axis=-1, keepdims=True)
    return centered * lax.rsqrt(variance + LN_EPS) * gain_f32


def gelu_tanh(pre_act):
    return jax.nn.gelu(pre_act, approximate=True)


def gather(v):
    near = jnp.concatenate([v, swap_core(v)], 0)
    far = swap_chip(v)
    return near, jnp.concatenate([far, swap_core(far)], 0)


def scatter(part_near, part_far):
    n = part_near.shape[0] // 2
    far = (part_far[:n].astype(F32) + swap_core(part_far[n:]).astype(F32)).astype(BF)
    got = swap_chip(far)
    near = part_near[:n].astype(F32) + swap_core(part_near[n:]).astype(F32)
    return near + got.astype(F32)


def local_layer(hidden_in, seg_ids, gain_attn, w_qkv, w_out, gain_mlp, w_up, w_down, grad_out):
    hidden, nh, _, dh = w_qkv.shape
    me = lax.axis_index('model').astype(jnp.int32).reshape(1)
    segr = seg_ids
    segc = seg_ids.reshape(-1, 1)
    wt = w_qkv.transpose(1, 2, 3, 0).reshape(nh * 3 * dh, hidden)
    wo = w_out.reshape(nh * dh, hidden)
    x = hidden_in[0].astype(F32)
    dy = grad_out[0]
    ln1, ln1_vjp = jax.vjp(layer_norm, x, gain_attn.astype(F32))
    a_near, a_far = gather(ln1.astype(BF))
    g_near, g_far = gather(dy)
    qkv_n = dotf(wt, a_near, 1, 1).astype(BF)
    qkv_f = dotf(wt, a_far, 1, 1).astype(BF)
    o_n, o_f, lse = attn_fwd(me, qkv_n, qkv_f, segr, segc, dh)
    att = scatter(dotf(o_n, wo, 0, 0).astype(BF), dotf(o_f, wo, 0, 0).astype(BF)).astype(BF)
    mid = (x + att.astype(F32)).astype(BF)
    ln2, ln2_vjp = jax.vjp(layer_norm, mid.astype(F32), gain_mlp.astype(F32))
    b_near, b_far = gather(ln2.astype(BF))

    def mlp(b, g):
        z = dotf(b, w_up, 1, 0)
        act, gelu_vjp = jax.vjp(gelu_tanh, z)
        dz = gelu_vjp(dotf(g, w_down, 1, 1))[0].astype(BF)
        return act.astype(BF), dz

    act_n, dz_n = mlp(b_near, g_near)
    act_f, dz_f = mlp(b_far, g_far)
    db = scatter(dotf(dz_n, w_up, 1, 1).astype(BF), dotf(dz_f, w_up, 1, 1).astype(BF)).astype(BF)
    y_sum = scatter(dotf(act_n, w_down, 1, 0).astype(BF), dotf(act_f, w_down, 1, 0).astype(BF)).astype(BF)
    y = (mid.astype(F32) + y_sum.astype(F32)).astype(BF)
    d_mid_ln, d_g2 = ln2_vjp(db.astype(F32))
    d_mid = (dy.astype(F32) + d_mid_ln).astype(BF)
    m_near, m_far = gather(d_mid)
    cat = lambda p, q: jnp.concatenate([p, q], 0)
    gw_down = dotf(cat(act_n, act_f), cat(g_near, g_far), 0, 0).astype(BF)
    gw_up = dotf(cat(b_near, b_far), cat(dz_n, dz_f), 0, 0).astype(BF)
    do_n = dotf(wo, m_near, 1, 1).astype(BF)
    do_f = dotf(wo, m_far, 1, 1).astype(BF)
    dq_n, dq_f = attn_bwd(me, qkv_n, qkv_f, o_n, o_f, do_n, do_f, segr, segc, lse, dh)
    da = scatter(dotf(dq_n, wt, 0, 0).astype(BF), dotf(dq_f, wt, 0, 0).astype(BF)).astype(BF)
    gw_out = dotf(jnp.concatenate([o_n, o_f], 1), cat(m_near, m_far), 1, 0).astype(BF)
    gw_qkv = dotf(jnp.concatenate([dq_n, dq_f], 1), cat(a_near, a_far), 1, 0).astype(BF)
    dx_ln, d_g1 = ln1_vjp(da.astype(F32))
    dx = (d_mid.astype(F32) + dx_ln).astype(BF)
    gains = jnp.stack([d_g1, d_g2])
    gains = gains + swap_core(gains)
    gains = (gains + swap_chip(gains)).astype(BF)
    gw_qkv = gw_qkv.reshape(nh, 3, dh, hidden).transpose(3, 0, 1, 2)
    return (y[None], dx[None], gw_qkv, gw_out.reshape(nh, dh, hidden), gw_up, gw_down, gains[0], gains[1])


def solution(mesh):
    act_spec = P('data', 'model', None)
    in_specs = (act_spec, P('data', None), P(), P(None, 'model', None, None), P('model', None, None), P(), P(None, 'model'), P('model', None), act_spec)
    out_specs = (act_spec, act_spec, P('data', 'model', None, None), P(('data', 'model'), None, None), P('data', 'model'), P(('data', 'model'), None), P('data'), P('data'))
    return jax.shard_map(local_layer, mesh=mesh, in_specs=in_specs, out_specs=out_specs, check_vma=False)
```

```python
import functools
import jax, jax.numpy as jnp
from jax import lax
from jax.experimental import pallas as pl
from jax.experimental.pallas import tpu as pltpu
from jax.sharding import PartitionSpec as P
BF=jnp.bfloat16; F32=jnp.float32
BLK=256

def dotf(a,b,ca,cb):
    return lax.dot_general(a,b,(((ca,),(cb,)),((),())),preferred_element_type=F32)

def gather_abs(dst, own, oth, me):
    for r in range(4):
        src = own if r < 2 else oth
        off = pl.multiple_of(jnp.bitwise_xor(me, r)*BLK, BLK)
        dst[:, pl.ds(off, BLK)] = src[:, (r%2)*BLK:(r%2+1)*BLK]

def scatter_rel(own, oth, src, me):
    for r in range(4):
        dst = own if r < 2 else oth
        off = pl.multiple_of(jnp.bitwise_xor(me, r)*BLK, BLK)
        dst[:, (r%2)*BLK:(r%2+1)*BLK] = src[:, pl.ds(off, BLK)].astype(dst.dtype)

def vis_tile(segc, segr, b, a):
    vis = segc[b*BLK:(b+1)*BLK, :] == segr[:, a*BLK:(a+1)*BLK]
    if a == b:
        kp = lax.broadcasted_iota(jnp.int32, (BLK, BLK), 0)
        qp = lax.broadcasted_iota(jnp.int32, (BLK, BLK), 1)
        vis = vis & (kp <= qp)
    return vis

def fwd_kernel(dh, me_ref, own_ref, oth_ref, segr_ref, segc_ref, oo_ref, ot_ref, lse_ref, qkv, osc):
    me = me_ref[0]
    gather_abs(qkv, own_ref, oth_ref, me)
    k = (qkv[dh:2*dh, :].astype(F32)*dh**-0.5).T.astype(BF)
    for a in range(4):
        q = qkv[0:dh, a*BLK:(a+1)*BLK]
        s = [jnp.where(vis_tile(segc_ref, segr_ref, b, a), dotf(k[b*BLK:(b+1)*BLK], q, 1, 0), -1e30) for b in range(a+1)]
        m = functools.reduce(jnp.maximum, [jnp.max(t, axis=0, keepdims=True) for t in s])
        p = [jnp.exp(t - m) for t in s]
        l = functools.reduce(jnp.add, [jnp.sum(t, axis=0, keepdims=True) for t in p])
        inv = 1.0/l
        o = functools.reduce(jnp.add, [dotf(qkv[2*dh:3*dh, b*BLK:(b+1)*BLK], (p[b]*inv).astype(BF), 1, 0) for b in range(a+1)])
        osc[:, a*BLK:(a+1)*BLK] = o.astype(BF)
        lse_ref[0, :, a*BLK:(a+1)*BLK] = m + jnp.log(l)
    scatter_rel(oo_ref, ot_ref, osc, me)

def bwd_kernel(dh, me_ref, own_ref, oth_ref, oo_ref, ot_ref, do_ref, dt_ref, segr_ref, segc_ref, lse_ref, gown_ref, goth_ref, qkv, osc, dsc, gsc):
    me = me_ref[0]
    gather_abs(qkv, own_ref, oth_ref, me)
    gather_abs(osc, oo_ref, ot_ref, me)
    gather_abs(dsc, do_ref, dt_ref, me)
    sc = dh**-0.5
    k = (qkv[dh:2*dh, :].astype(F32)*sc).T.astype(BF)
    v = qkv[2*dh:3*dh, :].astype(F32).T.astype(BF)
    for a in range(4):
        ca = slice(a*BLK, (a+1)*BLK)
        q = qkv[0:dh, ca]
        do = dsc[:, ca]
        delta = jnp.sum(do.astype(F32)*osc[:, ca].astype(F32), axis=0, keepdims=True)
        lse = lse_ref[0, :, ca]
        dq = None
        for b in range(a+1):
            cb = slice(b*BLK, (b+1)*BLK)
            s = dotf(k[cb], q, 1, 0)
            p = jnp.exp(jnp.where(vis_tile(segc_ref, segr_ref, b, a), s - lse, -1e30))
            dp = dotf(v[cb], do, 1, 0)
            ds = (p*(dp-delta)*sc).astype(BF)
            t = dotf(qkv[dh:2*dh, cb], ds, 1, 0)
            dq = t if dq is None else dq + t
            dk = dotf(q, ds, 1, 1)
            dv = dotf(do, p.astype(BF), 1, 1)
            if a == b:
                gsc[dh:2*dh, cb] = dk
                gsc[2*dh:3*dh, cb] = dv
            else:
                gsc[dh:2*dh, cb] += dk
                gsc[2*dh:3*dh, cb] += dv
        gsc[0:dh, ca] = dq
    scatter_rel(gown_ref, goth_ref, gsc, me)

def attn_fwd(me, qo, qt, segr, segc, dh=64):
    nh = qo.shape[0]//(3*dh); half = qo.shape[1]; S = 2*half
    blk = lambda r: pl.BlockSpec((r, half), lambda h, *_: (h, 0))
    return pl.pallas_call(
        functools.partial(fwd_kernel, dh),
        grid_spec=pltpu.PrefetchScalarGridSpec(num_scalar_prefetch=1, grid=(nh,),
            in_specs=[blk(3*dh), blk(3*dh), pl.BlockSpec((1,S), lambda h,*_:(0,0)), pl.BlockSpec((S,1), lambda h,*_:(0,0))],
            out_specs=[blk(dh), blk(dh), pl.BlockSpec((1,1,S), lambda h,*_:(h,0,0))],
            scratch_shapes=[pltpu.VMEM((3*dh,S),BF), pltpu.VMEM((dh,S),BF)]),
        out_shape=[jax.ShapeDtypeStruct((nh*dh,half),BF)]*2+[jax.ShapeDtypeStruct((nh,1,S),F32)],
        name="attn_fwd",
        cost_estimate=pl.CostEstimate(flops=int(10e9), bytes_accessed=8<<20, transcendentals=nh*S*S//2),
        compiler_params=pltpu.CompilerParams(dimension_semantics=("arbitrary",)),
    )(me, qo, qt, segr, segc)

def attn_bwd(me, qo, qt, oo, ot, do, dt, segr, segc, lse, dh=64):
    nh = qo.shape[0]//(3*dh); half = qo.shape[1]; S = 2*half
    blk = lambda r: pl.BlockSpec((r, half), lambda h, *_: (h, 0))
    return pl.pallas_call(
        functools.partial(bwd_kernel, dh),
        grid_spec=pltpu.PrefetchScalarGridSpec(num_scalar_prefetch=1, grid=(nh,),
            in_specs=[blk(3*dh), blk(3*dh)]+[blk(dh)]*4+[pl.BlockSpec((1,S), lambda h,*_:(0,0)), pl.BlockSpec((S,1), lambda h,*_:(0,0)), pl.BlockSpec((1,1,S), lambda h,*_:(h,0,0))],
            out_specs=[blk(3*dh), blk(3*dh)],
            scratch_shapes=[pltpu.VMEM((3*dh,S),BF), pltpu.VMEM((dh,S),BF), pltpu.VMEM((dh,S),BF), pltpu.VMEM((3*dh,S),F32)]),
        out_shape=[jax.ShapeDtypeStruct((nh*3*dh,half),BF)]*2,
        name="attn_bwd",
        cost_estimate=pl.CostEstimate(flops=int(20e9), bytes_accessed=8<<20, transcendentals=nh*S*S//2),
        compiler_params=pltpu.CompilerParams(dimension_semantics=("arbitrary",)),
    )(me, qo, qt, oo, ot, do, dt, segr, segc, lse)


LN_EPS = 1e-5
PC = [(i, i ^ 1) for i in range(4)]
PX = [(i, i ^ 2) for i in range(4)]


R = 128
MESH_ID = pl.DeviceIdType.MESH


def gelu_pair(z):
    c0, c1 = 0.7978845608028654, 0.044715
    z2 = z * z
    t = jnp.tanh(z * (c0 + (c0 * c1) * z2))
    h = 0.5 + 0.5 * t
    return z * h, h + (0.5 * z) * (1.0 - t * t) * (c0 + (3 * c0 * c1) * z2)


def partners():
    me = lax.axis_index('model')
    return me + 1 - 2 * lax.rem(me, 2), lax.rem(me + 2, 4)


def enter():
    core, chip = partners()
    sem = pltpu.get_barrier_semaphore()
    for dev in (core, chip):
        pl.semaphore_signal(sem, inc=1, device_id={'model': dev}, device_id_type=MESH_ID)
    pl.semaphore_wait(sem, 2)
    return core, chip


class Links:
    def __init__(self, send, recv):
        self.send, self.recv, self.n = send, recv, 0
        self.core, self.chip = partners()

    def copy(self, src, dst, dev):
        i = self.n
        self.n += 1
        return pltpu.make_async_remote_copy(src_ref=src, dst_ref=dst, send_sem=self.send.at[i], recv_sem=self.recv.at[i], device_id={'model': dev}, device_id_type=MESH_ID)

    def to_core(self, src, dst):
        return self.copy(src, dst, self.core)

    def to_chip(self, src, dst):
        return self.copy(src, dst, self.chip)


def tiles(n, size, body):
    def step(i, c):
        body(pl.ds(pl.multiple_of(i * size, size), size))
        return c
    lax.fori_loop(0, n // size, step, 0)


def norm_stats(v):
    mean = jnp.mean(v, axis=-1, keepdims=True)
    c = v - mean
    rstd = lax.rsqrt(jnp.mean(c * c, axis=-1, keepdims=True) + LN_EPS)
    return c * rstd, rstd


def mid_kernel(on_ref, of_ref, x_ref, gain_ref, wo_h, wu_h, wd_h, gy_h, mid_o, dg_o, b_h, act_h, dz_h, m_h, y_h,
               wo, wu, wd, gm, bv, dgv, act, dz, acc, csf, csn, crf, crn, xs, xr, ys, lsem, osem, ysem, send, recv):
    D = x_ref.shape[1]
    F = wu.shape[1]
    T = 512
    L = Links(send, recv)

    def row(r, s):
        return (r // 2) * 512 + s * 256 + (r % 2) * R

    def loc(src, dst, i):
        return pltpu.make_async_copy(src, dst, lsem.at[i])
    l_wo = loc(wo_h, wo, 0)
    l_wd = loc(wd_h, wd, 1)
    l_wu = loc(wu_h, wu, 2)
    l_g = [loc(gy_h[r].at[pl.ds(s * R, R)], gm.at[pl.ds(row(r, s), R)], 3 + 2 * r + s) for r in range(4) for s in range(2)]
    l_wo.start()
    l_wd.start()
    for c in l_g:
        c.start()
    l_wu.start()
    enter()

    def near(s):
        return pl.ds(row(0, s), R)

    def reduce_copies():
        far = [L.to_core(csf.at[pl.ds(s * R, R)], crf.at[pl.ds(s * R, R)]) for s in range(2)]
        nr = [L.to_core(csn.at[pl.ds(s * R, R)], crn.at[pl.ds(s * R, R)]) for s in range(2)]
        xc = [L.to_chip(xs.at[pl.ds(s * R, R)], xr.at[pl.ds(s * R, R)]) for s in range(2)]
        return far, nr, xc

    def gather_copies(buf):
        xc = [L.to_chip(buf.at[near(s)], buf.at[pl.ds(row(2, s), R)]) for s in range(2)]
        own = [L.to_core(buf.at[near(s)], buf.at[pl.ds(row(1, s), R)]) for s in range(2)]
        fwd = [L.to_core(buf.at[pl.ds(row(2, s), R)], buf.at[pl.ds(row(3, s), R)]) for s in range(2)]
        return xc, own, fwd

    b_far, b_near, b_x = reduce_copies()
    c_x, c_own, c_fwd = gather_copies(bv)
    f_far, f_near, f_x = reduce_copies()
    g_x, g_own, g_fwd = gather_copies(gm)

    def chip_sum(s, far, xc):
        far[s].wait_recv()
        rs = pl.ds(s * R, R)
        tiles(R, 32, lambda q: add_into(pl.ds(s * R + q.start, 32)))
        xc[s].start()

    def add_into(rs):
        xs[rs, :] = (xs[rs, :].astype(F32) + crf[rs, :].astype(F32)).astype(BF)

    l_wo.wait()

    def out_part(o_ref, lane, store):
        def body(q):
            store(q, dotf(o_ref[:, lane:lane + R], wo[:, q], 0, 0))
        tiles(D, T, body)

    def put(ref, lo):
        def store(q, v):
            ref[lo:lo + R, q] = v.astype(ref.dtype)
        return store

    for s in range(2):
        out_part(of_ref, 256 + s * R, put(csf, s * R))
        b_far[s].start()
    for s in range(2):
        out_part(of_ref, s * R, put(xs, s * R))
        chip_sum(s, b_far, b_x)
    for s in range(2):
        out_part(on_ref, 256 + s * R, put(csn, s * R))
        b_near[s].start()
    for s in range(2):
        out_part(on_ref, s * R, put(acc, s * R))

    l_wd.wait()
    for c in l_g:
        c.wait()

    def dact(o):
        def body(q):
            dgv[o:o + 256, q] = dotf(gm[o:o + 256, :], wd[q, :], 1, 1)
        tiles(F, T, body)
    for o in (512, 768, 0, 256):
        dact(o)
    l_wu.wait()

    def total(rs):
        return acc[rs, :] + crn[rs, :].astype(F32) + xr[rs, :].astype(F32)

    def norm2(s):
        b_near[s].wait_recv()
        b_x[s].wait_recv()

        def body(q):
            rs = pl.ds(s * R + q.start, 32)
            att = total(rs).astype(BF).astype(F32)
            mid = (x_ref[rs, :].astype(F32) + att).astype(BF)
            mid_o[rs, :] = mid
            h, _ = norm_stats(mid.astype(F32))
            bv[pl.ds(row(0, s) + q.start, 32), :] = (h * gain_ref[...]).astype(BF)
        tiles(R, 32, body)
        c_x[s].start()
        c_own[s].start()

    def mlp(o):
        def body(q):
            g, d = gelu_pair(dotf(bv[o:o + 256, :], wu[:, q], 1, 0))
            act[o:o + 256, q] = g.astype(BF)
            dz[o:o + 256, q] = (d * dgv[o:o + 256, q]).astype(BF)
        tiles(F, T, body)

    def dmlp(o, s, keep, give):
        def body(q):
            v = dotf(dz[o:o + 256, :], wu[q, :], 1, 1)
            keep[s * R:s * R + R, q] = v[:R].astype(keep.dtype)
            give[s * R:s * R + R, q] = v[R:].astype(BF)
        tiles(D, T, body)

    ycopies = []

    def ydown(o, k):
        if k >= 2:
            for c in ycopies[k - 2]:
                c.wait()
        slot = k % 2

        def body(q):
            ys[slot * 256:slot * 256 + 256, q] = dotf(act[o:o + 256, :], wd[:, q], 1, 0).astype(BF)
        tiles(D, T, body)
        r0, s = (o // 512) * 2, (o % 512) // 256
        cs = [pltpu.make_async_copy(ys.at[pl.ds(slot * 256 + j * R, R)], y_h.at[pl.ds((r0 + j) * 256 + s * R, R)], ysem.at[2 * k + j]) for j in range(2)]
        for c in cs:
            c.start()
        ycopies.append(cs)

    def out_rows(src, dst, r, s, i):
        c = pltpu.make_async_copy(src.at[pl.ds(row(r, s), R)], dst.at[pl.ds(r * 256 + s * R, R)], osem.at[i])
        c.start()
        return c

    outs = []

    def emit(src, dst, rr, s, base):
        for r in rr:
            outs.append(out_rows(src, dst, r, s, base + 2 * r + s))

    def near_step(s):
        c_own[s].wait_recv()
        mlp(s * 256)
        b_near[s].wait_send()
        dmlp(s * 256, s, acc, csn)
        f_near[s].start()
        emit(act, act_h, (0, 1), s, 8)
        emit(dz, dz_h, (0, 1), s, 16)

    norm2(0)
    near_step(0)
    norm2(1)
    near_step(1)

    def far_step(s):
        c_fwd[s].wait_recv()
        mlp(512 + s * 256)
        b_far[s].wait_send()
        b_x[s].wait_send()
        dmlp(512 + s * 256, s, xs, csf)
        f_far[s].start()
        emit(act, act_h, (2, 3), s, 8)
        emit(dz, dz_h, (2, 3), s, 16)

    c_x[0].wait_recv()
    c_fwd[0].start()
    far_step(0)
    chip_sum(0, f_far, f_x)
    c_x[1].wait_recv()
    c_fwd[1].start()
    far_step(1)
    chip_sum(1, f_far, f_x)
    for s in range(2):
        emit(bv, b_h, (0, 1, 2, 3), s, 0)
    ydown(512, 0)

    def dnorm2(s):
        f_near[s].wait_recv()
        f_x[s].wait_recv()

        def step(i, dgain):
            rs = pl.ds(pl.multiple_of(s * R + i * 32, 32), 32)
            db = total(rs).astype(BF).astype(F32)
            h, rstd = norm_stats(mid_o[rs, :].astype(F32))
            v = db * gain_ref[...]
            dm = rstd * (v - jnp.mean(v, -1, keepdims=True) - h * jnp.mean(v * h, -1, keepdims=True))
            gr = pl.ds(pl.multiple_of(row(0, s) + i * 32, 32), 32)
            gm[gr, :] = (gm[gr, :].astype(F32) + dm).astype(BF)
            return dgain + jnp.sum(db * h, axis=0, keepdims=True)
        dgain = lax.fori_loop(0, R // 32, step, jnp.zeros((1, D), F32))
        if s == 0:
            dg_o[...] = dgain
        else:
            dg_o[...] += dgain
        g_x[s].start()
        g_own[s].start()

    dnorm2(0)
    ydown(768, 1)
    dnorm2(1)
    ydown(0, 2)
    g_x[0].wait_recv()
    g_fwd[0].start()
    ydown(256, 3)
    for s in range(2):
        g_own[s].wait_recv()
        emit(gm, m_h, (0, 1), s, 24)
    g_x[1].wait_recv()
    g_fwd[1].start()
    for s in range(2):
        g_fwd[s].wait_recv()
        emit(gm, m_h, (2, 3), s, 24)
    for c in outs:
        c.wait()
    for cs in ycopies[2:]:
        for c in cs:
            c.wait()
    for c in f_far + f_near + f_x + c_x + c_own + c_fwd + g_x + g_own + g_fwd:
        c.wait_send()


def mid_call(o_n, o_f, x, gain, wo, wu, wd, gys):
    D = x.shape[1]
    F = wu.shape[1]
    S = 4 * x.shape[0]
    V = pl.BlockSpec(memory_space=pltpu.VMEM)
    H = pl.BlockSpec(memory_space=pl.ANY)
    sd = jax.ShapeDtypeStruct

    def kern(on_ref, of_ref, x_ref, gain_ref, wo_h, wu_h, wd_h, g0, g1, g2, g3, *rest):
        mid_kernel(on_ref, of_ref, x_ref, gain_ref, wo_h, wu_h, wd_h, (g0, g1, g2, g3), *rest)
    full = pltpu.VMEM((S, D), BF)
    quarter = pltpu.VMEM((256, D), BF)
    return pl.pallas_call(
        kern,
        in_specs=[V] * 4 + [H] * 7,
        out_specs=[V, V] + [H] * 5,
        out_shape=[sd((256, D), BF), sd((1, D), F32), sd((S, D), BF), sd((S, F), BF), sd((S, F), BF), sd((S, D), BF), sd((S, D), BF)],
        scratch_shapes=[pltpu.VMEM(wo.shape, BF), pltpu.VMEM(wu.shape, BF), pltpu.VMEM(wd.shape, BF), full, full,
                        pltpu.VMEM((S, F), F32), pltpu.VMEM((S, F), BF), pltpu.VMEM((S, F), BF), pltpu.VMEM((256, D), F32)]
        + [quarter] * 6 + [pltpu.VMEM((512, D), BF), pltpu.SemaphoreType.DMA((11,)), pltpu.SemaphoreType.DMA((32,)),
                           pltpu.SemaphoreType.DMA((8,)), pltpu.SemaphoreType.DMA((24,)), pltpu.SemaphoreType.DMA((24,))],
        name="mid",
        cost_estimate=pl.CostEstimate(flops=int(6e10), bytes_accessed=40 << 20, transcendentals=S * F),
        compiler_params=pltpu.CompilerParams(collective_id=0, has_side_effects=True, vmem_limit_bytes=66900000),
    )(o_n, o_f, x, gain, wo, wu, wd, *gys)


def swap_core(v):
    return lax.ppermute(v, 'model', PC)


def swap_chip(v):
    return lax.ppermute(v, 'model', PX)


def layer_norm(x_f32, gain_f32):
    mean_val = jnp.mean(x_f32, axis=-1, keepdims=True)
    centered = x_f32 - mean_val
    variance = jnp.mean(centered * centered, axis=-1, keepdims=True)
    return centered * lax.rsqrt(variance + LN_EPS) * gain_f32


def gather(v):
    near = jnp.concatenate([v, swap_core(v)], 0)
    far = swap_chip(v)
    return near, jnp.concatenate([far, swap_core(far)], 0)


def scatter(part_near, part_far):
    n = part_near.shape[0] // 2
    far = (part_far[:n].astype(F32) + swap_core(part_far[n:]).astype(F32)).astype(BF)
    got = swap_chip(far)
    near = part_near[:n].astype(F32) + swap_core(part_near[n:]).astype(F32)
    return near + got.astype(F32)


def local_layer(hidden_in, seg_ids, gain_attn, w_qkv, w_out, gain_mlp, w_up, w_down, grad_out):
    hidden, nh, _, dh = w_qkv.shape
    me = lax.axis_index('model').astype(jnp.int32).reshape(1)
    segr = seg_ids
    segc = seg_ids.reshape(-1, 1)
    wt = w_qkv.transpose(1, 2, 3, 0).reshape(nh * 3 * dh, hidden)
    wo = w_out.reshape(nh * dh, hidden)
    x = hidden_in[0].astype(F32)
    dy = grad_out[0]
    ln1, ln1_vjp = jax.vjp(layer_norm, x, gain_attn.astype(F32))
    a_near, a_far = gather(ln1.astype(BF))
    far = swap_chip(dy)
    gs = (dy, swap_core(dy), far, swap_core(far))
    qkv_n = dotf(wt, a_near, 1, 1).astype(BF)
    qkv_f = dotf(wt, a_far, 1, 1).astype(BF)
    o_n, o_f, lse = attn_fwd(me, qkv_n, qkv_f, segr, segc, dh)
    mid, d_g2, b_all, act, dz, m_all, y_part = mid_call(o_n, o_f, hidden_in[0], gain_mlp.astype(F32)[None], wo, w_up, w_down, gs)
    m_near, m_far = m_all[:512], m_all[512:]
    d_mid = m_all[:256]
    g_all = jnp.concatenate(gs, 0)
    gw_down = dotf(act, g_all, 0, 0).astype(BF)
    gw_up = dotf(b_all, dz, 0, 0).astype(BF)
    y_sum = scatter(y_part[:512], y_part[512:]).astype(BF)
    y = (mid.astype(F32) + y_sum.astype(F32)).astype(BF)
    cat = lambda p, q: jnp.concatenate([p, q], 0)
    do_n = dotf(wo, m_near, 1, 1).astype(BF)
    do_f = dotf(wo, m_far, 1, 1).astype(BF)
    dq_n, dq_f = attn_bwd(me, qkv_n, qkv_f, o_n, o_f, do_n, do_f, segr, segc, lse, dh)
    da = scatter(dotf(dq_n, wt, 0, 0).astype(BF), dotf(dq_f, wt, 0, 0).astype(BF)).astype(BF)
    gw_out = dotf(jnp.concatenate([o_n, o_f], 1), m_all, 1, 0).astype(BF)
    gw_qkv = dotf(jnp.concatenate([dq_n, dq_f], 1), cat(a_near, a_far), 1, 0).astype(BF)
    dx_ln, d_g1 = ln1_vjp(da.astype(F32))
    dx = (d_mid.astype(F32) + dx_ln).astype(BF)
    gains = jnp.stack([d_g1, d_g2[0]])
    gains = gains + swap_core(gains)
    gains = (gains + swap_chip(gains)).astype(BF)
    gw_qkv = gw_qkv.reshape(nh, 3, dh, hidden).transpose(3, 0, 1, 2)
    return (y[None], dx[None], gw_qkv, gw_out.reshape(nh, dh, hidden), gw_up, gw_down, gains[0], gains[1])


def solution(mesh):
    act_spec = P('data', 'model', None)
    in_specs = (act_spec, P('data', None), P(), P(None, 'model', None, None), P('model', None, None), P(), P(None, 'model'), P('model', None), act_spec)
    out_specs = (act_spec, act_spec, P('data', 'model', None, None), P(('data', 'model'), None, None), P('data', 'model'), P(('data', 'model'), None), P('data'), P('data'))
    return jax.shard_map(local_layer, mesh=mesh, in_specs=in_specs, out_specs=out_specs, check_vma=False)
```

```python
import functools
import jax, jax.numpy as jnp
from jax import lax
from jax.experimental import pallas as pl
from jax.experimental.pallas import tpu as pltpu
from jax.sharding import PartitionSpec as P
BF=jnp.bfloat16; F32=jnp.float32
BLK=256

HALVES = range(2)
COLS = dict(axis=0, keepdims=True)
ROWS = dict(axis=-1, keepdims=True)


def half(s):
    return pl.ds(s * R, R)


def nn(a, b):
    return dotf(a, b, 1, 0)


def nt(a, b):
    return dotf(a, b, 1, 1)


def tn(a, b):
    return dotf(a, b, 0, 0)


def dotf(a,b,ca,cb):
    return lax.dot_general(a,b,(((ca,),(cb,)),((),())),preferred_element_type=F32)

LN_EPS = 1e-5
BIG = 1e30


def split3(v):
    hi = v.astype(BF)
    r = v - hi.astype(F32)
    md = r.astype(BF)
    return [hi, md, (r - md.astype(F32)).astype(BF)]


def attn_setup(segr, qside, kside, tri):
    S = segr.shape[1]
    seg = segr[...]
    pad = jnp.zeros((9, S), F32)
    one = jnp.ones((3, S), F32)
    hot = jnp.concatenate([(seg == d).astype(F32) for d in range(4)], 0)
    kside[...] = jnp.concatenate([hot, one, pad], 0)
    qside[...] = jnp.concatenate([(hot - 1.0) * BIG, 0.0 * one, pad], 0)
    kp = lax.broadcasted_iota(jnp.int32, (BLK, BLK), 0)
    qp = lax.broadcasted_iota(jnp.int32, (BLK, BLK), 1)
    tri[...] = jnp.where(kp <= qp, 0.0, -BIG)


def head_rows(h, dh, c):
    return pl.ds(pl.multiple_of(h * (3 * dh) + c * dh, dh), dh)


def causal(s, tri):
    n = s.shape[0]
    if n == BLK:
        return s + tri[...]
    return jnp.concatenate([s[:n - BLK], s[n - BLK:] + tri[...]], 0)


def attn_head_fwd(h, dh, qkv, qside, kside, tri, out, lse_ref):
    kt = jnp.concatenate([qkv[head_rows(h, dh, 1), :].astype(F32) * dh ** -0.5, kside[...]], 0)
    ka = kt.T.astype(BF)
    qa = jnp.concatenate([qkv[head_rows(h, dh, 0), :], qside[...].astype(BF)], 0)
    vr = head_rows(h, dh, 2)
    sc = {}

    def scores(a):
        sc[a] = nn(ka[:(a + 1) * BLK], qa[:, a * BLK:(a + 1) * BLK])
    scores(3)
    for a in range(3, -1, -1):
        ca, K = slice(a * BLK, (a + 1) * BLK), (a + 1) * BLK
        if a > 0:
            scores(a - 1)
        s = causal(sc[a], tri)
        m = jnp.max(s, **COLS)
        p = jnp.exp(s - m)
        l = jnp.sum(p, **COLS)
        o = nn(qkv[vr, 0:K], (p * (1.0 / l)).astype(BF))
        out[pl.ds(pl.multiple_of(h * dh, dh), dh), ca] = o.astype(BF)
        lse_ref[h, :, ca] = m + jnp.log(l)


def attn_head_bwd(h, dh, qkv, oall, doall, lse_ref, qside, kside, tri, gsc, dqkv):
    sc = dh ** -0.5
    S = qkv.shape[1]
    hr = pl.ds(pl.multiple_of(h * dh, dh), dh)
    kr, qr = head_rows(h, dh, 1), head_rows(h, dh, 0)
    ka = jnp.concatenate([qkv[kr, :].astype(F32) * sc, kside[...]], 0).T.astype(BF)
    one, pad = jnp.ones((3, S), F32), jnp.zeros((13, S), F32)
    va = jnp.concatenate([qkv[head_rows(h, dh, 2), :].astype(F32), one, pad], 0).T.astype(BF)
    do32 = doall[hr, :].astype(F32)
    delta = jnp.sum(do32 * oall[hr, :].astype(F32), **COLS)
    side = qside[...].astype(BF)
    qa = jnp.concatenate([qkv[qr, :], side[0:4]] + split3(-lse_ref[h]) + [side[7:16]], 0)
    da = jnp.concatenate([(do32 * sc).astype(BF)] + split3(-sc * delta) + [pad.astype(BF)], 0)
    sdp = {}

    def scores(a):
        ca, K = slice(a * BLK, (a + 1) * BLK), (a + 1) * BLK
        sdp[a] = nn(ka[:K], qa[:, ca]), nn(va[:K], da[:, ca])
    scores(3)
    for a in range(3, -1, -1):
        ca, K = slice(a * BLK, (a + 1) * BLK), (a + 1) * BLK
        q, do = qkv[qr, ca], doall[hr, ca]
        if a > 0:
            scores(a - 1)
        p = jnp.exp(causal(sdp[a][0], tri))
        ds = (p * sdp[a][1]).astype(BF)
        dqkv[qr, ca] = nn(qkv[kr, 0:K], ds).astype(BF)
        dk = nt(ds, q)
        dv = nt(p.astype(BF), do)
        if a == 3:
            gsc[0] = dk
            gsc[1] = dv
        else:
            gsc[0, 0:K] += dk
            gsc[1, 0:K] += dv
    dqkv[kr, :] = gsc[0].T.astype(BF)
    dqkv[head_rows(h, dh, 2), :] = gsc[1].T.astype(BF)


R = 128
MESH_ID = pl.DeviceIdType.MESH


def gelu_pair(z):
    c0, c1 = 0.7978845608028654, 0.044715
    z2 = z * z
    t = jnp.tanh(z * (c0 + (c0 * c1) * z2))
    h = 0.5 + 0.5 * t
    return z * h, h + (0.5 * z) * (1.0 - t * t) * (c0 + (3 * c0 * c1) * z2)


PAIR = 2


def partners():
    me = lax.axis_index('model')
    return me + 1 - 2 * lax.rem(me, 2), lax.rem(me + 2, 4)


def enter():
    core, chip = partners()
    sem = pltpu.get_barrier_semaphore()
    for dev in (core, chip):
        pl.semaphore_signal(sem, inc=1, device_id={'model': dev}, device_id_type=MESH_ID)
    pl.semaphore_wait(sem, 2)
    return core, chip


def grad_blocks(lhs, rhs, out, st, sem, across, first, last, drain=True):
    def block(i):
        return pl.ds(pl.multiple_of(i * 256, 256), 256)

    def sent(i):
        return pltpu.make_async_copy(st.at[lax.rem(i, 2)], out.at[block(i)], sem.at[lax.rem(i, 2)])

    def step(i, c):
        @pl.when(i >= 2)
        def _():
            sent(i - 2).wait()

        def body(q):
            v = tn(lhs[:, block(i)], rhs[:, q]) if across else nn(lhs[block(i), :], rhs[:, q])
            st[lax.rem(i, 2), :, q] = v.astype(BF)
        for j in range(rhs.shape[1] // 512):
            body(pl.ds(j * 512, 512))
        sent(i).start()
        return c
    lax.fori_loop(first, last, step, 0)
    if drain:
        sent(last - 2).wait()
        sent(last - 1).wait()


class Links:
    def __init__(self, send, recv):
        self.send, self.recv, self.n = send, recv, 0
        self.core, self.chip = partners()

    def copy(self, src, dst, dev):
        i = self.n
        self.n += 1
        return pltpu.make_async_remote_copy(src_ref=src, dst_ref=dst, send_sem=self.send.at[i], recv_sem=self.recv.at[i], device_id={'model': dev}, device_id_type=MESH_ID)

    def to_core(self, src, dst):
        return self.copy(src, dst, self.core)

    def to_chip(self, src, dst):
        return self.copy(src, dst, self.chip)


def tiles(n, size, body, together=1):
    def step(i, c):
        for j in range(together):
            body(pl.ds(pl.multiple_of((i * together + j) * size, size), size))
        return c
    lax.fori_loop(0, n // (size * together), step, 0)


def row_of(g):
    return g[...].astype(F32).reshape(1, g.shape[0])


def norm_stats(v):
    mean = jnp.mean(v, **ROWS)
    c = v - mean
    rstd = lax.rsqrt(jnp.mean(c * c, **ROWS) + LN_EPS)
    return c * rstd, rstd


def positions():
    me = lax.axis_index('model')
    core, chip = partners()
    return me, core, chip, 3 - me


def front_kernel(dh, x_ref, g1_ref, g2_ref, segr, wt_h, wo_h, wu_h, wd_h, gy_h, mid_o, dg_o, qkv, att, lse, ysum_o, ynear_o, a_h, g_h, act_h, m_h, gu_h,
                 wo, wu, wd, gm, bv, dgv, act, dz, acc, csf, csn, crf, crn, xs, xr, st, qside, kside, tri, lsem, osem, ssem, send, recv):
    D = x_ref.shape[1]
    F = wu.shape[1]
    T = 512
    QW = qkv.shape[0]
    L = Links(send, recv)
    at = positions()

    def row(r, s):
        return (r // 2) * 512 + s * 256 + (r % 2) * R

    def lanes(r, s):
        return pl.ds(pl.multiple_of(at[r] * 256 + s * R, R), R)

    def loc(src, dst, i):
        return pltpu.make_async_copy(src, dst, lsem.at[i])
    l_g = [loc(gy_h.at[half(s)], gm.at[pl.ds(row(0, s), R)], s) for s in HALVES]
    l_wt = loc(wt_h, wu.at[pl.ds(0, QW)], 2)
    l_wo = loc(wo_h, wo, 3)
    l_wd = loc(wd_h, wd, 4)
    l_wu = loc(wu_h, wu, 5)
    for c in l_g + [l_wt, l_wo, l_wd]:
        c.start()
    enter()

    def near(s):
        return pl.ds(row(0, s), R)

    def reduce_copies(cross=True):
        far = [L.to_core(csf.at[half(s)], crf.at[half(s)]) for s in HALVES]
        nr = [L.to_core(csn.at[half(s)], crn.at[half(s)]) for s in HALVES]
        return far, nr, [L.to_chip(xs.at[half(s)], xr.at[half(s)]) for s in HALVES] if cross else None

    def gather_copies(buf):
        xc = [L.to_chip(buf.at[near(s)], buf.at[pl.ds(row(2, s), R)]) for s in HALVES]
        own = [L.to_core(buf.at[near(s)], buf.at[pl.ds(row(1, s), R)]) for s in HALVES]
        fwd = [L.to_core(buf.at[pl.ds(row(2, s), R)], buf.at[pl.ds(row(3, s), R)]) for s in HALVES]
        return xc, own, fwd

    a_x, a_own, a_fwd = gather_copies(bv)
    e_x, e_own, e_fwd = gather_copies(gm)
    b_far, b_near, b_x = reduce_copies()
    c_x, c_own, c_fwd = gather_copies(bv)
    f_far, f_near, f_x = reduce_copies()
    g_x, g_own, g_fwd = gather_copies(gm)

    def chip_sum(s, far, xc):
        far[s].wait_recv()
        rs = half(s)
        tiles(R, 32, lambda q: add_into(pl.ds(s * R + q.start, 32)))
        xc[s].start()

    def add_into(rs):
        xs[rs, :] = (xs[rs, :].astype(F32) + crf[rs, :].astype(F32)).astype(BF)

    outs = []

    def emit(src, dst, rr, s, base):
        for r in rr:
            c = pltpu.make_async_copy(src.at[pl.ds(row(r, s), R)], dst.at[pl.ds(r * 256 + s * R, R)], osem.at[base + 2 * r + s])
            c.start()
            outs.append(c)

    for s in HALVES:
        def norm1(q):
            h, _ = norm_stats(x_ref[pl.ds(s * R + q.start, 32), :].astype(F32))
            bv[pl.ds(row(0, s) + q.start, 32), :] = (h * row_of(g1_ref)).astype(BF)
        tiles(R, 32, norm1)
        a_x[s].start()
        a_own[s].start()
    for s in HALVES:
        l_g[s].wait()
        e_x[s].start()
        e_own[s].start()
    attn_setup(segr, qside, kside, tri)
    l_wt.wait()

    def qkv_rows(o, r, s):
        def body(q):
            v = nt(wu[q, :], bv[o:o + 256, :]).astype(BF)
            qkv[q, lanes(r, s)] = v[:, :R]
            qkv[q, lanes(r + 1, s)] = v[:, R:]
        tiles(QW, T, body)
    for s in HALVES:
        a_own[s].wait_recv()
        qkv_rows(s * 256, 0, s)
    for s in HALVES:
        a_x[s].wait_recv()
        a_fwd[s].start()
        a_fwd[s].wait_recv()
        qkv_rows(512 + s * 256, 2, s)
    l_wu.start()
    a_out = [pltpu.make_async_copy(bv.at[pl.ds(row(r, s), R)], a_h.at[lanes(r, s)], osem.at[40 + 2 * r + s]) for r in range(4) for s in HALVES]
    for c in a_out:
        c.start()
    lax.fori_loop(0, lse.shape[0], lambda h, c: (attn_head_fwd(h, dh, qkv, qside, kside, tri, att, lse), c)[1], 0)
    e_x[0].wait_recv()
    e_fwd[0].start()
    for c in a_out:
        c.wait()
    for c in a_x + a_own + a_fwd:
        c.wait_send()

    l_wo.wait()

    def out_part(r, s, store):
        def body(q):
            store(q, tn(att[:, lanes(r, s)], wo[:, q]))
        tiles(D, T, body, PAIR)

    def put(ref, lo):
        def store(q, v):
            ref[lo:lo + R, q] = v.astype(ref.dtype)
        return store

    for s in HALVES:
        out_part(3, s, put(csf, s * R))
        b_far[s].start()
    for s in HALVES:
        out_part(2, s, put(xs, s * R))
        chip_sum(s, b_far, b_x)
    for s in HALVES:
        out_part(1, s, put(csn, s * R))
        b_near[s].start()
    e_x[1].wait_recv()
    e_fwd[1].start()
    for s in HALVES:
        out_part(0, s, put(acc, s * R))

    l_wd.wait()

    def dact(o):
        def body(q):
            dgv[o:o + 256, q] = nt(gm[512 + o:768 + o, :], wd[q, :])
        tiles(F, T, body, PAIR)
    for s in HALVES:
        e_own[s].wait_recv()
        e_fwd[s].wait_recv()
        emit(gm, g_h, (0, 1, 2, 3), s, 32)
        dact(s * 256)
    g_out = list(outs)
    outs.clear()
    l_wu.wait()
    for c in e_x + e_own + e_fwd:
        c.wait_send()

    def total(rs):
        return acc[rs, :] + crn[rs, :].astype(F32) + xr[rs, :].astype(F32)

    def norm2(s):
        b_near[s].wait_recv()
        b_x[s].wait_recv()

        def body(q):
            rs = pl.ds(s * R + q.start, 32)
            att = total(rs).astype(BF).astype(F32)
            mid = (x_ref[rs, :].astype(F32) + att).astype(BF)
            mid_o[rs, :] = mid
            h, _ = norm_stats(mid.astype(F32))
            bv[pl.ds(row(0, s) + q.start, 32), :] = (h * row_of(g2_ref)).astype(BF)
        tiles(R, 32, body)
        c_x[s].start()
        c_own[s].start()

    def mlp(o):
        def body(q):
            g, d = gelu_pair(nn(bv[o:o + 256, :], wu[:, q]))
            act[o:o + 256, q] = g.astype(BF)
            up = dgv[o - 512:o - 256, q] if o >= 512 else nt(gm[o:o + 256, :], wd[q, :])
            dz[o:o + 256, q] = (d * up).astype(BF)
        tiles(F, T, body, PAIR)

    def dmlp(o, s, keep, give):
        def body(q):
            v = nt(dz[o:o + 256, :], wu[q, :])
            keep[half(s), q] = v[:R].astype(keep.dtype)
            give[half(s), q] = v[R:].astype(BF)
        tiles(D, T, body, PAIR)

    def ydown(o, s, keep, give):
        def body(q):
            v = nn(act[o:o + 256, :], wd[:, q])
            keep[half(s), q] = v[:R].astype(keep.dtype)
            give[half(s), q] = v[R:].astype(BF)
        tiles(D, T, body, PAIR)

    def near_step(s):
        c_own[s].wait_recv()
        mlp(s * 256)
        b_near[s].wait_send()
        dmlp(s * 256, s, acc, csn)
        f_near[s].start()
        emit(act, act_h, (0, 1), s, 8)

    norm2(0)
    for c in g_out:
        c.wait()
    near_step(0)
    norm2(1)
    near_step(1)

    def far_step(s):
        c_fwd[s].wait_recv()
        mlp(512 + s * 256)
        b_far[s].wait_send()
        b_x[s].wait_send()
        dmlp(512 + s * 256, s, xs, csf)
        f_far[s].start()
        emit(act, act_h, (2, 3), s, 8)

    c_x[0].wait_recv()
    c_fwd[0].start()
    far_step(0)
    chip_sum(0, f_far, f_x)
    c_x[1].wait_recv()
    c_fwd[1].start()
    far_step(1)
    chip_sum(1, f_far, f_x)
    def dnorm2(s):
        f_near[s].wait_recv()
        f_x[s].wait_recv()

        def step(i, dgain):
            rs = pl.ds(pl.multiple_of(s * R + i * 32, 32), 32)
            db = total(rs).astype(BF).astype(F32)
            h, rstd = norm_stats(mid_o[rs, :].astype(F32))
            v = db * row_of(g2_ref)
            dm = rstd * (v - jnp.mean(v, **ROWS) - h * jnp.mean(v * h, **ROWS))
            gr = pl.ds(pl.multiple_of(row(0, s) + i * 32, 32), 32)
            gm[gr, :] = (gm[gr, :].astype(F32) + dm).astype(BF)
            return dgain + jnp.sum(db * h, **COLS)
        dgain = lax.fori_loop(0, R // 32, step, jnp.zeros((1, D), F32))
        if s == 0:
            dg_o[...] = dgain
        else:
            dg_o[...] += dgain
        g_x[s].start()
        g_own[s].start()

    grad_blocks(bv, dz, gu_h, st, ssem, True, 0, 3, False)
    dnorm2(0)
    grad_blocks(bv, dz, gu_h, st, ssem, True, 3, F // 256)
    dnorm2(1)
    y_far, y_near = reduce_copies(False)[:2]
    for s in HALVES:
        g_own[s].wait_recv()
        emit(gm, m_h, (0, 1), s, 24)
        f_far[s].wait_send()
        f_x[s].wait_send()
        ydown(512 + s * 256, s, xs, csf)
        y_far[s].start()
    g_x[0].wait_recv()
    g_fwd[0].start()
    for s in HALVES:
        f_near[s].wait_send()
        ydown(s * 256, s, acc, csn)
        y_near[s].start()
    for s in HALVES:
        y_far[s].wait_recv()
        y_near[s].wait_recv()

    def ysum(q):
        ysum_o[q, :] = (xs[q, :].astype(F32) + crf[q, :].astype(F32)).astype(BF)
        ynear_o[q, :] = (acc[q, :] + crn[q, :].astype(F32)).astype(BF)
    tiles(256, 32, ysum)
    g_x[1].wait_recv()
    g_fwd[1].start()
    for s in HALVES:
        g_fwd[s].wait_recv()
        emit(gm, m_h, (2, 3), s, 24)
    for c in outs:
        c.wait()
    for c in y_far + y_near + c_x + c_own + c_fwd + g_x + g_own + g_fwd:
        c.wait_send()


def front_call(x, g1, g2, segr, wt, wo, wu, wd, gy, nh):
    D = x.shape[1]
    F = wu.shape[1]
    S = 4 * x.shape[0]
    dh = wo.shape[0] // nh
    V = pl.BlockSpec(memory_space=pltpu.VMEM)
    H = pl.BlockSpec(memory_space=pl.ANY)
    sd = jax.ShapeDtypeStruct
    full = pltpu.VMEM((S, D), BF)
    quarter = pltpu.VMEM((256, D), BF)
    return pl.pallas_call(
        functools.partial(front_kernel, dh),
        in_specs=[V] * 4 + [H] * 5,
        out_specs=[V] * 7 + [H] * 5,
        out_shape=[sd((256, D), BF), sd((1, D), F32), sd(wt.shape[:1] + (S,), BF), sd((nh * dh, S), BF), sd((nh, 1, S), F32), sd((256, D), BF), sd((256, D), BF),
                   sd((S, D), BF), sd((S, D), BF), sd((S, F), BF), sd((S, D), BF), sd(wu.shape, BF)],
        scratch_shapes=[pltpu.VMEM(wo.shape, BF), pltpu.VMEM(wu.shape, BF), pltpu.VMEM(wd.shape, BF), full, full,
                        pltpu.VMEM((S // 2, F), F32), pltpu.VMEM((S, F), BF), pltpu.VMEM((S, F), BF), pltpu.VMEM((256, D), F32)]
        + [quarter] * 6 + [pltpu.VMEM((2, 256, F), BF), pltpu.VMEM((16, S), F32), pltpu.VMEM((16, S), F32), pltpu.VMEM((BLK, BLK), F32),
                           pltpu.SemaphoreType.DMA((6,)), pltpu.SemaphoreType.DMA((48,)),
                           pltpu.SemaphoreType.DMA((8,)), pltpu.SemaphoreType.DMA((42,)), pltpu.SemaphoreType.DMA((42,))],
        name="front",
        cost_estimate=pl.CostEstimate(flops=int(8e10), bytes_accessed=60 << 20, transcendentals=S * F),
        compiler_params=pltpu.CompilerParams(collective_id=0, has_side_effects=True, vmem_limit_bytes=66900000),
    )(x, g1, g2, segr, wt, wo, wu, wd, gy)


def back_kernel(dh, segr, qkv, att, lse, ysum, wt_h, wo_h, m_h, yr_o, hx_o, hn_o, dqkv,
                wt, wo, mv, doall, gsc, csf, csn, crf, crn, qside, kside, tri, lsem, send, recv):
    D = wt.shape[1]
    T = 512
    nh = lse.shape[0]
    L = Links(send, recv)
    at = positions()

    def lanes(r, s):
        return pl.ds(pl.multiple_of(at[r] * 256 + s * R, R), R)

    def loc(src, dst, i):
        c = pltpu.make_async_copy(src, dst, lsem.at[i])
        c.start()
        return c
    l_wo = loc(wo_h, wo, 0)
    l_m = [loc(m_h.at[pl.ds(r * 256, 256)], mv.at[pl.ds(pl.multiple_of(at[r] * 256, 256), 256)], 1 + r) for r in range(4)]
    l_wt = loc(wt_h, wt, 5)
    enter()
    y_x = L.to_chip(ysum, yr_o)
    y_x.start()
    h_far = [L.to_core(csf.at[half(s)], crf.at[half(s)]) for s in HALVES]
    h_near = [L.to_core(csn.at[half(s)], crn.at[half(s)]) for s in HALVES]
    attn_setup(segr, qside, kside, tri)
    l_wo.wait()
    for c in l_m:
        c.wait()

    def dout(q):
        doall[:, q] = nt(wo[...], mv[q, :]).astype(BF)
    tiles(4 * 256, 256, dout)
    lax.fori_loop(0, nh, lambda h, c: (attn_head_bwd(h, dh, qkv, att, doall, lse, qside, kside, tri, gsc, dqkv), c)[1], 0)
    l_wt.wait()

    def part(r, s, ref):
        def body(q):
            ref[half(s), q] = tn(dqkv[:, lanes(r, s)], wt[:, q]).astype(ref.dtype)
        tiles(D, T, body, PAIR)

    def add_into(ref, got, s):
        def body(q):
            rs = pl.ds(s * R + q.start, 32)
            ref[rs, :] = (ref[rs, :].astype(F32) + got[rs, :].astype(F32)).astype(ref.dtype)
        tiles(R, 32, body)

    for s in HALVES:
        part(3, s, csf)
        h_far[s].start()
    for s in HALVES:
        part(1, s, csn)
        h_near[s].start()
    for s in HALVES:
        part(2, s, hx_o)
        h_far[s].wait_recv()
        add_into(hx_o, crf, s)
    for s in HALVES:
        part(0, s, hn_o)
        h_near[s].wait_recv()
        add_into(hn_o, crn, s)
    y_x.wait_recv()
    for c in [y_x] + h_far + h_near:
        c.wait_send()


def back_call(segr, qkv, att, lse, ysum, wt, wo, m_all):
    S, D = m_all.shape
    nh = lse.shape[0]
    dh = wo.shape[0] // nh
    V = pl.BlockSpec(memory_space=pltpu.VMEM)
    H = pl.BlockSpec(memory_space=pl.ANY)
    sd = jax.ShapeDtypeStruct
    quarter = pltpu.VMEM((256, D), BF)
    return pl.pallas_call(
        functools.partial(back_kernel, dh),
        in_specs=[V] * 5 + [H] * 3,
        out_specs=[V] * 4,
        out_shape=[sd((256, D), BF), sd((256, D), BF), sd((256, D), F32), sd(wt.shape[:1] + (S,), BF)],
        scratch_shapes=[pltpu.VMEM(wt.shape, BF), pltpu.VMEM(wo.shape, BF), pltpu.VMEM((S, D), BF),
                        pltpu.VMEM(att.shape, BF), pltpu.VMEM((2, S, dh), F32)]
        + [quarter] * 4 + [pltpu.VMEM((16, S), F32), pltpu.VMEM((16, S), F32), pltpu.VMEM((BLK, BLK), F32),
                           pltpu.SemaphoreType.DMA((6,)), pltpu.SemaphoreType.DMA((5,)), pltpu.SemaphoreType.DMA((5,))],
        name="back",
        cost_estimate=pl.CostEstimate(flops=int(3e10), bytes_accessed=30 << 20, transcendentals=nh * S * S // 2),
        compiler_params=pltpu.CompilerParams(collective_id=1, has_side_effects=True, vmem_limit_bytes=66900000),
    )(segr, qkv, att, lse, ysum, wt, wo, m_all)


def grads_kernel(dqkv, mid_ref, ynear, yr, a_h, act_h, g_h, gu_h, y_o, gq_h, gd_h, gu_o, av, act, gv, guv, st, lsem, ssem):
    def loc(src, dst, i):
        c = pltpu.make_async_copy(src, dst, lsem.at[i])
        c.start()
        return c
    l_a = loc(a_h, av, 0)
    l_act = loc(act_h, act, 1)
    l_gv = loc(g_h, gv, 2)
    l_gu = loc(gu_h, guv, 3)

    def yout(q):
        v = ynear[q, :].astype(F32) + yr[q, :].astype(F32)
        y_o[q, :] = (mid_ref[q, :].astype(F32) + v.astype(BF).astype(F32)).astype(BF)
    tiles(256, 32, yout)
    l_a.wait()
    grad_blocks(dqkv, av, gq_h, st, ssem, False, 0, dqkv.shape[0] // 256)
    l_act.wait()
    l_gv.wait()
    l_gu.wait()
    s_gu = loc(guv, gu_o, 4)
    grad_blocks(act, gv, gd_h, st, ssem, True, 0, act.shape[1] // 256)
    s_gu.wait()


def grads_call(dqkv, mid, ynear, yr, a_all, act, g_all, gu):
    D = a_all.shape[1]
    V = pl.BlockSpec(memory_space=pltpu.VMEM)
    H = pl.BlockSpec(memory_space=pl.ANY)
    sd = jax.ShapeDtypeStruct
    full = pltpu.VMEM(a_all.shape, BF)
    rows = dqkv.shape[0] + act.shape[1]
    return pl.pallas_call(
        grads_kernel,
        in_specs=[V] * 4 + [H] * 4,
        out_specs=[V] + [H] * 3,
        out_shape=[sd(mid.shape, BF), sd((dqkv.shape[0], D), BF), sd((act.shape[1], D), BF), sd(gu.shape, BF)],
        scratch_shapes=[full, pltpu.VMEM(act.shape, BF), full, pltpu.VMEM(gu.shape, BF), pltpu.VMEM((2, 256, D), BF),
                        pltpu.SemaphoreType.DMA((5,)), pltpu.SemaphoreType.DMA((2,))],
        name="grads",
        cost_estimate=pl.CostEstimate(flops=2 * rows * D * a_all.shape[0], bytes_accessed=40 << 20, transcendentals=0),
        compiler_params=pltpu.CompilerParams(vmem_limit_bytes=66900000),
    )(dqkv, mid, ynear, yr, a_all, act, g_all, gu)


def out_grad_kernel(att, m_h, dep, go_h, mv, st, lsem, ssem):
    at = positions()
    l_m = [pltpu.make_async_copy(m_h.at[pl.ds(r * 256, 256)], mv.at[pl.ds(pl.multiple_of(at[r] * 256, 256), 256)], lsem.at[r]) for r in range(4)]
    for c in l_m:
        c.start()
    for c in l_m:
        c.wait()
    grad_blocks(att, mv, go_h, st, ssem, False, 0, att.shape[0] // 256)


def out_grad_call(att, m_all, dep):
    D = m_all.shape[1]
    V = pl.BlockSpec(memory_space=pltpu.VMEM)
    H = pl.BlockSpec(memory_space=pl.ANY)
    return pl.pallas_call(
        out_grad_kernel,
        in_specs=[V, H, H],
        out_specs=H,
        out_shape=jax.ShapeDtypeStruct((att.shape[0], D), BF),
        scratch_shapes=[pltpu.VMEM(m_all.shape, BF), pltpu.VMEM((2, 256, D), BF), pltpu.SemaphoreType.DMA((4,)), pltpu.SemaphoreType.DMA((2,))],
        name="out_grad",
        cost_estimate=pl.CostEstimate(flops=2 * att.shape[0] * m_all.size, bytes_accessed=8 << 20, transcendentals=0),
    )(att, m_all, dep)


def tail_kernel(x_ref, g_ref, hn, hr, m_ref, dg2_ref, dx_o, dg_o):
    da = (hn[...] + hr[...].astype(F32)).astype(BF).astype(F32)
    h, rstd = norm_stats(x_ref[...].astype(F32))
    v = da * row_of(g_ref)
    dx = rstd * (v - jnp.mean(v, **ROWS) - h * jnp.mean(v * h, **ROWS))
    dx_o[...] = (m_ref[...].astype(F32) + dx).astype(BF)
    s = jnp.sum(da * h, **COLS)
    i = pl.program_id(0)

    @pl.when(i == 0)
    def _():
        dg_o[...] = jnp.concatenate([s, dg2_ref[...]], 0)

    @pl.when(i > 0)
    def _():
        dg_o[0:1, :] += s


def tail_call(x, g1, hn, hr, m_all, dg2):
    n, D = x.shape
    blk = pl.BlockSpec((64, D), lambda i: (i, 0))
    whole = lambda r: pl.BlockSpec((r, D), lambda i: (0, 0))
    sd = jax.ShapeDtypeStruct
    return pl.pallas_call(
        tail_kernel, grid=(n // 64,),
        in_specs=[blk, pl.BlockSpec((D,), lambda i: (0,))] + [blk] * 3 + [whole(1)],
        out_specs=[blk, whole(2)],
        out_shape=[sd((n, D), BF), sd((2, D), F32)],
        name="tail",
        cost_estimate=pl.CostEstimate(flops=20 * n * D, bytes_accessed=14 * n * D, transcendentals=n),
    )(x, g1, hn, hr, m_all, dg2)


def swap(v, k):
    return lax.ppermute(v, 'model', [(i, i ^ k) for i in range(4)])


def local_layer(hidden_in, seg_ids, gain_attn, w_qkv, w_out, gain_mlp, w_up, w_down, grad_out):
    hidden, nh, _, dh = w_qkv.shape
    wt = w_qkv.transpose(1, 2, 3, 0).reshape(nh * 3 * dh, hidden)
    wo = w_out.reshape(nh * dh, hidden)
    x = hidden_in[0]
    mid, d_g2, qkv, att, lse, ysum, ynear, a_all, g_all, act, m_all, gw_up = front_call(x, gain_attn, gain_mlp, seg_ids, wt, wo, w_up, w_down, grad_out[0], nh)
    yr, hx, hn, dqkv = back_call(seg_ids, qkv, att, lse, ysum, wt, wo, m_all)
    hr = swap(hx, 2)
    y, gq, gw_down, gw_up = grads_call(dqkv, mid, ynear, yr, a_all, act, g_all, gw_up)
    hr, y, gq, gw_down, gw_up = lax.optimization_barrier((hr, y, gq, gw_down, gw_up))
    dx, dg = tail_call(x, gain_attn, hn, hr, m_all, d_g2)
    others = [swap(dg, k) for k in (2, 3, 1)]
    go = out_grad_call(att, m_all, dg)
    others, go = lax.optimization_barrier((others, go))
    dg = (dg + others[0] + others[1] + others[2]).astype(BF)
    gq = gq.reshape(nh, 3, dh, hidden).transpose(3, 0, 1, 2)
    return y[None], dx[None], gq, go.reshape(nh, dh, hidden), gw_up, gw_down, dg[0], dg[1]


def solution(mesh):
    act_spec = P('data', 'model', None)
    in_specs = (act_spec, P('data', None), P(), P(None, 'model', None, None), P('model', None, None), P(), P(None, 'model'), P('model', None), act_spec)
    out_specs = (act_spec, act_spec, P('data', 'model', None, None), P(('data', 'model'), None, None), P('data', 'model'), P(('data', 'model'), None), P('data'), P('data'))
    return jax.shard_map(local_layer, mesh=mesh, in_specs=in_specs, out_specs=out_specs, check_vma=False)
```

```python
import functools
import jax, jax.numpy as jnp
from jax import lax
from jax.experimental import pallas as pl
from jax.experimental.pallas import tpu as pltpu
from jax.sharding import PartitionSpec as P
BF=jnp.bfloat16; F32=jnp.float32
BLK=256

HALVES = range(2)
COLS = dict(axis=0, keepdims=True)
ROWS = dict(axis=-1, keepdims=True)


def half(s):
    return pl.ds(s * R, R)


def nn(a, b):
    return dotf(a, b, 1, 0)


def nt(a, b):
    return dotf(a, b, 1, 1)


def tn(a, b):
    return dotf(a, b, 0, 0)


def dotf(a,b,ca,cb):
    return lax.dot_general(a,b,(((ca,),(cb,)),((),())),preferred_element_type=F32)

LN_EPS = 1e-5
BIG = 1e30


def split3(v):
    hi = v.astype(BF)
    r = v - hi.astype(F32)
    md = r.astype(BF)
    return [hi, md, (r - md.astype(F32)).astype(BF)]


def attn_setup(segr, qside, kside, tri):
    S = segr.shape[1]
    seg = segr[...]
    pad = jnp.zeros((9, S), F32)
    one = jnp.ones((3, S), F32)
    hot = jnp.concatenate([(seg == d).astype(F32) for d in range(4)], 0)
    kside[...] = jnp.concatenate([hot, one, pad], 0)
    qside[...] = jnp.concatenate([(hot - 1.0) * BIG, 0.0 * one, pad], 0)
    kp = lax.broadcasted_iota(jnp.int32, (BLK, BLK), 0)
    qp = lax.broadcasted_iota(jnp.int32, (BLK, BLK), 1)
    tri[...] = jnp.where(kp <= qp, 0.0, -BIG)


def head_rows(h, dh, c):
    return pl.ds(pl.multiple_of(h * (3 * dh) + c * dh, dh), dh)


def causal(s, tri):
    n = s.shape[0]
    if n == BLK:
        return s + tri[...]
    return jnp.concatenate([s[:n - BLK], s[n - BLK:] + tri[...]], 0)


def attn_head_fwd(h, dh, qkv, qside, kside, tri, out, lse_ref):
    kt = jnp.concatenate([qkv[head_rows(h, dh, 1), :].astype(F32) * dh ** -0.5, kside[...]], 0)
    ka = kt.T.astype(BF)
    qa = jnp.concatenate([qkv[head_rows(h, dh, 0), :], qside[...].astype(BF)], 0)
    vr = head_rows(h, dh, 2)
    sc = {}

    def scores(a):
        sc[a] = nn(ka[:(a + 1) * BLK], qa[:, a * BLK:(a + 1) * BLK])
    scores(3)
    for a in range(3, -1, -1):
        ca, K = slice(a * BLK, (a + 1) * BLK), (a + 1) * BLK
        if a > 0:
            scores(a - 1)
        s = causal(sc[a], tri)
        m = jnp.max(s, **COLS)
        p = jnp.exp(s - m)
        l = jnp.sum(p, **COLS)
        o = nn(qkv[vr, 0:K], (p * (1.0 / l)).astype(BF))
        out[pl.ds(pl.multiple_of(h * dh, dh), dh), ca] = o.astype(BF)
        lse_ref[h, :, ca] = m + jnp.log(l)


def attn_head_bwd(h, dh, qkv, oall, doall, lse_ref, qside, kside, tri, gsc, dqkv):
    sc = dh ** -0.5
    S = qkv.shape[1]
    hr = pl.ds(pl.multiple_of(h * dh, dh), dh)
    kr, qr = head_rows(h, dh, 1), head_rows(h, dh, 0)
    ka = jnp.concatenate([qkv[kr, :].astype(F32) * sc, kside[...]], 0).T.astype(BF)
    one, pad = jnp.ones((3, S), F32), jnp.zeros((13, S), F32)
    va = jnp.concatenate([qkv[head_rows(h, dh, 2), :].astype(F32), one, pad], 0).T.astype(BF)
    do32 = doall[hr, :].astype(F32)
    delta = jnp.sum(do32 * oall[hr, :].astype(F32), **COLS)
    side = qside[...].astype(BF)
    qa = jnp.concatenate([qkv[qr, :], side[0:4]] + split3(-lse_ref[h]) + [side[7:16]], 0)
    da = jnp.concatenate([(do32 * sc).astype(BF)] + split3(-sc * delta) + [pad.astype(BF)], 0)
    sdp = {}

    def scores(a):
        ca, K = slice(a * BLK, (a + 1) * BLK), (a + 1) * BLK
        sdp[a] = nn(ka[:K], qa[:, ca]), nn(va[:K], da[:, ca])
    scores(3)
    for a in range(3, -1, -1):
        ca, K = slice(a * BLK, (a + 1) * BLK), (a + 1) * BLK
        q, do = qkv[qr, ca], doall[hr, ca]
        if a > 0:
            scores(a - 1)
        p = jnp.exp(causal(sdp[a][0], tri))
        ds = (p * sdp[a][1]).astype(BF)
        dqkv[qr, ca] = nn(qkv[kr, 0:K], ds).astype(BF)
        dk = nt(ds, q)
        dv = nt(p.astype(BF), do)
        if a == 3:
            gsc[0] = dk
            gsc[1] = dv
        else:
            gsc[0, 0:K] += dk
            gsc[1, 0:K] += dv
    dqkv[kr, :] = gsc[0].T.astype(BF)
    dqkv[head_rows(h, dh, 2), :] = gsc[1].T.astype(BF)


R = 128
MESH_ID = pl.DeviceIdType.MESH


def gelu_pair(z):
    c0, c1 = 0.7978845608028654, 0.044715
    z2 = z * z
    t = jnp.tanh(z * (c0 + (c0 * c1) * z2))
    h = 0.5 + 0.5 * t
    return z * h, h + (0.5 * z) * (1.0 - t * t) * (c0 + (3 * c0 * c1) * z2)


PAIR = 2
EARLY = 4


def partners():
    me = lax.axis_index('model')
    return me + 1 - 2 * lax.rem(me, 2), lax.rem(me + 2, 4)


def enter():
    core, chip = partners()
    sem = pltpu.get_barrier_semaphore()
    for dev in (core, chip):
        pl.semaphore_signal(sem, inc=1, device_id={'model': dev}, device_id_type=MESH_ID)
    pl.semaphore_wait(sem, 2)
    return core, chip


def grad_blocks(lhs, rhs, out, st, sem, across, first, last, base=0, drain=True):
    def block(i):
        return pl.ds(pl.multiple_of(i * 256, 256), 256)

    def sent(i):
        return pltpu.make_async_copy(st.at[lax.rem(i, 2)], out.at[block(i)], sem.at[lax.rem(i, 2)])

    def step(i, c):
        @pl.when(i >= base + 2)
        def _():
            sent(i - 2).wait()

        def body(q):
            v = tn(lhs[:, block(i)], rhs[:, q]) if across else nn(lhs[block(i), :], rhs[:, q])
            st[lax.rem(i, 2), :, q] = v.astype(BF)
        for j in range(rhs.shape[1] // 512):
            body(pl.ds(j * 512, 512))
        sent(i).start()
        return c
    lax.fori_loop(first, last, step, 0)
    if drain:
        sent(last - 2).wait()
        sent(last - 1).wait()


class Links:
    def __init__(self, send, recv):
        self.send, self.recv, self.n = send, recv, 0
        self.core, self.chip = partners()

    def copy(self, src, dst, dev):
        i = self.n
        self.n += 1
        return pltpu.make_async_remote_copy(src_ref=src, dst_ref=dst, send_sem=self.send.at[i], recv_sem=self.recv.at[i], device_id={'model': dev}, device_id_type=MESH_ID)

    def to_core(self, src, dst):
        return self.copy(src, dst, self.core)

    def to_chip(self, src, dst):
        return self.copy(src, dst, self.chip)


def tiles(n, size, body, together=1):
    def step(i, c):
        for j in range(together):
            body(pl.ds(pl.multiple_of((i * together + j) * size, size), size))
        return c
    lax.fori_loop(0, n // (size * together), step, 0)


def row_of(g):
    return g[...].astype(F32).reshape(1, g.shape[0])


def norm_stats(v):
    mean = jnp.mean(v, **ROWS)
    c = v - mean
    rstd = lax.rsqrt(jnp.mean(c * c, **ROWS) + LN_EPS)
    return c * rstd, rstd


def positions():
    me = lax.axis_index('model')
    core, chip = partners()
    return me, core, chip, 3 - me


def front_kernel(dh, x_ref, g1_ref, g2_ref, segr, wt_h, wo_h, wu_h, wd_h, gy_h, mid_o, dg_o, qkv, att, lse, ysum_o, ynear_o, a_h, g_h, act_h, m_h, gu_h, gd_h,
                 wo, wu, wd, gm, mb, bv, dgv, act, dz, acc, csf, csn, crf, crn, xs, xr, st, qside, kside, tri, lsem, osem, ssem, send, recv):
    D = x_ref.shape[1]
    F = wu.shape[1]
    T = 512
    QW = qkv.shape[0]
    L = Links(send, recv)
    at = positions()

    def row(r, s):
        return (r // 2) * 512 + s * 256 + (r % 2) * R

    def lanes(r, s):
        return pl.ds(pl.multiple_of(at[r] * 256 + s * R, R), R)

    def loc(src, dst, i):
        return pltpu.make_async_copy(src, dst, lsem.at[i])
    l_g = [loc(gy_h.at[half(s)], gm.at[pl.ds(row(0, s), R)], s) for s in HALVES]
    l_wt = loc(wt_h, wu.at[pl.ds(0, QW)], 2)
    l_wo = loc(wo_h, wo, 3)
    l_wd = loc(wd_h, wd, 4)
    l_wu = loc(wu_h, wu, 5)
    for c in l_g + [l_wt, l_wo, l_wd]:
        c.start()
    enter()

    def near(s):
        return pl.ds(row(0, s), R)

    def reduce_copies(cross=True):
        far = [L.to_core(csf.at[half(s)], crf.at[half(s)]) for s in HALVES]
        nr = [L.to_core(csn.at[half(s)], crn.at[half(s)]) for s in HALVES]
        return far, nr, [L.to_chip(xs.at[half(s)], xr.at[half(s)]) for s in HALVES] if cross else None

    def gather_copies(buf, first=0):
        skip = [first, 0]
        xc = [L.to_chip(buf.at[pl.ds(row(0, s) + skip[s], R - skip[s])], buf.at[pl.ds(row(2, s) + skip[s], R - skip[s])]) for s in HALVES]
        own = [L.to_core(buf.at[near(s)], buf.at[pl.ds(row(1, s), R)]) for s in HALVES]
        fwd = [L.to_core(buf.at[pl.ds(row(2, s), R)], buf.at[pl.ds(row(3, s), R)]) for s in HALVES]
        return xc, own, fwd

    pre = pl.ds(0, 32)
    e_pre = L.to_chip(gy_h.at[pre], gm.at[pl.ds(row(2, 0), 32)])
    e_pre.start()
    a_x, a_own, a_fwd = gather_copies(bv)
    e_x, e_own, e_fwd = gather_copies(gm, 32)
    b_far, b_near, b_x = reduce_copies()
    c_x, c_own, c_fwd = gather_copies(bv)
    f_far, f_near, f_x = reduce_copies()
    g_x, g_own, g_fwd = gather_copies(mb)

    def chip_sum(s, far, xc):
        far[s].wait_recv()
        rs = half(s)
        tiles(R, 32, lambda q: add_into(pl.ds(s * R + q.start, 32)))
        xc[s].start()

    def add_into(rs):
        xs[rs, :] = (xs[rs, :].astype(F32) + crf[rs, :].astype(F32)).astype(BF)

    outs = []

    def emit(src, dst, rr, s, base):
        for r in rr:
            c = pltpu.make_async_copy(src.at[pl.ds(row(r, s), R)], dst.at[pl.ds(r * 256 + s * R, R)], osem.at[base + 2 * r + s])
            c.start()
            outs.append(c)

    for s in HALVES:
        def norm1(q):
            h, _ = norm_stats(x_ref[pl.ds(s * R + q.start, 32), :].astype(F32))
            bv[pl.ds(row(0, s) + q.start, 32), :] = (h * row_of(g1_ref)).astype(BF)
        tiles(R, 32, norm1)
        a_x[s].start()
        a_own[s].start()
    for s in HALVES:
        l_g[s].wait()
        e_x[s].start()
        e_own[s].start()
    attn_setup(segr, qside, kside, tri)
    l_wt.wait()

    def qkv_rows(o, r, s):
        def body(q):
            v = nt(wu[q, :], bv[o:o + 256, :]).astype(BF)
            qkv[q, lanes(r, s)] = v[:, :R]
            qkv[q, lanes(r + 1, s)] = v[:, R:]
        tiles(QW, T, body)
    for s in HALVES:
        a_own[s].wait_recv()
        qkv_rows(s * 256, 0, s)
    for s in HALVES:
        a_x[s].wait_recv()
        a_fwd[s].start()
        a_fwd[s].wait_recv()
        qkv_rows(512 + s * 256, 2, s)
    l_wu.start()
    a_out = [pltpu.make_async_copy(bv.at[pl.ds(row(r, s), R)], a_h.at[lanes(r, s)], osem.at[40 + 2 * r + s]) for r in range(4) for s in HALVES]
    for c in a_out:
        c.start()
    lax.fori_loop(0, lse.shape[0], lambda h, c: (attn_head_fwd(h, dh, qkv, qside, kside, tri, att, lse), c)[1], 0)
    e_pre.wait_recv()
    e_x[0].wait_recv()
    e_fwd[0].start()
    for c in a_out:
        c.wait()
    for c in a_x + a_own + a_fwd:
        c.wait_send()

    l_wo.wait()

    def out_part(pos, ref, rows=slice(None)):
        def body(q):
            ref[rows, q] = tn(att[:, pos], wo[:, q]).astype(ref.dtype)
        tiles(D, T, body, PAIR)

    def whole(r):
        return pl.ds(pl.multiple_of(at[r] * 256, 256), 256)

    for s in HALVES:
        out_part(lanes(3, s), csf, half(s))
        b_far[s].start()
    for s in HALVES:
        out_part(lanes(2, s), xs, half(s))
        chip_sum(s, b_far, b_x)
    e_x[1].wait_recv()
    e_fwd[1].start()
    out_part(whole(1), csn)
    for s in HALVES:
        b_near[s].start()
    out_part(whole(0), acc)

    l_wd.wait()

    for s in HALVES:
        e_own[s].wait_recv()
        e_fwd[s].wait_recv()
        emit(gm, g_h, (0, 1, 2, 3), s, 32)

    def dact(i, c):
        def body(q):
            dgv[pl.ds(pl.multiple_of(i * 256, 256), 256), q] = nt(gm[pl.ds(pl.multiple_of(512 + i * 256, 256), 256), :], wd[q, :])
        tiles(F, T, body, PAIR)
        return c
    lax.fori_loop(0, 2, dact, 0)
    g_out = list(outs)
    outs.clear()
    l_wu.wait()
    for c in [e_pre] + e_x + e_own + e_fwd:
        c.wait_send()

    def total(rs):
        return acc[rs, :] + crn[rs, :].astype(F32) + xr[rs, :].astype(F32)

    def norm2(s):
        b_near[s].wait_recv()
        b_x[s].wait_recv()

        def body(q):
            rs = pl.ds(s * R + q.start, 32)
            att = total(rs).astype(BF).astype(F32)
            mid = (x_ref[rs, :].astype(F32) + att).astype(BF)
            mid_o[rs, :] = mid
            h, _ = norm_stats(mid.astype(F32))
            bv[pl.ds(row(0, s) + q.start, 32), :] = (h * row_of(g2_ref)).astype(BF)
        tiles(R, 32, body)
        c_x[s].start()
        c_own[s].start()

    def mlp(o):
        def body(q):
            g, d = gelu_pair(nn(bv[o:o + 256, :], wu[:, q]))
            act[o:o + 256, q] = g.astype(BF)
            up = dgv[o - 512:o - 256, q] if o >= 512 else nt(gm[o:o + 256, :], wd[q, :])
            dz[o:o + 256, q] = (d * up).astype(BF)
        tiles(F, T, body, PAIR)

    def dmlp(o, s, keep, give):
        def body(q):
            v = nt(dz[o:o + 256, :], wu[q, :])
            keep[half(s), q] = v[:R].astype(keep.dtype)
            give[half(s), q] = v[R:].astype(BF)
        tiles(D, T, body, PAIR)

    def ydown(base, keep, give):
        def chunk(s, c):
            o = pl.ds(pl.multiple_of(base + s * 256, 256), 256)
            rs = pl.ds(pl.multiple_of(s * R, R), R)

            def body(q):
                v = nn(act[o, :], wd[:, q])
                keep[rs, q] = v[:R].astype(keep.dtype)
                give[rs, q] = v[R:].astype(BF)
            tiles(D, T, body, PAIR)
            return c
        lax.fori_loop(0, 2, chunk, 0)

    def near_step(s):
        c_own[s].wait_recv()
        mlp(s * 256)
        b_near[s].wait_send()
        dmlp(s * 256, s, acc, csn)
        f_near[s].start()
        emit(act, act_h, (0, 1), s, 8)

    norm2(0)
    for c in g_out:
        c.wait()
    near_step(0)
    norm2(1)
    near_step(1)

    def far_step(s):
        c_fwd[s].wait_recv()
        mlp(512 + s * 256)
        b_far[s].wait_send()
        b_x[s].wait_send()
        dmlp(512 + s * 256, s, xs, csf)
        f_far[s].start()
        emit(act, act_h, (2, 3), s, 8)

    c_x[0].wait_recv()
    c_fwd[0].start()
    far_step(0)
    chip_sum(0, f_far, f_x)
    c_x[1].wait_recv()
    c_fwd[1].start()
    far_step(1)
    chip_sum(1, f_far, f_x)
    def dnorm2(s):
        f_near[s].wait_recv()
        f_x[s].wait_recv()

        def step(i, dgain):
            rs = pl.ds(pl.multiple_of(s * R + i * 32, 32), 32)
            db = total(rs).astype(BF).astype(F32)
            h, rstd = norm_stats(mid_o[rs, :].astype(F32))
            v = db * row_of(g2_ref)
            dm = rstd * (v - jnp.mean(v, **ROWS) - h * jnp.mean(v * h, **ROWS))
            gr = pl.ds(pl.multiple_of(row(0, s) + i * 32, 32), 32)
            mb[gr, :] = (gm[gr, :].astype(F32) + dm).astype(BF)
            return dgain + jnp.sum(db * h, **COLS)
        dgain = lax.fori_loop(0, R // 32, step, jnp.zeros((1, D), F32))
        if s == 0:
            dg_o[...] = dgain
        else:
            dg_o[...] += dgain
        g_x[s].start()
        g_own[s].start()

    def up_blocks(first, last, drain=False):
        grad_blocks(bv, dz, gu_h, st, ssem, True, first, last, drain=drain)

    up_blocks(0, 1)
    dnorm2(0)
    up_blocks(1, F // 256 - 1)
    dnorm2(1)
    y_far, y_near = reduce_copies(False)[:2]
    for s in HALVES:
        g_own[s].wait_recv()
        emit(mb, m_h, (0, 1), s, 24)
        f_far[s].wait_send()
        f_x[s].wait_send()
        f_near[s].wait_send()
    ydown(512, xs, csf)
    for c in y_far:
        c.start()
    ydown(0, acc, csn)
    for c in y_near:
        c.start()
    g_x[0].wait_recv()
    g_fwd[0].start()
    up_blocks(F // 256 - 1, F // 256, True)
    for s in HALVES:
        y_far[s].wait_recv()
        y_near[s].wait_recv()

    def ysum(q):
        ysum_o[q, :] = (xs[q, :].astype(F32) + crf[q, :].astype(F32)).astype(BF)
        ynear_o[q, :] = (acc[q, :] + crn[q, :].astype(F32)).astype(BF)
    tiles(256, 32, ysum)
    grad_blocks(act, gm, gd_h, st, ssem, True, 0, EARLY)
    g_x[1].wait_recv()
    g_fwd[1].start()
    for s in HALVES:
        g_fwd[s].wait_recv()
        emit(mb, m_h, (2, 3), s, 24)
    for c in outs:
        c.wait()
    for c in y_far + y_near + c_x + c_own + c_fwd + g_x + g_own + g_fwd:
        c.wait_send()


def front_call(x, g1, g2, segr, wt, wo, wu, wd, gy, nh):
    D = x.shape[1]
    F = wu.shape[1]
    S = 4 * x.shape[0]
    dh = wo.shape[0] // nh
    V = pl.BlockSpec(memory_space=pltpu.VMEM)
    H = pl.BlockSpec(memory_space=pl.ANY)
    sd = jax.ShapeDtypeStruct
    full = pltpu.VMEM((S, D), BF)
    quarter = pltpu.VMEM((256, D), BF)
    return pl.pallas_call(
        functools.partial(front_kernel, dh),
        in_specs=[V] * 4 + [H] * 5,
        out_specs=[V] * 7 + [H] * 6,
        out_shape=[sd((256, D), BF), sd((1, D), F32), sd(wt.shape[:1] + (S,), BF), sd((nh * dh, S), BF), sd((nh, 1, S), F32), sd((256, D), BF), sd((256, D), BF),
                   sd((S, D), BF), sd((S, D), BF), sd((S, F), BF), sd((S, D), BF), sd(wu.shape, BF), sd(wd.shape, BF)],
        scratch_shapes=[pltpu.VMEM(wo.shape, BF), pltpu.VMEM(wu.shape, BF), pltpu.VMEM(wd.shape, BF), full, full, full,
                        pltpu.VMEM((S // 2, F), F32), pltpu.VMEM((S, F), BF), pltpu.VMEM((S, F), BF), pltpu.VMEM((256, D), F32)]
        + [quarter] * 6 + [pltpu.VMEM((2, 256, F), BF), pltpu.VMEM((16, S), F32), pltpu.VMEM((16, S), F32), pltpu.VMEM((BLK, BLK), F32),
                           pltpu.SemaphoreType.DMA((6,)), pltpu.SemaphoreType.DMA((48,)),
                           pltpu.SemaphoreType.DMA((8,)), pltpu.SemaphoreType.DMA((43,)), pltpu.SemaphoreType.DMA((43,))],
        name="front",
        cost_estimate=pl.CostEstimate(flops=int(8e10), bytes_accessed=60 << 20, transcendentals=S * F),
        compiler_params=pltpu.CompilerParams(collective_id=0, has_side_effects=True, vmem_limit_bytes=66900000),
    )(x, g1, g2, segr, wt, wo, wu, wd, gy)


def back_kernel(dh, segr, qkv, att, lse, ysum, wt_h, wo_h, m_h, yr_o, hx_o, hn_o, dqkv,
                wt, wo, mv, doall, gsc, csf, csn, crf, crn, qside, kside, tri, lsem, send, recv):
    D = wt.shape[1]
    T = 512
    nh = lse.shape[0]
    L = Links(send, recv)
    at = positions()

    def lanes(r, s):
        return pl.ds(pl.multiple_of(at[r] * 256 + s * R, R), R)

    def loc(src, dst, i):
        c = pltpu.make_async_copy(src, dst, lsem.at[i])
        c.start()
        return c
    l_wo = loc(wo_h, wo, 0)
    l_m = [loc(m_h.at[pl.ds(r * 256, 256)], mv.at[pl.ds(pl.multiple_of(at[r] * 256, 256), 256)], 1 + r) for r in range(4)]
    l_wt = loc(wt_h, wt, 5)
    enter()
    y_x = L.to_chip(ysum, yr_o)
    y_x.start()
    h_far = L.to_core(csf, crf)
    h_near = L.to_core(csn, crn)
    attn_setup(segr, qside, kside, tri)
    l_wo.wait()
    for c in l_m:
        c.wait()

    def dout(q):
        doall[:, q] = nt(wo[...], mv[q, :]).astype(BF)
    tiles(4 * 256, 256, dout)
    lax.fori_loop(0, nh, lambda h, c: (attn_head_bwd(h, dh, qkv, att, doall, lse, qside, kside, tri, gsc, dqkv), c)[1], 0)
    l_wt.wait()

    def parts(far, near, to_far, to_near):
        rows = [pl.ds(pl.multiple_of(at[r] * 256, 256), 256) for r in (far, near)]

        def body(q):
            v = tn(jnp.concatenate([dqkv[:, w] for w in rows], 1), wt[:, q])
            to_far[:, q] = v[:256].astype(to_far.dtype)
            to_near[:, q] = v[256:].astype(to_near.dtype)
        tiles(D, T, body)

    def add_into(ref, got):
        def body(q):
            ref[q, :] = (ref[q, :].astype(F32) + got[q, :].astype(F32)).astype(ref.dtype)
        tiles(256, 32, body)

    parts(3, 1, csf, csn)
    h_far.start()
    h_near.start()
    parts(2, 0, hx_o, hn_o)
    h_far.wait_recv()
    add_into(hx_o, crf)
    h_near.wait_recv()
    add_into(hn_o, crn)
    y_x.wait_recv()
    for c in (y_x, h_far, h_near):
        c.wait_send()


def back_call(segr, qkv, att, lse, ysum, wt, wo, m_all):
    S, D = m_all.shape
    nh = lse.shape[0]
    dh = wo.shape[0] // nh
    V = pl.BlockSpec(memory_space=pltpu.VMEM)
    H = pl.BlockSpec(memory_space=pl.ANY)
    sd = jax.ShapeDtypeStruct
    quarter = pltpu.VMEM((256, D), BF)
    return pl.pallas_call(
        functools.partial(back_kernel, dh),
        in_specs=[V] * 5 + [H] * 3,
        out_specs=[V] * 4,
        out_shape=[sd((256, D), BF), sd((256, D), BF), sd((256, D), BF), sd(wt.shape[:1] + (S,), BF)],
        scratch_shapes=[pltpu.VMEM(wt.shape, BF), pltpu.VMEM(wo.shape, BF), pltpu.VMEM((S, D), BF),
                        pltpu.VMEM(att.shape, BF), pltpu.VMEM((2, S, dh), F32)]
        + [quarter] * 4 + [pltpu.VMEM((16, S), F32), pltpu.VMEM((16, S), F32), pltpu.VMEM((BLK, BLK), F32),
                           pltpu.SemaphoreType.DMA((6,)), pltpu.SemaphoreType.DMA((3,)), pltpu.SemaphoreType.DMA((3,))],
        name="back",
        cost_estimate=pl.CostEstimate(flops=int(3e10), bytes_accessed=30 << 20, transcendentals=nh * S * S // 2),
        compiler_params=pltpu.CompilerParams(collective_id=1, has_side_effects=True, vmem_limit_bytes=66900000),
    )(segr, qkv, att, lse, ysum, wt, wo, m_all)


def grads_kernel(dqkv, att, mid_ref, ynear, yr, a_h, m_h, act_h, g_h, gu_h, gd_h, y_o, gq_o, go_o, gd_o, gu_o, av, mv, act, gv, guv, gdv, st, lsem, ssem):
    at = positions()
    early = pl.ds(0, EARLY * 256)
    late = (act.shape[1] // 256) - EARLY

    def loc(src, dst, i):
        c = pltpu.make_async_copy(src, dst, lsem.at[i])
        c.start()
        return c
    l_a = loc(a_h, av, 0)
    l_m = [loc(m_h.at[pl.ds(r * 256, 256)], mv.at[pl.ds(pl.multiple_of(at[r] * 256, 256), 256)], 1 + r) for r in range(4)]
    l_act = loc(act_h, act, 5)
    l_gv = loc(g_h, gv, 6)
    l_gu = loc(gu_h, guv, 7)
    l_gd = loc(gd_h.at[early], gdv, 8)

    def yout(q):
        v = ynear[q, :].astype(F32) + yr[q, :].astype(F32)
        y_o[q, :] = (mid_ref[q, :].astype(F32) + v.astype(BF).astype(F32)).astype(BF)
    tiles(256, 32, yout)
    l_a.wait()
    grad_blocks(dqkv, av, gq_o, st, ssem, False, 0, dqkv.shape[0] // 256)
    for c in l_m:
        c.wait()
    l_gu.wait()
    s_gu = loc(guv, gu_o, 9)
    grad_blocks(att, mv, go_o, st, ssem, False, 0, att.shape[0] // 256)
    l_act.wait()
    l_gv.wait()
    l_gd.wait()
    s_gd = loc(gdv, gd_o.at[early], 10)
    grad_blocks(act, gv, gd_o, st, ssem, True, EARLY, EARLY + late, EARLY)
    s_gu.wait()
    s_gd.wait()


def grads_call(dqkv, att, mid, ynear, yr, a_all, m_all, act, g_all, gu, gd):
    D = a_all.shape[1]
    V = pl.BlockSpec(memory_space=pltpu.VMEM)
    H = pl.BlockSpec(memory_space=pl.ANY)
    sd = jax.ShapeDtypeStruct
    full = pltpu.VMEM(a_all.shape, BF)
    rows = dqkv.shape[0] + att.shape[0]
    return pl.pallas_call(
        grads_kernel,
        in_specs=[V] * 5 + [H] * 6,
        out_specs=[V] + [H] * 4,
        out_shape=[sd(mid.shape, BF), sd((dqkv.shape[0], D), BF), sd((att.shape[0], D), BF), sd(gd.shape, BF), sd(gu.shape, BF)],
        scratch_shapes=[full, full, pltpu.VMEM(act.shape, BF), full, pltpu.VMEM(gu.shape, BF), pltpu.VMEM((EARLY * 256, D), BF), pltpu.VMEM((2, 256, D), BF),
                        pltpu.SemaphoreType.DMA((11,)), pltpu.SemaphoreType.DMA((2,))],
        name="grads",
        cost_estimate=pl.CostEstimate(flops=3 * rows * D * a_all.shape[0], bytes_accessed=60 << 20, transcendentals=0),
        compiler_params=pltpu.CompilerParams(vmem_limit_bytes=66900000),
    )(dqkv, att, mid, ynear, yr, a_all, m_all, act, g_all, gu, gd)


def tail_kernel(x_ref, g_ref, hn, hr, m_ref, dg2_ref, dx_o, dg_o):
    da = (hn[...].astype(F32) + hr[...].astype(F32)).astype(BF).astype(F32)
    h, rstd = norm_stats(x_ref[...].astype(F32))
    v = da * row_of(g_ref)
    dx = rstd * (v - jnp.mean(v, **ROWS) - h * jnp.mean(v * h, **ROWS))
    dx_o[...] = (m_ref[...].astype(F32) + dx).astype(BF)
    s = jnp.sum(da * h, **COLS)
    i = pl.program_id(0)

    @pl.when(i == 0)
    def _():
        dg_o[...] = jnp.concatenate([s, dg2_ref[...]], 0)

    @pl.when(i > 0)
    def _():
        dg_o[0:1, :] += s


def tail_call(x, g1, hn, hr, m_all, dg2):
    n, D = x.shape
    blk = pl.BlockSpec((128, D), lambda i: (i, 0))
    whole = lambda r: pl.BlockSpec((r, D), lambda i: (0, 0))
    sd = jax.ShapeDtypeStruct
    return pl.pallas_call(
        tail_kernel, grid=(n // 128,),
        in_specs=[blk, pl.BlockSpec((D,), lambda i: (0,))] + [blk] * 3 + [whole(1)],
        out_specs=[blk, whole(2)],
        out_shape=[sd((n, D), BF), sd((2, D), F32)],
        name="tail",
        cost_estimate=pl.CostEstimate(flops=20 * n * D, bytes_accessed=14 * n * D, transcendentals=n),
    )(x, g1, hn, hr, m_all, dg2)


def swap(v, k):
    return lax.ppermute(v, 'model', [(i, i ^ k) for i in range(4)])


def local_layer(hidden_in, seg_ids, gain_attn, w_qkv, w_out, gain_mlp, w_up, w_down, grad_out):
    hidden, nh, _, dh = w_qkv.shape
    wt = w_qkv.transpose(1, 2, 3, 0).reshape(nh * 3 * dh, hidden)
    wo = w_out.reshape(nh * dh, hidden)
    x = hidden_in[0]
    mid, d_g2, qkv, att, lse, ysum, ynear, a_all, g_all, act, m_all, gw_up, gw_down = front_call(x, gain_attn, gain_mlp, seg_ids, wt, wo, w_up, w_down, grad_out[0], nh)
    yr, hx, hn, dqkv = back_call(seg_ids, qkv, att, lse, ysum, wt, wo, m_all)
    hr = swap(hx, 2)
    y, gq, go, gw_down, gw_up = grads_call(dqkv, att, mid, ynear, yr, a_all, m_all, act, g_all, gw_up, gw_down)
    hr, y, gq, go, gw_down, gw_up = lax.optimization_barrier((hr, y, gq, go, gw_down, gw_up))
    dx, dg = tail_call(x, gain_attn, hn, hr, m_all, d_g2)
    others = [swap(dg, k) for k in (2, 3, 1)]
    dg = ((dg + others[2]) + (others[0] + others[1])).astype(BF)
    gq = gq.reshape(nh, 3, dh, hidden).transpose(3, 0, 1, 2)
    return y[None], dx[None], gq, go.reshape(nh, dh, hidden), gw_up, gw_down, dg[0], dg[1]


def solution(mesh):
    act_spec = P('data', 'model', None)
    in_specs = (act_spec, P('data', None), P(), P(None, 'model', None, None), P('model', None, None), P(), P(None, 'model'), P('model', None), act_spec)
    out_specs = (act_spec, act_spec, P('data', 'model', None, None), P(('data', 'model'), None, None), P('data', 'model'), P(('data', 'model'), None), P('data'), P('data'))
    return jax.shard_map(local_layer, mesh=mesh, in_specs=in_specs, out_specs=out_specs, check_vma=False)
```

```python
import functools
import jax, jax.numpy as jnp
from jax import lax
from jax.experimental import pallas as pl
from jax.experimental.pallas import tpu as pltpu
from jax.sharding import PartitionSpec as P
BF=jnp.bfloat16; F32=jnp.float32
BLK=256

HALVES = range(2)
COLS = dict(axis=0, keepdims=True)
ROWS = dict(axis=-1, keepdims=True)


def half(s):
    return pl.ds(s * R, R)


def nn(a, b):
    return dotf(a, b, 1, 0)


def nt(a, b):
    return dotf(a, b, 1, 1)


def tn(a, b):
    return dotf(a, b, 0, 0)


def dotf(a,b,ca,cb):
    return lax.dot_general(a,b,(((ca,),(cb,)),((),())),preferred_element_type=F32)

LN_EPS = 1e-5
BIG = 1e30


def split3(v):
    hi = v.astype(BF)
    r = v - hi.astype(F32)
    md = r.astype(BF)
    return [hi, md, (r - md.astype(F32)).astype(BF)]


def attn_setup(segr, qside, kside, tri):
    S = segr.shape[1]
    seg = segr[...]
    pad = jnp.zeros((9, S), F32)
    one = jnp.ones((3, S), F32)
    hot = jnp.concatenate([(seg == d).astype(F32) for d in range(4)], 0)
    kside[...] = jnp.concatenate([hot, one, pad], 0)
    qside[...] = jnp.concatenate([(hot - 1.0) * BIG, 0.0 * one, pad], 0)
    kp = lax.broadcasted_iota(jnp.int32, (BLK, BLK), 0)
    qp = lax.broadcasted_iota(jnp.int32, (BLK, BLK), 1)
    tri[...] = jnp.where(kp <= qp, 0.0, -BIG)


def head_rows(h, dh, c):
    return pl.ds(pl.multiple_of(h * (3 * dh) + c * dh, dh), dh)


def causal(s, tri):
    n = s.shape[0]
    if n == BLK:
        return s + tri[...]
    return jnp.concatenate([s[:n - BLK], s[n - BLK:] + tri[...]], 0)


def attn_head_fwd(h, dh, qkv, qside, kside, tri, out, lse_ref):
    kt = jnp.concatenate([qkv[head_rows(h, dh, 1), :].astype(F32) * dh ** -0.5, kside[...]], 0)
    ka = kt.T.astype(BF)
    qa = jnp.concatenate([qkv[head_rows(h, dh, 0), :], qside[...].astype(BF)], 0)
    vr = head_rows(h, dh, 2)
    sc = {}

    def scores(a):
        sc[a] = nn(ka[:(a + 1) * BLK], qa[:, a * BLK:(a + 1) * BLK])
    scores(3)
    for a in range(3, -1, -1):
        ca, K = slice(a * BLK, (a + 1) * BLK), (a + 1) * BLK
        if a > 0:
            scores(a - 1)
        s = causal(sc[a], tri)
        m = jnp.max(s, **COLS)
        p = jnp.exp(s - m)
        l = jnp.sum(p, **COLS)
        o = nn(qkv[vr, 0:K], (p * (1.0 / l)).astype(BF))
        out[pl.ds(pl.multiple_of(h * dh, dh), dh), ca] = o.astype(BF)
        lse_ref[h, :, ca] = m + jnp.log(l)


def attn_head_bwd(h, dh, qkv, oall, doall, lse_ref, qside, kside, tri, gsc, dqkv):
    sc = dh ** -0.5
    S = qkv.shape[1]
    hr = pl.ds(pl.multiple_of(h * dh, dh), dh)
    kr, qr = head_rows(h, dh, 1), head_rows(h, dh, 0)
    ka = jnp.concatenate([qkv[kr, :].astype(F32) * sc, kside[...]], 0).T.astype(BF)
    one, pad = jnp.ones((3, S), F32), jnp.zeros((13, S), F32)
    va = jnp.concatenate([qkv[head_rows(h, dh, 2), :].astype(F32), one, pad], 0).T.astype(BF)
    do32 = doall[hr, :].astype(F32)
    delta = jnp.sum(do32 * oall[hr, :].astype(F32), **COLS)
    side = qside[...].astype(BF)
    qa = jnp.concatenate([qkv[qr, :], side[0:4]] + split3(-lse_ref[h]) + [side[7:16]], 0)
    da = jnp.concatenate([(do32 * sc).astype(BF)] + split3(-sc * delta) + [pad.astype(BF)], 0)
    sdp = {}

    def scores(a):
        ca, K = slice(a * BLK, (a + 1) * BLK), (a + 1) * BLK
        sdp[a] = nn(ka[:K], qa[:, ca]), nn(va[:K], da[:, ca])
    scores(3)
    for a in range(3, -1, -1):
        ca, K = slice(a * BLK, (a + 1) * BLK), (a + 1) * BLK
        q, do = qkv[qr, ca], doall[hr, ca]
        if a > 0:
            scores(a - 1)
        p = jnp.exp(causal(sdp[a][0], tri))
        ds = (p * sdp[a][1]).astype(BF)
        dqkv[qr, ca] = nn(qkv[kr, 0:K], ds).astype(BF)
        dk = nt(ds, q)
        dv = nt(p.astype(BF), do)
        if a == 3:
            gsc[0] = dk
            gsc[1] = dv
        else:
            gsc[0, 0:K] += dk
            gsc[1, 0:K] += dv
    dqkv[kr, :] = gsc[0].T.astype(BF)
    dqkv[head_rows(h, dh, 2), :] = gsc[1].T.astype(BF)


R = 128
MESH_ID = pl.DeviceIdType.MESH


def gelu_pair(z):
    c0, c1 = 0.7978845608028654, 0.044715
    z2 = z * z
    t = jnp.tanh(z * (c0 + (c0 * c1) * z2))
    h = 0.5 + 0.5 * t
    return z * h, h + (0.5 * z) * (1.0 - t * t) * (c0 + (3 * c0 * c1) * z2)


PAIR = 2
EARLY = 4


def partners():
    me = lax.axis_index('model')
    return me + 1 - 2 * lax.rem(me, 2), lax.rem(me + 2, 4)


def enter():
    core, chip = partners()
    sem = pltpu.get_barrier_semaphore()
    for dev in (core, chip):
        pl.semaphore_signal(sem, inc=1, device_id={'model': dev}, device_id_type=MESH_ID)
    pl.semaphore_wait(sem, 2)
    return core, chip


def grad_blocks(lhs, rhs, out, st, sem, across, first, last, base=0, drain=True):
    def sent(i):
        return pltpu.make_async_copy(st.at[lax.rem(i, 2)], out.at[block(i)], sem.at[lax.rem(i, 2)])

    def step(i, c):
        @pl.when(i >= base + 2)
        def _():
            sent(i - 2).wait()

        def body(q):
            v = tn(lhs[:, block(i)], rhs[:, q]) if across else nn(lhs[block(i), :], rhs[:, q])
            st[lax.rem(i, 2), :, q] = v.astype(BF)
        for j in range(rhs.shape[1] // 512):
            body(pl.ds(j * 512, 512))
        sent(i).start()
        return c
    lax.fori_loop(first, last, step, 0)
    if drain:
        sent(last - 2).wait()
        sent(last - 1).wait()


class Links:
    def __init__(self, send, recv):
        self.send, self.recv, self.n = send, recv, 0
        self.core, self.chip = partners()

    def copy(self, src, dst, dev):
        i = self.n
        self.n += 1
        return pltpu.make_async_remote_copy(src_ref=src, dst_ref=dst, send_sem=self.send.at[i], recv_sem=self.recv.at[i], device_id={'model': dev}, device_id_type=MESH_ID)

    def to_core(self, src, dst):
        return self.copy(src, dst, self.core)

    def to_chip(self, src, dst):
        return self.copy(src, dst, self.chip)


def tiles(n, size, body, together=1):
    def step(i, c):
        for j in range(together):
            body(pl.ds(pl.multiple_of((i * together + j) * size, size), size))
        return c
    lax.fori_loop(0, n // (size * together), step, 0)


def pairs(n, body):
    def step(i, c):
        for j in HALVES:
            body(i * 2 + j, j)
        return c
    lax.fori_loop(0, n // 2, step, 0)


def block(i, n=BLK):
    return pl.ds(pl.multiple_of(i * n, n), n)


def block_at(r):
    return pl.ds(r * BLK, BLK)


def row_of(g):
    return g[...].astype(F32).reshape(1, g.shape[0])


def norm_stats(v):
    mean = jnp.mean(v, **ROWS)
    c = v - mean
    rstd = lax.rsqrt(jnp.mean(c * c, **ROWS) + LN_EPS)
    return c * rstd, rstd


def positions():
    me = lax.axis_index('model')
    core, chip = partners()
    return me, core, chip, 3 - me


def front_kernel(dh, g1_ref, g2_ref, segr, x_h, wt_h, wo_h, wu_h, wd_h, gy_h, dg_o, lse, mid_h, qkv_h, att_h, ysum_h, ynear_h, a_h, g_h, act_h, m_h, gu_h, gd_h,
                 x_ref, mid_o, qkv, att, wo, wu, wd, gm, mb, bv, dgv, act, dz, acc, csf, csn, crf, crn, xs, xr, st, qside, kside, tri, lsem, osem, ssem, send, recv):
    D, F = wu.shape
    T = 512
    QW = qkv.shape[0]
    L = Links(send, recv)
    at = positions()

    def row(r, s):
        return (r // 2) * 512 + s * 256 + (r % 2) * R

    def lanes(r, s):
        return pl.ds(pl.multiple_of(at[r] * 256 + s * R, R), R)

    def loc(src, dst, i):
        return pltpu.make_async_copy(src, dst, lsem.at[i])
    l_g = [loc(gy_h.at[half(s)], gm.at[pl.ds(row(0, s), R)], s) for s in HALVES]
    l_wt = loc(wt_h, wu.at[pl.ds(0, QW)], 2)
    l_wo = loc(wo_h, wo, 3)
    l_wd = loc(wd_h, wd, 4)
    l_wu = loc(wu_h, wu, 5)
    l_x = [loc(x_h.at[half(s)], x_ref.at[half(s)], 6 + s) for s in HALVES]
    for c in l_x + l_g + [l_wt, l_wo, l_wd]:
        c.start()
    enter()

    def near(s):
        return pl.ds(row(0, s), R)

    def reduce_copies(cross=True):
        far = [L.to_core(csf.at[half(s)], crf.at[half(s)]) for s in HALVES]
        nr = [L.to_core(csn.at[half(s)], crn.at[half(s)]) for s in HALVES]
        return far, nr, [L.to_chip(xs.at[half(s)], xr.at[half(s)]) for s in HALVES] if cross else None

    def gather_copies(buf, first=0):
        skip = [first, 0]
        xc = [L.to_chip(buf.at[pl.ds(row(0, s) + skip[s], R - skip[s])], buf.at[pl.ds(row(2, s) + skip[s], R - skip[s])]) for s in HALVES]
        own = [L.to_core(buf.at[near(s)], buf.at[pl.ds(row(1, s), R)]) for s in HALVES]
        fwd = [L.to_core(buf.at[pl.ds(row(2, s), R)], buf.at[pl.ds(row(3, s), R)]) for s in HALVES]
        return xc, own, fwd

    pre = pl.ds(0, 32)
    e_pre = L.to_chip(gy_h.at[pre], gm.at[pl.ds(row(2, 0), 32)])
    e_pre.start()
    a_x, a_own, a_fwd = gather_copies(bv)
    e_x, e_own, e_fwd = gather_copies(gm, 32)
    b_far, b_near, b_x = reduce_copies()
    c_x, c_own, c_fwd = gather_copies(bv)
    f_far, f_near, f_x = reduce_copies()
    g_x, g_own, g_fwd = gather_copies(mb)

    def chip_sum(s, far, xc):
        far[s].wait_recv()
        rs = half(s)
        tiles(R, 32, lambda q: add_into(pl.ds(s * R + q.start, 32)))
        xc[s].start()

    def add_into(rs):
        xs[rs, :] = (xs[rs, :].astype(F32) + crf[rs, :].astype(F32)).astype(BF)

    outs = []

    def emit(src, dst, rr, s, base):
        for r in rr:
            c = pltpu.make_async_copy(src.at[pl.ds(row(r, s), R)], dst.at[pl.ds(r * 256 + s * R, R)], osem.at[base + 2 * r + s])
            c.start()
            outs.append(c)

    for s in HALVES:
        def norm1(q):
            h, _ = norm_stats(x_ref[pl.ds(s * R + q.start, 32), :].astype(F32))
            bv[pl.ds(row(0, s) + q.start, 32), :] = (h * row_of(g1_ref)).astype(BF)
        l_x[s].wait()
        tiles(R, 32, norm1)
        a_x[s].start()
        a_own[s].start()
    for s in HALVES:
        l_g[s].wait()
        e_x[s].start()
        e_own[s].start()
    attn_setup(segr, qside, kside, tri)
    l_wt.wait()

    def qkv_rows(o, r, s):
        def body(q):
            v = nt(wu[q, :], bv[o:o + 256, :]).astype(BF)
            qkv[q, lanes(r, s)] = v[:, :R]
            qkv[q, lanes(r + 1, s)] = v[:, R:]
        tiles(QW, T, body)
    for s in HALVES:
        a_own[s].wait_recv()
        qkv_rows(s * 256, 0, s)
    for s in HALVES:
        a_x[s].wait_recv()
        a_fwd[s].start()
        a_fwd[s].wait_recv()
        qkv_rows(512 + s * 256, 2, s)
    l_wu.start()
    a_out = [pltpu.make_async_copy(bv.at[pl.ds(row(r, s), R)], a_h.at[lanes(r, s)], osem.at[40 + 2 * r + s]) for r in range(4) for s in HALVES]
    for c in a_out:
        c.start()
    pairs(lse.shape[0], lambda h, j: attn_head_fwd(h, dh, qkv, qside, kside, tri, att, lse))
    late = []

    def put_out(src, dst):
        late.append(pltpu.make_async_copy(src, dst, osem.at[len(late)]))
        late[-1].start()
    put_out(qkv, qkv_h)
    put_out(att, att_h)
    e_pre.wait_recv()
    e_x[0].wait_recv()
    e_fwd[0].start()
    for c in a_out:
        c.wait()
    for c in a_x + a_own + a_fwd:
        c.wait_send()

    l_wo.wait()

    def out_part(pos, ref, rows=slice(None)):
        def body(q):
            ref[rows, q] = tn(att[:, pos], wo[:, q]).astype(ref.dtype)
        tiles(D, T, body, PAIR)

    def whole(r):
        return block(at[r])

    for s in HALVES:
        out_part(lanes(3, s), csf, half(s))
        b_far[s].start()
    for s in HALVES:
        out_part(lanes(2, s), xs, half(s))
        chip_sum(s, b_far, b_x)
    e_x[1].wait_recv()
    e_fwd[1].start()
    out_part(whole(1), csn)
    for s in HALVES:
        b_near[s].start()
    out_part(whole(0), acc)

    l_wd.wait()

    for s in HALVES:
        e_own[s].wait_recv()
        e_fwd[s].wait_recv()
        emit(gm, g_h, (0, 1, 2, 3), s, 32)

    def dact(i, c):
        def body(q):
            dgv[block(i), q] = nt(gm[pl.ds(pl.multiple_of(512 + i * 256, 256), 256), :], wd[q, :])
        tiles(F, T, body, PAIR)
        return c
    lax.fori_loop(0, 2, dact, 0)
    g_out = list(outs)
    outs.clear()
    l_wu.wait()
    for c in [e_pre] + e_x + e_own + e_fwd:
        c.wait_send()

    def total(rs):
        return acc[rs, :] + crn[rs, :].astype(F32) + xr[rs, :].astype(F32)

    def norm2(s):
        b_near[s].wait_recv()
        b_x[s].wait_recv()

        def body(q):
            rs = pl.ds(s * R + q.start, 32)
            att = total(rs).astype(BF).astype(F32)
            mid = (x_ref[rs, :].astype(F32) + att).astype(BF)
            mid_o[rs, :] = mid
            h, _ = norm_stats(mid.astype(F32))
            bv[pl.ds(row(0, s) + q.start, 32), :] = (h * row_of(g2_ref)).astype(BF)
        tiles(R, 32, body)
        c_x[s].start()
        c_own[s].start()

    def mlp(o):
        def body(q):
            g, d = gelu_pair(nn(bv[o:o + 256, :], wu[:, q]))
            act[o:o + 256, q] = g.astype(BF)
            up = dgv[o - 512:o - 256, q] if o >= 512 else nt(gm[o:o + 256, :], wd[q, :])
            dz[o:o + 256, q] = (d * up).astype(BF)
        tiles(F, T, body, PAIR)

    def dmlp(o, s, keep, give):
        def body(q):
            v = nt(dz[o:o + 256, :], wu[q, :])
            keep[half(s), q] = v[:R].astype(keep.dtype)
            give[half(s), q] = v[R:].astype(BF)
        tiles(D, T, body, PAIR)

    def ydown(base, keep, give):
        def chunk(s, c):
            o = pl.ds(pl.multiple_of(base + s * 256, 256), 256)
            rs = block(s, R)

            def body(q):
                v = nn(act[o, :], wd[:, q])
                keep[rs, q] = v[:R].astype(keep.dtype)
                give[rs, q] = v[R:].astype(BF)
            tiles(D, T, body, PAIR)
            return c
        lax.fori_loop(0, 2, chunk, 0)

    def near_step(s):
        c_own[s].wait_recv()
        mlp(s * 256)
        b_near[s].wait_send()
        dmlp(s * 256, s, acc, csn)
        f_near[s].start()
        emit(act, act_h, (0, 1), s, 8)

    norm2(0)
    for c in g_out:
        c.wait()
    near_step(0)
    norm2(1)
    put_out(mid_o, mid_h)
    near_step(1)

    def far_step(s):
        c_fwd[s].wait_recv()
        mlp(512 + s * 256)
        b_far[s].wait_send()
        b_x[s].wait_send()
        dmlp(512 + s * 256, s, xs, csf)
        f_far[s].start()
        emit(act, act_h, (2, 3), s, 8)

    c_x[0].wait_recv()
    c_fwd[0].start()
    far_step(0)
    chip_sum(0, f_far, f_x)
    c_x[1].wait_recv()
    c_fwd[1].start()
    far_step(1)
    chip_sum(1, f_far, f_x)
    def dnorm2(s):
        f_near[s].wait_recv()
        f_x[s].wait_recv()

        def step(i, dgain):
            rs = pl.ds(pl.multiple_of(s * R + i * 32, 32), 32)
            db = total(rs).astype(BF).astype(F32)
            h, rstd = norm_stats(mid_o[rs, :].astype(F32))
            v = db * row_of(g2_ref)
            dm = rstd * (v - jnp.mean(v, **ROWS) - h * jnp.mean(v * h, **ROWS))
            gr = pl.ds(pl.multiple_of(row(0, s) + i * 32, 32), 32)
            mb[gr, :] = (gm[gr, :].astype(F32) + dm).astype(BF)
            return dgain + jnp.sum(db * h, **COLS)
        dgain = lax.fori_loop(0, R // 32, step, jnp.zeros((1, D), F32))
        if s == 0:
            dg_o[...] = dgain
        else:
            dg_o[...] += dgain
        g_x[s].start()
        g_own[s].start()

    def up_blocks(first, last, drain=False):
        grad_blocks(bv, dz, gu_h, st, ssem, True, first, last, drain=drain)

    up_blocks(0, 1)
    dnorm2(0)
    up_blocks(1, F // 256 - 1)
    dnorm2(1)
    y_far, y_near = reduce_copies(False)[:2]
    for s in HALVES:
        g_own[s].wait_recv()
        emit(mb, m_h, (0, 1), s, 24)
        f_far[s].wait_send()
        f_x[s].wait_send()
        f_near[s].wait_send()
    ydown(512, xs, csf)
    for c in y_far:
        c.start()
    ydown(0, acc, csn)
    for c in y_near:
        c.start()
    g_x[0].wait_recv()
    g_fwd[0].start()
    up_blocks(F // 256 - 1, F // 256, True)
    for s in HALVES:
        y_far[s].wait_recv()
        y_near[s].wait_recv()

    def ysum(q):
        xs[q, :] = (xs[q, :].astype(F32) + crf[q, :].astype(F32)).astype(BF)
        crn[q, :] = (acc[q, :] + crn[q, :].astype(F32)).astype(BF)
    tiles(256, 32, ysum)
    put_out(xs, ysum_h)
    put_out(crn, ynear_h)
    grad_blocks(act, gm, gd_h, st, ssem, True, 0, EARLY)
    g_x[1].wait_recv()
    g_fwd[1].start()
    for s in HALVES:
        g_fwd[s].wait_recv()
        emit(mb, m_h, (2, 3), s, 24)
    for c in outs + late:
        c.wait()
    for c in y_far + y_near + c_x + c_own + c_fwd + g_x + g_own + g_fwd:
        c.wait_send()


def front_call(x, g1, g2, segr, wt, wo, wu, wd, gy, nh):
    D = x.shape[1]
    F = wu.shape[1]
    S = 4 * x.shape[0]
    dh = wo.shape[0] // nh
    V = pl.BlockSpec(memory_space=pltpu.VMEM)
    H = pl.BlockSpec(memory_space=pl.ANY)
    sd = jax.ShapeDtypeStruct
    full = pltpu.VMEM((S, D), BF)
    quarter = pltpu.VMEM((256, D), BF)
    return pl.pallas_call(
        functools.partial(front_kernel, dh),
        in_specs=[V] * 3 + [H] * 6,
        out_specs=[V] * 2 + [H] * 11,
        out_shape=[sd((1, D), F32), sd((nh, 1, S), F32), sd(x.shape, BF), sd(wt.shape[:1] + (S,), BF), sd((nh * dh, S), BF), sd(x.shape, BF), sd(x.shape, BF),
                   sd((S, D), BF), sd((S, D), BF), sd((S, F), BF), sd((S, D), BF), sd(wu.shape, BF), sd(wd.shape, BF)],
        scratch_shapes=[quarter, quarter, pltpu.VMEM(wt.shape[:1] + (S,), BF), pltpu.VMEM((nh * dh, S), BF), pltpu.VMEM(wo.shape, BF), pltpu.VMEM(wu.shape, BF), pltpu.VMEM(wd.shape, BF), full, full, full,
                        pltpu.VMEM((S // 2, F), F32), pltpu.VMEM((S, F), BF), pltpu.VMEM((S, F), BF), pltpu.VMEM((256, D), F32)]
        + [quarter] * 6 + [pltpu.VMEM((2, 256, F), BF), pltpu.VMEM((16, S), F32), pltpu.VMEM((16, S), F32), pltpu.VMEM((BLK, BLK), F32),
                           pltpu.SemaphoreType.DMA((8,)), pltpu.SemaphoreType.DMA((48,)),
                           pltpu.SemaphoreType.DMA((8,)), pltpu.SemaphoreType.DMA((43,)), pltpu.SemaphoreType.DMA((43,))],
        name="front",
        cost_estimate=pl.CostEstimate(flops=int(8e10), bytes_accessed=60 << 20, transcendentals=S * F),
        compiler_params=pltpu.CompilerParams(collective_id=0, has_side_effects=True, vmem_limit_bytes=66900000),
    )(g1, g2, segr, x, wt, wo, wu, wd, gy)


def back_kernel(dh, segr, lse, qkv_h, att_h, ysum, wt_h, wo_h, m_h, yr_o, hx_h, hn_h, dqkv_h,
                qkv, att, dqkv, hx_o, hn_o, wt, wo, mv, doall, gsc, csf, csn, crf, crn, qside, kside, tri, lsem, send, recv):
    D = wt.shape[1]
    T = 512
    nh = lse.shape[0]
    L = Links(send, recv)
    at = positions()

    def lanes(r, s):
        return pl.ds(pl.multiple_of(at[r] * 256 + s * R, R), R)

    def loc(src, dst, i):
        c = pltpu.make_async_copy(src, dst, lsem.at[i])
        c.start()
        return c
    l_wo = loc(wo_h, wo, 0)
    l_m = [loc(m_h.at[block_at(r)], mv.at[block(at[r])], 1 + r) for r in range(4)]
    enter()
    l_qkv = loc(qkv_h, qkv, 6)
    l_att = loc(att_h, att, 7)
    y_x = L.to_chip(ysum, yr_o)
    y_x.start()
    h_far = L.to_core(csf, crf)
    h_near = L.to_core(csn, crn)
    attn_setup(segr, qside, kside, tri)
    l_wo.wait()
    for c in l_m:
        c.wait()

    def dout(q):
        doall[:, q] = nt(wo[...], mv[q, :]).astype(BF)
    tiles(4 * 256, 256, dout)
    l_wt = loc(wt_h, wt, 5)
    l_qkv.wait()
    l_att.wait()
    pairs(nh, lambda h, j: attn_head_bwd(h, dh, qkv, att, doall, lse, qside, kside, tri, gsc.at[j], dqkv))
    o_dqkv = loc(dqkv, dqkv_h, 8)
    l_wt.wait()

    def parts(far, near, to_far, to_near):
        rows = [block(at[r]) for r in (far, near)]

        def body(q):
            v = tn(jnp.concatenate([dqkv[:, w] for w in rows], 1), wt[:, q])
            to_far[:, q] = v[:256].astype(to_far.dtype)
            to_near[:, q] = v[256:].astype(to_near.dtype)
        tiles(D, T, body)

    def add_into(ref, got):
        def body(q):
            ref[q, :] = (ref[q, :].astype(F32) + got[q, :].astype(F32)).astype(ref.dtype)
        tiles(256, 32, body)

    parts(3, 1, csf, csn)
    h_far.start()
    h_near.start()
    parts(2, 0, hx_o, hn_o)
    h_far.wait_recv()
    add_into(hx_o, crf)
    o_hx = loc(hx_o, hx_h, 9)
    h_near.wait_recv()
    add_into(hn_o, crn)
    o_hn = loc(hn_o, hn_h, 10)
    for c in (o_dqkv, o_hx, o_hn):
        c.wait()
    y_x.wait_recv()
    for c in (y_x, h_far, h_near):
        c.wait_send()


def back_call(segr, qkv, att, lse, ysum, wt, wo, m_all):
    S, D = m_all.shape
    nh = lse.shape[0]
    dh = wo.shape[0] // nh
    V = pl.BlockSpec(memory_space=pltpu.VMEM)
    H = pl.BlockSpec(memory_space=pl.ANY)
    sd = jax.ShapeDtypeStruct
    quarter = pltpu.VMEM((256, D), BF)
    return pl.pallas_call(
        functools.partial(back_kernel, dh),
        in_specs=[V] * 2 + [H] * 6,
        out_specs=[H] * 4,
        out_shape=[sd(ysum.shape, BF), sd(ysum.shape, BF), sd(ysum.shape, BF), sd(qkv.shape, BF)],
        scratch_shapes=[pltpu.VMEM(qkv.shape, BF), pltpu.VMEM(att.shape, BF), pltpu.VMEM(qkv.shape, BF), quarter, quarter,
                        pltpu.VMEM(wt.shape, BF), pltpu.VMEM(wo.shape, BF), pltpu.VMEM((S, D), BF),
                        pltpu.VMEM(att.shape, BF), pltpu.VMEM((2, 2, S, dh), F32)]
        + [quarter] * 4 + [pltpu.VMEM((16, S), F32), pltpu.VMEM((16, S), F32), pltpu.VMEM((BLK, BLK), F32),
                           pltpu.SemaphoreType.DMA((11,)), pltpu.SemaphoreType.DMA((3,)), pltpu.SemaphoreType.DMA((3,))],
        name="back",
        cost_estimate=pl.CostEstimate(flops=int(3e10), bytes_accessed=30 << 20, transcendentals=nh * S * S // 2),
        compiler_params=pltpu.CompilerParams(collective_id=1, has_side_effects=True, vmem_limit_bytes=66900000),
    )(segr, lse, qkv, att, ysum, wt, wo, m_all)


def grads_kernel(dqkv_h, att_h, mid_h, ynear_h, yr_h, a_h, m_h, act_h, g_h, gu_h, gd_h, y_h, gq_o, go_o, gd_o, gu_o, dqkv, att, mid_ref, ynear, yr, y_o, av, mv, act, gv, guv, gdv, st, lsem, ssem):
    at = positions()
    early = pl.ds(0, EARLY * 256)
    late = (act.shape[1] // 256) - EARLY

    def loc(src, dst, i):
        c = pltpu.make_async_copy(src, dst, lsem.at[i])
        c.start()
        return c
    l_a = loc(a_h, av, 0)
    l_dqkv = loc(dqkv_h, dqkv, 11)
    l_m = [loc(m_h.at[block_at(r)], mv.at[block(at[r])], 1 + r) for r in range(4)]
    l_att = loc(att_h, att, 12)
    l_y = [loc(p, q, 13 + i) for i, (p, q) in enumerate(((mid_h, mid_ref), (ynear_h, ynear), (yr_h, yr)))]
    l_act = loc(act_h, act, 5)
    l_gv = loc(g_h, gv, 6)
    l_gu = loc(gu_h, guv, 7)
    l_gd = loc(gd_h.at[early], gdv, 8)

    def yout(q):
        v = ynear[q, :].astype(F32) + yr[q, :].astype(F32)
        y_o[q, :] = (mid_ref[q, :].astype(F32) + v.astype(BF).astype(F32)).astype(BF)
    l_a.wait()
    l_dqkv.wait()
    grad_blocks(dqkv, av, gq_o, st, ssem, False, 0, dqkv.shape[0] // 256)
    for c in l_m + l_y + [l_att, l_gu]:
        c.wait()
    tiles(256, 32, yout)
    s_y = loc(y_o, y_h, 16)
    s_gu = loc(guv, gu_o, 9)
    grad_blocks(att, mv, go_o, st, ssem, False, 0, att.shape[0] // 256)
    l_act.wait()
    l_gv.wait()
    l_gd.wait()
    s_gd = loc(gdv, gd_o.at[early], 10)
    grad_blocks(act, gv, gd_o, st, ssem, True, EARLY, EARLY + late, EARLY)
    for c in (s_y, s_gu, s_gd):
        c.wait()


def grads_call(dqkv, att, mid, ynear, yr, a_all, m_all, act, g_all, gu, gd):
    D = a_all.shape[1]
    H = pl.BlockSpec(memory_space=pl.ANY)
    sd = jax.ShapeDtypeStruct
    full = pltpu.VMEM(a_all.shape, BF)
    rows = dqkv.shape[0] + att.shape[0]
    return pl.pallas_call(
        grads_kernel,
        in_specs=[H] * 11,
        out_specs=[H] * 5,
        out_shape=[sd(mid.shape, BF), sd((dqkv.shape[0], D), BF), sd((att.shape[0], D), BF), sd(gd.shape, BF), sd(gu.shape, BF)],
        scratch_shapes=[pltpu.VMEM(v.shape, BF) for v in (dqkv, att, mid, mid, mid, mid)] + [full, full, pltpu.VMEM(act.shape, BF), full, pltpu.VMEM(gu.shape, BF), pltpu.VMEM((EARLY * 256, D), BF), pltpu.VMEM((2, 256, D), BF),
                        pltpu.SemaphoreType.DMA((17,)), pltpu.SemaphoreType.DMA((2,))],
        name="grads",
        cost_estimate=pl.CostEstimate(flops=3 * rows * D * a_all.shape[0], bytes_accessed=60 << 20, transcendentals=0),
        compiler_params=pltpu.CompilerParams(vmem_limit_bytes=66900000),
    )(dqkv, att, mid, ynear, yr, a_all, m_all, act, g_all, gu, gd)


def tail_kernel(x_ref, g_ref, hn, hr, m_ref, dg2_ref, dx_o, dg_o):
    da = (hn[...].astype(F32) + hr[...].astype(F32)).astype(BF).astype(F32)
    h, rstd = norm_stats(x_ref[...].astype(F32))
    v = da * row_of(g_ref)
    dx = rstd * (v - jnp.mean(v, **ROWS) - h * jnp.mean(v * h, **ROWS))
    dx_o[...] = (m_ref[...].astype(F32) + dx).astype(BF)
    s = jnp.sum(da * h, **COLS)
    i = pl.program_id(0)

    @pl.when(i == 0)
    def _():
        dg_o[...] = jnp.concatenate([s, dg2_ref[...]], 0)

    @pl.when(i > 0)
    def _():
        dg_o[0:1, :] += s


def tail_call(x, g1, hn, hr, m_all, dg2):
    n, D = x.shape
    blk = pl.BlockSpec((128, D), lambda i: (i, 0))
    whole = lambda r: pl.BlockSpec((r, D), lambda i: (0, 0))
    sd = jax.ShapeDtypeStruct
    return pl.pallas_call(
        tail_kernel, grid=(n // 128,),
        in_specs=[blk, pl.BlockSpec((D,), lambda i: (0,))] + [blk] * 3 + [whole(1)],
        out_specs=[blk, whole(2)],
        out_shape=[sd((n, D), BF), sd((2, D), F32)],
        name="tail",
        cost_estimate=pl.CostEstimate(flops=20 * n * D, bytes_accessed=14 * n * D, transcendentals=n),
    )(x, g1, hn, hr, m_all, dg2)


def swap(v, k):
    return lax.ppermute(v, 'model', [(i, i ^ k) for i in range(4)])


def local_layer(hidden_in, seg_ids, gain_attn, w_qkv, w_out, gain_mlp, w_up, w_down, grad_out):
    hidden, nh, _, dh = w_qkv.shape
    wt = w_qkv.transpose(1, 2, 3, 0).reshape(nh * 3 * dh, hidden)
    wo = w_out.reshape(nh * dh, hidden)
    x = hidden_in[0]
    d_g2, lse, mid, qkv, att, ysum, ynear, a_all, g_all, act, m_all, gw_up, gw_down = front_call(x, gain_attn, gain_mlp, seg_ids, wt, wo, w_up, w_down, grad_out[0], nh)
    yr, hx, hn, dqkv = back_call(seg_ids, qkv, att, lse, ysum, wt, wo, m_all)
    hr = swap(hx, 2)
    y, gq, go, gw_down, gw_up = grads_call(dqkv, att, mid, ynear, yr, a_all, m_all, act, g_all, gw_up, gw_down)
    hr, y, gq, go, gw_down, gw_up = lax.optimization_barrier((hr, y, gq, go, gw_down, gw_up))
    dx, dg = tail_call(x, gain_attn, hn, hr, m_all, d_g2)
    others = [swap(dg, k) for k in (2, 3, 1)]
    dg = ((dg + others[2]) + (others[0] + others[1])).astype(BF)
    gq = gq.reshape(nh, 3, dh, hidden).transpose(3, 0, 1, 2)
    return y[None], dx[None], gq, go.reshape(nh, dh, hidden), gw_up, gw_down, dg[0], dg[1]


def solution(mesh):
    act_spec = P('data', 'model', None)
    in_specs = (act_spec, P('data', None), P(), P(None, 'model', None, None), P('model', None, None), P(), P(None, 'model'), P('model', None), act_spec)
    out_specs = (act_spec, act_spec, P('data', 'model', None, None), P(('data', 'model'), None, None), P('data', 'model'), P(('data', 'model'), None), P('data'), P('data'))
    return jax.shard_map(local_layer, mesh=mesh, in_specs=in_specs, out_specs=out_specs, check_vma=False)
```

```python
import functools
import jax, jax.numpy as jnp
from jax import lax
from jax.experimental import pallas as pl
from jax.experimental.pallas import tpu as pltpu
from jax.sharding import PartitionSpec as P
BF=jnp.bfloat16; F32=jnp.float32
BLK=256

HALVES = range(2)
COLS = dict(axis=0, keepdims=True)
ROWS = dict(axis=-1, keepdims=True)


def half(s):
    return pl.ds(s * R, R)


def nn(a, b):
    return dotf(a, b, 1, 0)


def nt(a, b):
    return dotf(a, b, 1, 1)


def tn(a, b):
    return dotf(a, b, 0, 0)


def dotf(a,b,ca,cb):
    return lax.dot_general(a,b,(((ca,),(cb,)),((),())),preferred_element_type=F32)

LN_EPS = 1e-5
BIG = 1e30


def split3(v):
    hi = v.astype(BF)
    r = v - hi.astype(F32)
    md = r.astype(BF)
    return [hi, md, (r - md.astype(F32)).astype(BF)]


def attn_setup(segr, qside, kside, tri):
    S = segr.shape[1]
    seg = segr[...]
    pad = jnp.zeros((9, S), F32)
    one = jnp.ones((3, S), F32)
    hot = jnp.concatenate([(seg == d).astype(F32) for d in range(4)], 0)
    kside[...] = jnp.concatenate([hot, one, pad], 0)
    qside[...] = jnp.concatenate([(hot - 1.0) * BIG, 0.0 * one, pad], 0)
    kp = lax.broadcasted_iota(jnp.int32, (BLK, BLK), 0)
    qp = lax.broadcasted_iota(jnp.int32, (BLK, BLK), 1)
    tri[...] = jnp.where(kp <= qp, 0.0, -BIG)


def head_rows(h, dh, c):
    return pl.ds(pl.multiple_of(h * (3 * dh) + c * dh, dh), dh)


def causal(s, tri):
    n = s.shape[0]
    if n == BLK:
        return s + tri[...]
    return jnp.concatenate([s[:n - BLK], s[n - BLK:] + tri[...]], 0)


def attn_head_fwd(h, dh, qkv, qside, kside, tri, out, lse_ref):
    kt = jnp.concatenate([qkv[head_rows(h, dh, 1), :].astype(F32) * dh ** -0.5, kside[...]], 0)
    ka = kt.T.astype(BF)
    qa = jnp.concatenate([qkv[head_rows(h, dh, 0), :], qside[...].astype(BF)], 0)
    vr = head_rows(h, dh, 2)
    sc = {}

    def scores(a):
        sc[a] = nn(ka[:(a + 1) * BLK], qa[:, a * BLK:(a + 1) * BLK])
    scores(3)
    for a in range(3, -1, -1):
        ca, K = slice(a * BLK, (a + 1) * BLK), (a + 1) * BLK
        if a > 0:
            scores(a - 1)
        s = causal(sc[a], tri)
        m = jnp.max(s, **COLS)
        p = jnp.exp(s - m)
        l = jnp.sum(p, **COLS)
        o = nn(qkv[vr, 0:K], (p * (1.0 / l)).astype(BF))
        out[pl.ds(pl.multiple_of(h * dh, dh), dh), ca] = o.astype(BF)
        lse_ref[h, :, ca] = m + jnp.log(l)


def attn_head_bwd(h, dh, qkv, oall, doall, lse_ref, qside, kside, tri, gsc, dqkv):
    sc = dh ** -0.5
    S = qkv.shape[1]
    hr = pl.ds(pl.multiple_of(h * dh, dh), dh)
    kr, qr = head_rows(h, dh, 1), head_rows(h, dh, 0)
    ka = jnp.concatenate([qkv[kr, :].astype(F32) * sc, kside[...]], 0).T.astype(BF)
    one, pad = jnp.ones((3, S), F32), jnp.zeros((13, S), F32)
    va = jnp.concatenate([qkv[head_rows(h, dh, 2), :].astype(F32), one, pad], 0).T.astype(BF)
    do32 = doall[hr, :].astype(F32)
    delta = jnp.sum(do32 * oall[hr, :].astype(F32), **COLS)
    side = qside[...].astype(BF)
    qa = jnp.concatenate([qkv[qr, :], side[0:4]] + split3(-lse_ref[h]) + [side[7:16]], 0)
    da = jnp.concatenate([(do32 * sc).astype(BF)] + split3(-sc * delta) + [pad.astype(BF)], 0)
    sdp = {}

    def scores(a):
        ca, K = slice(a * BLK, (a + 1) * BLK), (a + 1) * BLK
        sdp[a] = nn(ka[:K], qa[:, ca]), nn(va[:K], da[:, ca])
    scores(3)
    for a in range(3, -1, -1):
        ca, K = slice(a * BLK, (a + 1) * BLK), (a + 1) * BLK
        q, do = qkv[qr, ca], doall[hr, ca]
        if a > 0:
            scores(a - 1)
        p = jnp.exp(causal(sdp[a][0], tri))
        ds = (p * sdp[a][1]).astype(BF)
        dqkv[qr, ca] = nn(qkv[kr, 0:K], ds).astype(BF)
        dk = nt(ds, q)
        dv = nt(p.astype(BF), do)
        if a == 3:
            gsc[0] = dk
            gsc[1] = dv
        else:
            gsc[0, 0:K] += dk
            gsc[1, 0:K] += dv
    dqkv[kr, :] = gsc[0].T.astype(BF)
    dqkv[head_rows(h, dh, 2), :] = gsc[1].T.astype(BF)


R = 128
MESH_ID = pl.DeviceIdType.MESH


def gelu_pair(z):
    c0, c1 = 0.7978845608028654, 0.044715
    z2 = z * z
    t = jnp.tanh(z * (c0 + (c0 * c1) * z2))
    h = 0.5 + 0.5 * t
    return z * h, h + (0.5 * z) * (1.0 - t * t) * (c0 + (3 * c0 * c1) * z2)


PAIR = 2
EARLY = 5


def partners():
    me = lax.axis_index('model')
    return me + 1 - 2 * lax.rem(me, 2), lax.rem(me + 2, 4)


def enter():
    core, chip = partners()
    sem = pltpu.get_barrier_semaphore()
    for dev in (core, chip):
        pl.semaphore_signal(sem, inc=1, device_id={'model': dev}, device_id_type=MESH_ID)
    pl.semaphore_wait(sem, 2)
    return core, chip


def grad_blocks(lhs, rhs, out, st, sem, across, first, last, base=0, drain=True):
    def sent(i):
        return pltpu.make_async_copy(st.at[lax.rem(i, 2)], out.at[block(i)], sem.at[lax.rem(i, 2)])

    def step(i, c):
        @pl.when(i >= base + 2)
        def _():
            sent(i - 2).wait()

        def body(q):
            v = tn(lhs[:, block(i)], rhs[:, q]) if across else nn(lhs[block(i), :], rhs[:, q])
            st[lax.rem(i, 2), :, q] = v.astype(BF)
        for j in range(rhs.shape[1] // 512):
            body(pl.ds(j * 512, 512))
        sent(i).start()
        return c
    lax.fori_loop(first, last, step, 0)
    if drain:
        sent(last - 2).wait()
        sent(last - 1).wait()


class Links:
    def __init__(self, send, recv):
        self.send, self.recv, self.n = send, recv, 0
        self.core, self.chip = partners()

    def copy(self, src, dst, dev):
        i = self.n
        self.n += 1
        return pltpu.make_async_remote_copy(src_ref=src, dst_ref=dst, send_sem=self.send.at[i], recv_sem=self.recv.at[i], device_id={'model': dev}, device_id_type=MESH_ID)

    def to_core(self, src, dst):
        return self.copy(src, dst, self.core)

    def to_chip(self, src, dst):
        return self.copy(src, dst, self.chip)


def tiles(n, size, body, together=1):
    def step(i, c):
        for j in range(together):
            body(pl.ds(pl.multiple_of((i * together + j) * size, size), size))
        return c
    lax.fori_loop(0, n // (size * together), step, 0)


def pairs(n, body):
    def step(i, c):
        for j in HALVES:
            body(i * 2 + j, j)
        return c
    lax.fori_loop(0, n // 2, step, 0)


def block(i, n=BLK):
    return pl.ds(pl.multiple_of(i * n, n), n)


def block_at(r):
    return pl.ds(r * BLK, BLK)


def row_of(g):
    return g[...].astype(F32).reshape(1, g.shape[0])


def norm_stats(v):
    mean = jnp.mean(v, **ROWS)
    c = v - mean
    rstd = lax.rsqrt(jnp.mean(c * c, **ROWS) + LN_EPS)
    return c * rstd, rstd


def positions():
    me = lax.axis_index('model')
    core, chip = partners()
    return me, core, chip, 3 - me


def front_kernel(dh, g1_ref, g2_ref, segr, x_h, wt_h, wo_h, wu_h, wd_h, gy_h, dg_o, lse, mid_h, qkv_h, att_h, ysum_h, ynear_h, a_h, g_h, act_h, m_h, gu_h, gd_h,
                 x_ref, mid_o, qkv, att, wo, wu, wd, gm, mb, bv, dgv, act, dz, acc, csf, csn, crf, crn, xs, xr, st, qside, kside, tri, lsem, osem, ssem, send, recv):
    D, F = wu.shape
    T = 512
    QW = qkv.shape[0]
    L = Links(send, recv)
    at = positions()

    def row(r, s):
        return (r // 2) * 512 + s * 256 + (r % 2) * R

    def lanes(r, s):
        return pl.ds(pl.multiple_of(at[r] * 256 + s * R, R), R)

    def loc(src, dst, i):
        return pltpu.make_async_copy(src, dst, lsem.at[i])
    l_g = [loc(gy_h.at[half(s)], gm.at[pl.ds(row(0, s), R)], s) for s in HALVES]
    l_wt = loc(wt_h, wu.at[pl.ds(0, QW)], 2)
    l_wo = loc(wo_h, wo, 3)
    l_wd = loc(wd_h, wd, 4)
    l_wu = loc(wu_h, wu, 5)
    l_x = [loc(x_h.at[half(s)], x_ref.at[half(s)], 6 + s) for s in HALVES]
    for c in l_x + l_g + [l_wt, l_wo, l_wd]:
        c.start()
    enter()

    def near(s):
        return pl.ds(row(0, s), R)

    def reduce_copies(cross=True):
        far = [L.to_core(csf.at[half(s)], crf.at[half(s)]) for s in HALVES]
        nr = [L.to_core(csn.at[half(s)], crn.at[half(s)]) for s in HALVES]
        return far, nr, [L.to_chip(xs.at[half(s)], xr.at[half(s)]) for s in HALVES] if cross else None

    def gather_copies(buf, first=0):
        skip = [first, 0]
        xc = [L.to_chip(buf.at[pl.ds(row(0, s) + skip[s], R - skip[s])], buf.at[pl.ds(row(2, s) + skip[s], R - skip[s])]) for s in HALVES]
        own = [L.to_core(buf.at[near(s)], buf.at[pl.ds(row(1, s), R)]) for s in HALVES]
        fwd = [L.to_core(buf.at[pl.ds(row(2, s), R)], buf.at[pl.ds(row(3, s), R)]) for s in HALVES]
        return xc, own, fwd

    pre = pl.ds(0, 32)
    e_pre = L.to_chip(gy_h.at[pre], gm.at[pl.ds(row(2, 0), 32)])
    e_pre.start()
    a_x, a_own, a_fwd = gather_copies(bv)
    e_x, e_own, e_fwd = gather_copies(gm, 32)
    b_far, b_near, b_x = reduce_copies()
    c_x, c_own, c_fwd = gather_copies(bv)
    f_far, f_near, f_x = reduce_copies()
    g_x, g_own, g_fwd = gather_copies(mb)

    def chip_sum(s, far, xc):
        far[s].wait_recv()
        rs = half(s)
        tiles(R, 32, lambda q: add_into(pl.ds(s * R + q.start, 32)))
        xc[s].start()

    def add_into(rs):
        xs[rs, :] = (xs[rs, :].astype(F32) + crf[rs, :].astype(F32)).astype(BF)

    outs = []

    def emit(src, dst, rr, s, base):
        for r in rr:
            c = pltpu.make_async_copy(src.at[pl.ds(row(r, s), R)], dst.at[pl.ds(r * 256 + s * R, R)], osem.at[base + 2 * r + s])
            c.start()
            outs.append(c)

    for s in HALVES:
        def norm1(q):
            h, _ = norm_stats(x_ref[pl.ds(s * R + q.start, 32), :].astype(F32))
            bv[pl.ds(row(0, s) + q.start, 32), :] = (h * row_of(g1_ref)).astype(BF)
        l_x[s].wait()
        tiles(R, 32, norm1)
        a_x[s].start()
        a_own[s].start()
    for s in HALVES:
        l_g[s].wait()
        e_x[s].start()
        e_own[s].start()
    attn_setup(segr, qside, kside, tri)
    l_wt.wait()

    def qkv_rows(o, r, s):
        def body(q):
            v = nt(wu[q, :], bv[o:o + 256, :]).astype(BF)
            qkv[q, lanes(r, s)] = v[:, :R]
            qkv[q, lanes(r + 1, s)] = v[:, R:]
        tiles(QW, T, body)
    for s in HALVES:
        a_own[s].wait_recv()
        qkv_rows(s * 256, 0, s)
    for s in HALVES:
        a_x[s].wait_recv()
        a_fwd[s].start()
        a_fwd[s].wait_recv()
        qkv_rows(512 + s * 256, 2, s)
    l_wu.start()
    a_out = [pltpu.make_async_copy(bv.at[pl.ds(row(r, s), R)], a_h.at[lanes(r, s)], osem.at[40 + 2 * r + s]) for r in range(4) for s in HALVES]
    for c in a_out:
        c.start()
    pairs(lse.shape[0], lambda h, j: attn_head_fwd(h, dh, qkv, qside, kside, tri, att, lse))
    late = []

    def put_out(src, dst):
        late.append(pltpu.make_async_copy(src, dst, osem.at[len(late)]))
        late[-1].start()
    put_out(qkv, qkv_h)
    put_out(att, att_h)
    e_pre.wait_recv()
    e_x[0].wait_recv()
    e_fwd[0].start()
    for c in a_out:
        c.wait()
    for c in a_x + a_own + a_fwd:
        c.wait_send()

    l_wo.wait()

    def out_part(pos, ref, rows=slice(None)):
        def body(q):
            ref[rows, q] = tn(att[:, pos], wo[:, q]).astype(ref.dtype)
        tiles(D, T, body, PAIR)

    def whole(r):
        return block(at[r])

    for s in HALVES:
        out_part(lanes(3, s), csf, half(s))
        b_far[s].start()
    for s in HALVES:
        out_part(lanes(2, s), xs, half(s))
        chip_sum(s, b_far, b_x)
    e_x[1].wait_recv()
    e_fwd[1].start()
    out_part(whole(1), csn)
    for s in HALVES:
        b_near[s].start()
    out_part(whole(0), acc)

    l_wd.wait()

    for s in HALVES:
        e_own[s].wait_recv()
        e_fwd[s].wait_recv()
        emit(gm, g_h, (0, 1, 2, 3), s, 32)

    def dact(i, c):
        def body(q):
            dgv[block(i), q] = nt(gm[pl.ds(pl.multiple_of(512 + i * 256, 256), 256), :], wd[q, :])
        tiles(F, T, body, PAIR)
        return c
    lax.fori_loop(0, 2, dact, 0)
    g_out = list(outs)
    outs.clear()
    l_wu.wait()
    for c in [e_pre] + e_x + e_own + e_fwd:
        c.wait_send()

    def total(rs):
        return acc[rs, :] + crn[rs, :].astype(F32) + xr[rs, :].astype(F32)

    def norm2(s):
        b_near[s].wait_recv()
        b_x[s].wait_recv()

        def body(q):
            rs = pl.ds(s * R + q.start, 32)
            att = total(rs).astype(BF).astype(F32)
            mid = (x_ref[rs, :].astype(F32) + att).astype(BF)
            mid_o[rs, :] = mid
            h, _ = norm_stats(mid.astype(F32))
            bv[pl.ds(row(0, s) + q.start, 32), :] = (h * row_of(g2_ref)).astype(BF)
        tiles(R, 32, body)
        c_x[s].start()
        c_own[s].start()

    def mlp(o):
        def body(q):
            g, d = gelu_pair(nn(bv[o:o + 256, :], wu[:, q]))
            act[o:o + 256, q] = g.astype(BF)
            up = dgv[o - 512:o - 256, q] if o >= 512 else nt(gm[o:o + 256, :], wd[q, :])
            dz[o:o + 256, q] = (d * up).astype(BF)
        tiles(F, T, body, PAIR)

    def dmlp(o, s, keep, give):
        def body(q):
            v = nt(dz[o:o + 256, :], wu[q, :])
            keep[half(s), q] = v[:R].astype(keep.dtype)
            give[half(s), q] = v[R:].astype(BF)
        tiles(D, T, body, PAIR)

    def ydown(base, keep, give):
        def chunk(s, c):
            o = pl.ds(pl.multiple_of(base + s * 256, 256), 256)
            rs = block(s, R)

            def body(q):
                v = nn(act[o, :], wd[:, q])
                keep[rs, q] = v[:R].astype(keep.dtype)
                give[rs, q] = v[R:].astype(BF)
            tiles(D, T, body, PAIR)
            return c
        lax.fori_loop(0, 2, chunk, 0)

    def near_step(s):
        c_own[s].wait_recv()
        mlp(s * 256)
        b_near[s].wait_send()
        dmlp(s * 256, s, acc, csn)
        f_near[s].start()
        emit(act, act_h, (0, 1), s, 8)

    norm2(0)
    for c in g_out:
        c.wait()
    near_step(0)
    norm2(1)
    put_out(mid_o, mid_h)
    near_step(1)

    def far_step(s):
        c_fwd[s].wait_recv()
        mlp(512 + s * 256)
        b_far[s].wait_send()
        b_x[s].wait_send()
        dmlp(512 + s * 256, s, xs, csf)
        f_far[s].start()
        emit(act, act_h, (2, 3), s, 8)

    c_x[0].wait_recv()
    c_fwd[0].start()
    far_step(0)
    chip_sum(0, f_far, f_x)
    c_x[1].wait_recv()
    c_fwd[1].start()
    far_step(1)
    chip_sum(1, f_far, f_x)
    def dnorm2(s):
        f_near[s].wait_recv()
        f_x[s].wait_recv()

        def step(i, dgain):
            rs = pl.ds(pl.multiple_of(s * R + i * 32, 32), 32)
            db = total(rs).astype(BF).astype(F32)
            h, rstd = norm_stats(mid_o[rs, :].astype(F32))
            v = db * row_of(g2_ref)
            dm = rstd * (v - jnp.mean(v, **ROWS) - h * jnp.mean(v * h, **ROWS))
            gr = pl.ds(pl.multiple_of(row(0, s) + i * 32, 32), 32)
            mb[gr, :] = (gm[gr, :].astype(F32) + dm).astype(BF)
            return dgain + jnp.sum(db * h, **COLS)
        dgain = lax.fori_loop(0, R // 32, step, jnp.zeros((1, D), F32))
        if s == 0:
            dg_o[...] = dgain
        else:
            dg_o[...] += dgain
        g_x[s].start()
        g_own[s].start()

    def up_blocks(first, last, drain=False):
        grad_blocks(bv, dz, gu_h, st, ssem, True, first, last, drain=drain)

    dnorm2(0)
    up_blocks(0, F // 256 - 1)
    dnorm2(1)
    y_far, y_near = reduce_copies(False)[:2]
    for s in HALVES:
        g_own[s].wait_recv()
        emit(mb, m_h, (0, 1), s, 24)
        f_far[s].wait_send()
        f_x[s].wait_send()
        f_near[s].wait_send()
    ydown(512, xs, csf)
    for c in y_far:
        c.start()
    ydown(0, acc, csn)
    for c in y_near:
        c.start()
    g_x[0].wait_recv()
    g_fwd[0].start()
    up_blocks(F // 256 - 1, F // 256, True)
    for s in HALVES:
        y_far[s].wait_recv()
        y_near[s].wait_recv()

    def ysum(q):
        xs[q, :] = (xs[q, :].astype(F32) + crf[q, :].astype(F32)).astype(BF)
        crn[q, :] = (acc[q, :] + crn[q, :].astype(F32)).astype(BF)
    tiles(256, 32, ysum)
    put_out(xs, ysum_h)
    put_out(crn, ynear_h)
    grad_blocks(act, gm, gd_h, st, ssem, True, 0, EARLY - 1, drain=False)
    g_x[1].wait_recv()
    g_fwd[1].start()
    g_fwd[0].wait_recv()
    emit(mb, m_h, (2, 3), 0, 24)
    grad_blocks(act, gm, gd_h, st, ssem, True, EARLY - 1, EARLY)
    g_fwd[1].wait_recv()
    emit(mb, m_h, (2, 3), 1, 24)
    for c in outs + late:
        c.wait()
    for c in y_far + y_near + c_x + c_own + c_fwd + g_x + g_own + g_fwd:
        c.wait_send()


def front_call(x, g1, g2, segr, wt, wo, wu, wd, gy, nh):
    D = x.shape[1]
    F = wu.shape[1]
    S = 4 * x.shape[0]
    dh = wo.shape[0] // nh
    V = pl.BlockSpec(memory_space=pltpu.VMEM)
    H = pl.BlockSpec(memory_space=pl.ANY)
    sd = jax.ShapeDtypeStruct
    full = pltpu.VMEM((S, D), BF)
    quarter = pltpu.VMEM((256, D), BF)
    return pl.pallas_call(
        functools.partial(front_kernel, dh),
        in_specs=[V] * 3 + [H] * 6,
        out_specs=[V] * 2 + [H] * 11,
        out_shape=[sd((1, D), F32), sd((nh, 1, S), F32), sd(x.shape, BF), sd(wt.shape[:1] + (S,), BF), sd((nh * dh, S), BF), sd(x.shape, BF), sd(x.shape, BF),
                   sd((S, D), BF), sd((S, D), BF), sd((S, F), BF), sd((S, D), BF), sd(wu.shape, BF), sd(wd.shape, BF)],
        scratch_shapes=[quarter, quarter, pltpu.VMEM(wt.shape[:1] + (S,), BF), pltpu.VMEM((nh * dh, S), BF), pltpu.VMEM(wo.shape, BF), pltpu.VMEM(wu.shape, BF), pltpu.VMEM(wd.shape, BF), full, full, full,
                        pltpu.VMEM((S // 2, F), F32), pltpu.VMEM((S, F), BF), pltpu.VMEM((S, F), BF), pltpu.VMEM((256, D), F32)]
        + [quarter] * 6 + [pltpu.VMEM((2, 256, F), BF), pltpu.VMEM((16, S), F32), pltpu.VMEM((16, S), F32), pltpu.VMEM((BLK, BLK), F32),
                           pltpu.SemaphoreType.DMA((8,)), pltpu.SemaphoreType.DMA((48,)),
                           pltpu.SemaphoreType.DMA((8,)), pltpu.SemaphoreType.DMA((43,)), pltpu.SemaphoreType.DMA((43,))],
        name="front",
        cost_estimate=pl.CostEstimate(flops=int(8e10), bytes_accessed=60 << 20, transcendentals=S * F),
        compiler_params=pltpu.CompilerParams(collective_id=0, has_side_effects=True, vmem_limit_bytes=66900000),
    )(g1, g2, segr, x, wt, wo, wu, wd, gy)


def back_kernel(dh, segr, lse, qkv_h, att_h, ysum, wt_h, wo_h, m_h, yr_o, hx_h, hn_h, dqkv_h,
                qkv, att, dqkv, hx_o, hn_o, wt, wo, mv, doall, gsc, csf, csn, crf, crn, qside, kside, tri, lsem, send, recv):
    D = wt.shape[1]
    T = 512
    nh = lse.shape[0]
    L = Links(send, recv)
    at = positions()

    def lanes(r, s):
        return pl.ds(pl.multiple_of(at[r] * 256 + s * R, R), R)

    def loc(src, dst, i):
        c = pltpu.make_async_copy(src, dst, lsem.at[i])
        c.start()
        return c
    l_wo = loc(wo_h, wo, 0)
    l_m = [loc(m_h.at[block_at(r)], mv.at[block_at(r)], 1 + r) for r in range(4)]
    enter()
    l_qkv = loc(qkv_h, qkv, 6)
    l_att = loc(att_h, att, 7)
    y_x = L.to_chip(ysum, yr_o)
    y_x.start()
    h_far = L.to_core(csf, crf)
    h_near = L.to_core(csn, crn)
    attn_setup(segr, qside, kside, tri)
    l_wo.wait()

    def dout(r, c):
        pltpu.make_async_copy(m_h.at[block(r)], mv.at[block(r)], lsem.at[1 + r]).wait()
        me = lax.axis_index('model')
        pos = 2 * lax.rem(me // 2 + r // 2, 2) + lax.rem(me + r, 2)
        doall[:, block(pos)] = nt(wo[...], mv[block(r), :]).astype(BF)
        return c
    lax.fori_loop(0, len(l_m), dout, 0)
    l_wt = loc(wt_h, wt, 5)
    l_qkv.wait()
    l_att.wait()
    pairs(nh, lambda h, j: attn_head_bwd(h, dh, qkv, att, doall, lse, qside, kside, tri, gsc.at[j], dqkv))
    o_dqkv = loc(dqkv, dqkv_h, 8)
    l_wt.wait()

    def parts(far, near, to_far, to_near):
        rows = [block(at[r]) for r in (far, near)]

        def body(q):
            v = tn(jnp.concatenate([dqkv[:, w] for w in rows], 1), wt[:, q])
            to_far[:, q] = v[:256].astype(to_far.dtype)
            to_near[:, q] = v[256:].astype(to_near.dtype)
        tiles(D, T, body)

    def add_into(ref, got):
        def body(q):
            ref[q, :] = (ref[q, :].astype(F32) + got[q, :].astype(F32)).astype(ref.dtype)
        tiles(256, 32, body)

    parts(3, 1, csf, csn)
    h_far.start()
    h_near.start()
    parts(2, 0, hx_o, hn_o)
    h_far.wait_recv()
    add_into(hx_o, crf)
    o_hx = loc(hx_o, hx_h, 9)
    h_near.wait_recv()
    add_into(hn_o, crn)
    o_hn = loc(hn_o, hn_h, 10)
    for c in (o_dqkv, o_hx, o_hn):
        c.wait()
    y_x.wait_recv()
    for c in (y_x, h_far, h_near):
        c.wait_send()


def back_call(segr, qkv, att, lse, ysum, wt, wo, m_all):
    S, D = m_all.shape
    nh = lse.shape[0]
    dh = wo.shape[0] // nh
    V = pl.BlockSpec(memory_space=pltpu.VMEM)
    H = pl.BlockSpec(memory_space=pl.ANY)
    sd = jax.ShapeDtypeStruct
    quarter = pltpu.VMEM((256, D), BF)
    return pl.pallas_call(
        functools.partial(back_kernel, dh),
        in_specs=[V] * 2 + [H] * 6,
        out_specs=[H] * 4,
        out_shape=[sd(ysum.shape, BF), sd(ysum.shape, BF), sd(ysum.shape, BF), sd(qkv.shape, BF)],
        scratch_shapes=[pltpu.VMEM(qkv.shape, BF), pltpu.VMEM(att.shape, BF), pltpu.VMEM(qkv.shape, BF), quarter, quarter,
                        pltpu.VMEM(wt.shape, BF), pltpu.VMEM(wo.shape, BF), pltpu.VMEM((S, D), BF),
                        pltpu.VMEM(att.shape, BF), pltpu.VMEM((2, 2, S, dh), F32)]
        + [quarter] * 4 + [pltpu.VMEM((16, S), F32), pltpu.VMEM((16, S), F32), pltpu.VMEM((BLK, BLK), F32),
                           pltpu.SemaphoreType.DMA((11,)), pltpu.SemaphoreType.DMA((3,)), pltpu.SemaphoreType.DMA((3,))],
        name="back",
        cost_estimate=pl.CostEstimate(flops=int(3e10), bytes_accessed=30 << 20, transcendentals=nh * S * S // 2),
        compiler_params=pltpu.CompilerParams(collective_id=1, has_side_effects=True, vmem_limit_bytes=66900000),
    )(segr, lse, qkv, att, ysum, wt, wo, m_all)


def grads_kernel(dqkv_h, att_h, mid_h, ynear_h, yr_h, a_h, m_h, act_h, g_h, gu_h, gd_h, y_h, gq_o, go_o, gd_o, gu_o, dqkv, att, mid_ref, ynear, yr, y_o, av, mv, act, gv, guv, gdv, st, lsem, ssem):
    at = positions()
    early = pl.ds(0, EARLY * 256)
    late = (act.shape[1] // 256) - EARLY

    def loc(src, dst, i):
        c = pltpu.make_async_copy(src, dst, lsem.at[i])
        c.start()
        return c
    l_a = loc(a_h, av, 0)
    l_dqkv = loc(dqkv_h, dqkv, 11)
    l_m = [loc(m_h.at[block_at(r)], mv.at[block(at[r])], 1 + r) for r in range(4)]
    l_att = loc(att_h, att, 12)
    l_y = [loc(p, q, 13 + i) for i, (p, q) in enumerate(((mid_h, mid_ref), (ynear_h, ynear), (yr_h, yr)))]
    l_act = loc(act_h, act, 5)
    l_gv = loc(g_h, gv, 6)
    l_gu = loc(gu_h, guv, 7)
    l_gd = loc(gd_h.at[early], gdv, 8)

    def yout(q):
        v = ynear[q, :].astype(F32) + yr[q, :].astype(F32)
        y_o[q, :] = (mid_ref[q, :].astype(F32) + v.astype(BF).astype(F32)).astype(BF)
    l_a.wait()
    l_dqkv.wait()
    grad_blocks(dqkv, av, gq_o, st, ssem, False, 0, dqkv.shape[0] // 256)
    for c in l_m + l_y + [l_att, l_gu]:
        c.wait()
    tiles(256, 32, yout)
    s_y = loc(y_o, y_h, 16)
    s_gu = loc(guv, gu_o, 9)
    grad_blocks(att, mv, go_o, st, ssem, False, 0, att.shape[0] // 256)
    l_act.wait()
    l_gv.wait()
    l_gd.wait()
    s_gd = loc(gdv, gd_o.at[early], 10)
    grad_blocks(act, gv, gd_o, st, ssem, True, EARLY, EARLY + late, EARLY)
    for c in (s_y, s_gu, s_gd):
        c.wait()


def grads_call(dqkv, att, mid, ynear, yr, a_all, m_all, act, g_all, gu, gd):
    D = a_all.shape[1]
    H = pl.BlockSpec(memory_space=pl.ANY)
    sd = jax.ShapeDtypeStruct
    full = pltpu.VMEM(a_all.shape, BF)
    rows = dqkv.shape[0] + att.shape[0]
    return pl.pallas_call(
        grads_kernel,
        in_specs=[H] * 11,
        out_specs=[H] * 5,
        out_shape=[sd(mid.shape, BF), sd((dqkv.shape[0], D), BF), sd((att.shape[0], D), BF), sd(gd.shape, BF), sd(gu.shape, BF)],
        scratch_shapes=[pltpu.VMEM(v.shape, BF) for v in (dqkv, att, mid, mid, mid, mid)] + [full, full, pltpu.VMEM(act.shape, BF), full, pltpu.VMEM(gu.shape, BF), pltpu.VMEM((EARLY * 256, D), BF), pltpu.VMEM((2, 256, D), BF),
                        pltpu.SemaphoreType.DMA((17,)), pltpu.SemaphoreType.DMA((2,))],
        name="grads",
        cost_estimate=pl.CostEstimate(flops=3 * rows * D * a_all.shape[0], bytes_accessed=60 << 20, transcendentals=0),
        compiler_params=pltpu.CompilerParams(vmem_limit_bytes=66900000),
    )(dqkv, att, mid, ynear, yr, a_all, m_all, act, g_all, gu, gd)


def tail_kernel(x_ref, g_ref, hn, hr, m_ref, dg2_ref, dx_o, dg_o):
    da = (hn[...].astype(F32) + hr[...].astype(F32)).astype(BF).astype(F32)
    h, rstd = norm_stats(x_ref[...].astype(F32))
    v = da * row_of(g_ref)
    dx = rstd * (v - jnp.mean(v, **ROWS) - h * jnp.mean(v * h, **ROWS))
    dx_o[...] = (m_ref[...].astype(F32) + dx).astype(BF)
    s = jnp.sum(da * h, **COLS)
    i = pl.program_id(0)

    @pl.when(i == 0)
    def _():
        dg_o[...] = jnp.concatenate([s, dg2_ref[...]], 0)

    @pl.when(i > 0)
    def _():
        dg_o[0:1, :] += s


def tail_call(x, g1, hn, hr, m_all, dg2):
    n, D = x.shape
    blk = pl.BlockSpec((128, D), lambda i: (i, 0))
    whole = lambda r: pl.BlockSpec((r, D), lambda i: (0, 0))
    sd = jax.ShapeDtypeStruct
    return pl.pallas_call(
        tail_kernel, grid=(n // 128,),
        in_specs=[blk, pl.BlockSpec((D,), lambda i: (0,))] + [blk] * 3 + [whole(1)],
        out_specs=[blk, whole(2)],
        out_shape=[sd((n, D), BF), sd((2, D), F32)],
        name="tail",
        cost_estimate=pl.CostEstimate(flops=20 * n * D, bytes_accessed=14 * n * D, transcendentals=n),
    )(x, g1, hn, hr, m_all, dg2)


def swap(v, k):
    return lax.ppermute(v, 'model', [(i, i ^ k) for i in range(4)])


def local_layer(hidden_in, seg_ids, gain_attn, w_qkv, w_out, gain_mlp, w_up, w_down, grad_out):
    hidden, nh, _, dh = w_qkv.shape
    wt = w_qkv.transpose(1, 2, 3, 0).reshape(nh * 3 * dh, hidden)
    wo = w_out.reshape(nh * dh, hidden)
    x = hidden_in[0]
    d_g2, lse, mid, qkv, att, ysum, ynear, a_all, g_all, act, m_all, gw_up, gw_down = front_call(x, gain_attn, gain_mlp, seg_ids, wt, wo, w_up, w_down, grad_out[0], nh)
    yr, hx, hn, dqkv = back_call(seg_ids, qkv, att, lse, ysum, wt, wo, m_all)
    hr = swap(hx, 2)
    y, gq, go, gw_down, gw_up = grads_call(dqkv, att, mid, ynear, yr, a_all, m_all, act, g_all, gw_up, gw_down)
    hr, y, gq, go, gw_down, gw_up = lax.optimization_barrier((hr, y, gq, go, gw_down, gw_up))
    dx, dg = tail_call(x, gain_attn, hn, hr, m_all, d_g2)
    others = [swap(dg, k) for k in (2, 3, 1)]
    dg = ((dg + others[2]) + (others[0] + others[1])).astype(BF)
    gq = gq.reshape(nh, 3, dh, hidden).transpose(3, 0, 1, 2)
    return y[None], dx[None], gq, go.reshape(nh, dh, hidden), gw_up, gw_down, dg[0], dg[1]


def solution(mesh):
    act_spec = P('data', 'model', None)
    in_specs = (act_spec, P('data', None), P(), P(None, 'model', None, None), P('model', None, None), P(), P(None, 'model'), P('model', None), act_spec)
    out_specs = (act_spec, act_spec, P('data', 'model', None, None), P(('data', 'model'), None, None), P('data', 'model'), P(('data', 'model'), None), P('data'), P('data'))
    return jax.shard_map(local_layer, mesh=mesh, in_specs=in_specs, out_specs=out_specs, check_vma=False)
```

```python
import functools
import jax, jax.numpy as jnp
from jax import lax
from jax.experimental import pallas as pl
from jax.experimental.pallas import tpu as pltpu
from jax.sharding import PartitionSpec as P
BF=jnp.bfloat16; F32=jnp.float32
BLK=256

HALVES = range(2)
COLS = dict(axis=0, keepdims=True)
ROWS = dict(axis=-1, keepdims=True)


def half(s):
    return pl.ds(s * R, R)


def nn(a, b):
    return dotf(a, b, 1, 0)


def nt(a, b):
    return dotf(a, b, 1, 1)


def tn(a, b):
    return dotf(a, b, 0, 0)


def dotf(a,b,ca,cb):
    return lax.dot_general(a,b,(((ca,),(cb,)),((),())),preferred_element_type=F32)

LN_EPS = 1e-5
BIG = 1e30


def split3(v):
    hi = v.astype(BF)
    r = v - hi.astype(F32)
    md = r.astype(BF)
    return [hi, md, (r - md.astype(F32)).astype(BF)]


def attn_setup(segr, qside, kside, tri):
    S = segr.shape[1]
    seg = segr[...]
    pad = jnp.zeros((9, S), F32)
    one = jnp.ones((3, S), F32)
    hot = jnp.concatenate([(seg == d).astype(F32) for d in range(4)], 0)
    kside[...] = jnp.concatenate([hot, one, pad], 0)
    qside[...] = jnp.concatenate([(hot - 1.0) * BIG, 0.0 * one, pad], 0)
    kp = lax.broadcasted_iota(jnp.int32, (BLK, BLK), 0)
    qp = lax.broadcasted_iota(jnp.int32, (BLK, BLK), 1)
    tri[...] = jnp.where(kp <= qp, 0.0, -BIG)


def head_rows(h, dh, c):
    return pl.ds(pl.multiple_of(h * (3 * dh) + c * dh, dh), dh)


def causal(s, tri):
    n = s.shape[0]
    if n == BLK:
        return s + tri[...]
    return jnp.concatenate([s[:n - BLK], s[n - BLK:] + tri[...]], 0)


def attn_head_fwd(h, dh, qkv, qside, kside, tri, out, lse_ref):
    kt = jnp.concatenate([qkv[head_rows(h, dh, 1), :].astype(F32) * dh ** -0.5, kside[...]], 0)
    ka = kt.T.astype(BF)
    qa = jnp.concatenate([qkv[head_rows(h, dh, 0), :], qside[...].astype(BF)], 0)
    vr = head_rows(h, dh, 2)
    sc = {}

    def scores(a):
        sc[a] = nn(ka[:(a + 1) * BLK], qa[:, a * BLK:(a + 1) * BLK])
    scores(3)
    for a in range(3, -1, -1):
        ca, K = slice(a * BLK, (a + 1) * BLK), (a + 1) * BLK
        if a > 0:
            scores(a - 1)
        s = causal(sc[a], tri)
        m = jnp.max(s, **COLS)
        p = jnp.exp(s - m)
        l = jnp.sum(p, **COLS)
        o = nn(qkv[vr, 0:K], (p * (1.0 / l)).astype(BF))
        out[pl.ds(pl.multiple_of(h * dh, dh), dh), ca] = o.astype(BF)
        lse_ref[h, :, ca] = m + jnp.log(l)


def attn_head_bwd(h, dh, qkv, oall, doall, lse_ref, qside, kside, tri, gsc, dqkv):
    sc = dh ** -0.5
    S = qkv.shape[1]
    hr = pl.ds(pl.multiple_of(h * dh, dh), dh)
    kr, qr = head_rows(h, dh, 1), head_rows(h, dh, 0)
    ka = jnp.concatenate([qkv[kr, :].astype(F32) * sc, kside[...]], 0).T.astype(BF)
    one, pad = jnp.ones((3, S), F32), jnp.zeros((13, S), F32)
    va = jnp.concatenate([qkv[head_rows(h, dh, 2), :].astype(F32), one, pad], 0).T.astype(BF)
    do32 = doall[hr, :].astype(F32)
    delta = jnp.sum(do32 * oall[hr, :].astype(F32), **COLS)
    side = qside[...].astype(BF)
    qa = jnp.concatenate([qkv[qr, :], side[0:4]] + split3(-lse_ref[h]) + [side[7:16]], 0)
    da = jnp.concatenate([(do32 * sc).astype(BF)] + split3(-sc * delta) + [pad.astype(BF)], 0)
    sdp = {}

    def scores(a):
        ca, K = slice(a * BLK, (a + 1) * BLK), (a + 1) * BLK
        sdp[a] = nn(ka[:K], qa[:, ca]), nn(va[:K], da[:, ca])
    scores(3)
    for a in range(3, -1, -1):
        ca, K = slice(a * BLK, (a + 1) * BLK), (a + 1) * BLK
        q, do = qkv[qr, ca], doall[hr, ca]
        if a > 0:
            scores(a - 1)
        p = jnp.exp(causal(sdp[a][0], tri))
        ds = (p * sdp[a][1]).astype(BF)
        dqkv[qr, ca] = nn(qkv[kr, 0:K], ds).astype(BF)
        dk = nt(ds, q)
        dv = nt(p.astype(BF), do)
        if a == 3:
            gsc[0] = dk
            gsc[1] = dv
        else:
            gsc[0, 0:K] += dk
            gsc[1, 0:K] += dv
    dqkv[kr, :] = gsc[0].T.astype(BF)
    dqkv[head_rows(h, dh, 2), :] = gsc[1].T.astype(BF)


R = 128
MESH_ID = pl.DeviceIdType.MESH


def gelu_pair(z):
    c0, c1 = 0.7978845608028654, 0.044715
    z2 = z * z
    t = jnp.tanh(z * (c0 + (c0 * c1) * z2))
    h = 0.5 + 0.5 * t
    return z * h, h + (0.5 * z) * (1.0 - t * t) * (c0 + (3 * c0 * c1) * z2)


PAIR = 2
EARLY = 5


def partners():
    me = lax.axis_index('model')
    return me + 1 - 2 * lax.rem(me, 2), lax.rem(me + 2, 4)


def enter():
    core, chip = partners()
    sem = pltpu.get_barrier_semaphore()
    for dev in (core, chip):
        pl.semaphore_signal(sem, inc=1, device_id={'model': dev}, device_id_type=MESH_ID)
    pl.semaphore_wait(sem, 2)
    return core, chip


def grad_blocks(lhs, rhs, out, st, sem, across, first, last, base=0, drain=True):
    def sent(i):
        return pltpu.make_async_copy(st.at[lax.rem(i, 2)], out.at[block(i)], sem.at[lax.rem(i, 2)])

    def step(i, c):
        @pl.when(i >= base + 2)
        def _():
            sent(i - 2).wait()

        def body(q):
            v = tn(lhs[:, block(i)], rhs[:, q]) if across else nn(lhs[block(i), :], rhs[:, q])
            st[lax.rem(i, 2), :, q] = v.astype(BF)
        for j in range(rhs.shape[1] // 512):
            body(pl.ds(j * 512, 512))
        sent(i).start()
        return c
    lax.fori_loop(first, last, step, 0)
    if drain:
        sent(last - 2).wait()
        sent(last - 1).wait()


class Links:
    def __init__(self, send, recv):
        self.send, self.recv, self.n = send, recv, 0
        self.core, self.chip = partners()

    def copy(self, src, dst, dev):
        i = self.n
        self.n += 1
        return pltpu.make_async_remote_copy(src_ref=src, dst_ref=dst, send_sem=self.send.at[i], recv_sem=self.recv.at[i], device_id={'model': dev}, device_id_type=MESH_ID)

    def to_core(self, src, dst):
        return self.copy(src, dst, self.core)

    def to_chip(self, src, dst):
        return self.copy(src, dst, self.chip)


def tiles(n, size, body, together=1):
    def step(i, c):
        for j in range(together):
            body(pl.ds(pl.multiple_of((i * together + j) * size, size), size))
        return c
    lax.fori_loop(0, n // (size * together), step, 0)


def pairs(n, body):
    def step(i, c):
        for j in HALVES:
            body(i * 2 + j, j)
        return c
    lax.fori_loop(0, n // 2, step, 0)


def block(i, n=BLK):
    return pl.ds(pl.multiple_of(i * n, n), n)


def block_at(r):
    return pl.ds(r * BLK, BLK)


def row_of(g):
    return g[...].astype(F32).reshape(1, g.shape[0])


def norm_stats(v):
    mean = jnp.mean(v, **ROWS)
    c = v - mean
    rstd = lax.rsqrt(jnp.mean(c * c, **ROWS) + LN_EPS)
    return c * rstd, rstd


def positions():
    me = lax.axis_index('model')
    core, chip = partners()
    return me, core, chip, 3 - me


def front_kernel(dh, g1_ref, g2_ref, segr, x_h, wt_h, wo_h, wu_h, wd_h, gy_h, dg_o, lse, mid_h, qkv_h, att_h, ysum_h, ynear_h, a_h, g_h, act_h, m_h, gu_h, gd_h,
                 x_ref, mid_o, qkv, att, wo, wu, wd, gm, mb, bv, dgv, act, dz, acc, csf, csn, crf, crn, xs, xr, st, qside, kside, tri, lsem, osem, ssem, send, recv):
    D, F = wu.shape
    T = 512
    QW = qkv.shape[0]
    L = Links(send, recv)
    at = positions()

    def row(r, s):
        return (r // 2) * 512 + s * 256 + (r % 2) * R

    def lanes(r, s):
        return pl.ds(pl.multiple_of(at[r] * 256 + s * R, R), R)

    def loc(src, dst, i):
        return pltpu.make_async_copy(src, dst, lsem.at[i])
    l_g = [loc(gy_h.at[half(s)], gm.at[pl.ds(row(0, s), R)], s) for s in HALVES]
    l_wt = loc(wt_h, wu.at[pl.ds(0, QW)], 2)
    l_wo = loc(wo_h, wo, 3)
    l_wd = loc(wd_h, wd, 4)
    l_wu = loc(wu_h, wu, 5)
    l_x = [loc(x_h.at[half(s)], x_ref.at[half(s)], 6 + s) for s in HALVES]
    for c in l_x + l_g + [l_wt, l_wo, l_wd]:
        c.start()
    enter()

    def near(s):
        return pl.ds(row(0, s), R)

    def reduce_copies(cross=True):
        far = [L.to_core(csf.at[half(s)], crf.at[half(s)]) for s in HALVES]
        nr = [L.to_core(csn.at[half(s)], crn.at[half(s)]) for s in HALVES]
        return far, nr, [L.to_chip(xs.at[half(s)], xr.at[half(s)]) for s in HALVES] if cross else None

    def gather_copies(buf, first=0):
        skip = [first, 0]
        xc = [L.to_chip(buf.at[pl.ds(row(0, s) + skip[s], R - skip[s])], buf.at[pl.ds(row(2, s) + skip[s], R - skip[s])]) for s in HALVES]
        own = [L.to_core(buf.at[near(s)], buf.at[pl.ds(row(1, s), R)]) for s in HALVES]
        fwd = [L.to_core(buf.at[pl.ds(row(2, s), R)], buf.at[pl.ds(row(3, s), R)]) for s in HALVES]
        return xc, own, fwd

    pre = pl.ds(0, 16)
    e_pre = L.to_chip(gy_h.at[pre], gm.at[pl.ds(row(2, 0), 16)])
    e_pre.start()
    a_x, a_own, a_fwd = gather_copies(bv)
    e_x, e_own, e_fwd = gather_copies(gm, 16)
    b_far, b_near, b_x = reduce_copies()
    c_x, c_own, c_fwd = gather_copies(bv)
    f_far, f_near, f_x = reduce_copies()
    g_x, g_own, g_fwd = gather_copies(mb)

    def chip_sum(s, far, xc):
        far[s].wait_recv()
        rs = half(s)
        tiles(R, 32, lambda q: add_into(pl.ds(s * R + q.start, 32)))
        xc[s].start()

    def add_into(rs):
        xs[rs, :] = (xs[rs, :].astype(F32) + crf[rs, :].astype(F32)).astype(BF)

    outs = []

    def emit(src, dst, rr, s, base):
        for r in rr:
            c = pltpu.make_async_copy(src.at[pl.ds(row(r, s), R)], dst.at[pl.ds(r * 256 + s * R, R)], osem.at[base + 2 * r + s])
            c.start()
            outs.append(c)

    for s in HALVES:
        def norm1(q):
            h, _ = norm_stats(x_ref[pl.ds(s * R + q.start, 32), :].astype(F32))
            bv[pl.ds(row(0, s) + q.start, 32), :] = (h * row_of(g1_ref)).astype(BF)
        l_x[s].wait()
        tiles(R, 32, norm1)
        a_x[s].start()
        a_own[s].start()
    for s in HALVES:
        l_g[s].wait()
        e_x[s].start()
        e_own[s].start()
    attn_setup(segr, qside, kside, tri)
    l_wt.wait()

    def qkv_rows(o, r, s):
        def body(q):
            v = nt(wu[q, :], bv[o:o + 256, :]).astype(BF)
            qkv[q, lanes(r, s)] = v[:, :R]
            qkv[q, lanes(r + 1, s)] = v[:, R:]
        tiles(QW, T, body)
    for s in HALVES:
        a_own[s].wait_recv()
        qkv_rows(s * 256, 0, s)
    for s in HALVES:
        a_x[s].wait_recv()
        a_fwd[s].start()
        a_fwd[s].wait_recv()
        qkv_rows(512 + s * 256, 2, s)
    l_wu.start()
    a_out = [pltpu.make_async_copy(bv.at[pl.ds(row(r, s), R)], a_h.at[lanes(r, s)], osem.at[40 + 2 * r + s]) for r in range(4) for s in HALVES]
    for c in a_out:
        c.start()
    pairs(lse.shape[0], lambda h, j: attn_head_fwd(h, dh, qkv, qside, kside, tri, att, lse))
    late = []

    def put_out(src, dst):
        late.append(pltpu.make_async_copy(src, dst, osem.at[len(late)]))
        late[-1].start()
    put_out(qkv, qkv_h)
    put_out(att, att_h)
    e_pre.wait_recv()
    e_x[0].wait_recv()
    e_fwd[0].start()
    for c in a_out:
        c.wait()
    for c in a_x + a_own + a_fwd:
        c.wait_send()

    l_wo.wait()

    def out_part(pos, ref, rows=slice(None)):
        def body(q):
            ref[rows, q] = tn(att[:, pos], wo[:, q]).astype(ref.dtype)
        tiles(D, T, body, PAIR)

    def whole(r):
        return block(at[r])

    for s in HALVES:
        out_part(lanes(3, s), csf, half(s))
        b_far[s].start()
    for s in HALVES:
        out_part(lanes(2, s), xs, half(s))
        chip_sum(s, b_far, b_x)
    e_x[1].wait_recv()
    e_fwd[1].start()
    out_part(whole(1), csn)
    for s in HALVES:
        b_near[s].start()
    out_part(whole(0), acc)

    l_wd.wait()

    for s in HALVES:
        e_own[s].wait_recv()
        e_fwd[s].wait_recv()
        emit(gm, g_h, (0, 1, 2, 3), s, 32)

    def dact(i, c):
        def body(q):
            dgv[block(i), q] = nt(gm[pl.ds(pl.multiple_of(512 + i * 256, 256), 256), :], wd[q, :])
        tiles(F, T, body, PAIR)
        return c
    lax.fori_loop(0, 2, dact, 0)
    g_out = list(outs)
    outs.clear()
    l_wu.wait()
    for c in [e_pre] + e_x + e_own + e_fwd:
        c.wait_send()

    def total(rs):
        return acc[rs, :] + crn[rs, :].astype(F32) + xr[rs, :].astype(F32)

    def norm2(s):
        b_near[s].wait_recv()
        b_x[s].wait_recv()

        def body(q):
            rs = pl.ds(s * R + q.start, 32)
            att = total(rs).astype(BF).astype(F32)
            mid = (x_ref[rs, :].astype(F32) + att).astype(BF)
            mid_o[rs, :] = mid
            h, _ = norm_stats(mid.astype(F32))
            bv[pl.ds(row(0, s) + q.start, 32), :] = (h * row_of(g2_ref)).astype(BF)
        tiles(R, 32, body)
        c_x[s].start()
        c_own[s].start()

    def mlp(o):
        def body(q):
            g, d = gelu_pair(nn(bv[o:o + 256, :], wu[:, q]))
            act[o:o + 256, q] = g.astype(BF)
            up = dgv[o - 512:o - 256, q] if o >= 512 else nt(gm[o:o + 256, :], wd[q, :])
            dz[o:o + 256, q] = (d * up).astype(BF)
        tiles(F, T, body, PAIR)

    def dmlp(o, s, keep, give):
        def body(q):
            v = nt(dz[o:o + 256, :], wu[q, :])
            keep[half(s), q] = v[:R].astype(keep.dtype)
            give[half(s), q] = v[R:].astype(BF)
        tiles(D, T, body, PAIR)

    def ydown(base, keep, give):
        def chunk(s, c):
            o = pl.ds(pl.multiple_of(base + s * 256, 256), 256)
            rs = block(s, R)

            def body(q):
                v = nn(act[o, :], wd[:, q])
                keep[rs, q] = v[:R].astype(keep.dtype)
                give[rs, q] = v[R:].astype(BF)
            tiles(D, T, body, PAIR)
            return c
        lax.fori_loop(0, 2, chunk, 0)

    def near_step(s):
        c_own[s].wait_recv()
        mlp(s * 256)
        b_near[s].wait_send()
        dmlp(s * 256, s, acc, csn)
        f_near[s].start()
        emit(act, act_h, (0, 1), s, 8)

    norm2(0)
    for c in g_out:
        c.wait()
    near_step(0)
    norm2(1)
    put_out(mid_o, mid_h)
    near_step(1)

    def far_step(s):
        c_fwd[s].wait_recv()
        mlp(512 + s * 256)
        b_far[s].wait_send()
        b_x[s].wait_send()
        dmlp(512 + s * 256, s, xs, csf)
        f_far[s].start()
        emit(act, act_h, (2, 3), s, 8)

    c_x[0].wait_recv()
    c_fwd[0].start()
    far_step(0)
    chip_sum(0, f_far, f_x)
    c_x[1].wait_recv()
    c_fwd[1].start()
    far_step(1)
    chip_sum(1, f_far, f_x)
    def dnorm2(s):
        f_near[s].wait_recv()
        f_x[s].wait_recv()

        def step(i, dgain):
            rs = pl.ds(pl.multiple_of(s * R + i * 32, 32), 32)
            db = total(rs).astype(BF).astype(F32)
            h, rstd = norm_stats(mid_o[rs, :].astype(F32))
            v = db * row_of(g2_ref)
            dm = rstd * (v - jnp.mean(v, **ROWS) - h * jnp.mean(v * h, **ROWS))
            gr = pl.ds(pl.multiple_of(row(0, s) + i * 32, 32), 32)
            mb[gr, :] = (gm[gr, :].astype(F32) + dm).astype(BF)
            return dgain + jnp.sum(db * h, **COLS)
        dgain = lax.fori_loop(0, R // 32, step, jnp.zeros((1, D), F32))
        if s == 0:
            dg_o[...] = dgain
        else:
            dg_o[...] += dgain
        g_x[s].start()
        g_own[s].start()

    def up_blocks(first, last, drain=False):
        grad_blocks(bv, dz, gu_h, st, ssem, True, first, last, drain=drain)

    dnorm2(0)
    up_blocks(0, F // 256 - 1)
    dnorm2(1)
    y_far, y_near = reduce_copies(False)[:2]
    for s in HALVES:
        g_own[s].wait_recv()
        emit(mb, m_h, (0, 1), s, 24)
        f_far[s].wait_send()
        f_x[s].wait_send()
        f_near[s].wait_send()
    ydown(512, xs, csf)
    for c in y_far:
        c.start()
    ydown(0, acc, csn)
    for c in y_near:
        c.start()
    g_x[0].wait_recv()
    g_fwd[0].start()
    up_blocks(F // 256 - 1, F // 256, True)
    for s in HALVES:
        y_far[s].wait_recv()
        y_near[s].wait_recv()

    def ysum(q):
        xs[q, :] = (xs[q, :].astype(F32) + crf[q, :].astype(F32)).astype(BF)
        crn[q, :] = (acc[q, :] + crn[q, :].astype(F32)).astype(BF)
    tiles(256, 32, ysum)
    put_out(xs, ysum_h)
    put_out(crn, ynear_h)
    grad_blocks(act, gm, gd_h, st, ssem, True, 0, EARLY - 1, drain=False)
    g_x[1].wait_recv()
    g_fwd[1].start()
    g_fwd[0].wait_recv()
    emit(mb, m_h, (2, 3), 0, 24)
    grad_blocks(act, gm, gd_h, st, ssem, True, EARLY - 1, EARLY)
    g_fwd[1].wait_recv()
    emit(mb, m_h, (2, 3), 1, 24)
    for c in outs + late:
        c.wait()
    for c in y_far + y_near + c_x + c_own + c_fwd + g_x + g_own + g_fwd:
        c.wait_send()


def front_call(x, g1, g2, segr, wt, wo, wu, wd, gy, nh):
    D = x.shape[1]
    F = wu.shape[1]
    S = 4 * x.shape[0]
    dh = wo.shape[0] // nh
    V = pl.BlockSpec(memory_space=pltpu.VMEM)
    H = pl.BlockSpec(memory_space=pl.ANY)
    sd = jax.ShapeDtypeStruct
    full = pltpu.VMEM((S, D), BF)
    quarter = pltpu.VMEM((256, D), BF)
    return pl.pallas_call(
        functools.partial(front_kernel, dh),
        in_specs=[V] * 3 + [H] * 6,
        out_specs=[V] * 2 + [H] * 11,
        out_shape=[sd((1, D), F32), sd((nh, 1, S), F32), sd(x.shape, BF), sd(wt.shape[:1] + (S,), BF), sd((nh * dh, S), BF), sd(x.shape, BF), sd(x.shape, BF),
                   sd((S, D), BF), sd((S, D), BF), sd((S, F), BF), sd((S, D), BF), sd(wu.shape, BF), sd(wd.shape, BF)],
        scratch_shapes=[quarter, quarter, pltpu.VMEM(wt.shape[:1] + (S,), BF), pltpu.VMEM((nh * dh, S), BF), pltpu.VMEM(wo.shape, BF), pltpu.VMEM(wu.shape, BF), pltpu.VMEM(wd.shape, BF), full, full, full,
                        pltpu.VMEM((S // 2, F), F32), pltpu.VMEM((S, F), BF), pltpu.VMEM((S, F), BF), pltpu.VMEM((256, D), F32)]
        + [quarter] * 6 + [pltpu.VMEM((2, 256, F), BF), pltpu.VMEM((16, S), F32), pltpu.VMEM((16, S), F32), pltpu.VMEM((BLK, BLK), F32),
                           pltpu.SemaphoreType.DMA((8,)), pltpu.SemaphoreType.DMA((48,)),
                           pltpu.SemaphoreType.DMA((8,)), pltpu.SemaphoreType.DMA((43,)), pltpu.SemaphoreType.DMA((43,))],
        name="front",
        cost_estimate=pl.CostEstimate(flops=int(8e10), bytes_accessed=60 << 20, transcendentals=S * F),
        compiler_params=pltpu.CompilerParams(collective_id=0, has_side_effects=True, vmem_limit_bytes=66900000),
    )(g1, g2, segr, x, wt, wo, wu, wd, gy)


def back_kernel(dh, segr, lse, qkv_h, att_h, ysum, wt_h, wo_h, m_h, yr_o, hx_h, hn_h, dqkv_h,
                qkv, att, dqkv, hx_o, hn_o, wt, wo, mv, doall, gsc, csf, csn, crf, crn, qside, kside, tri, lsem, send, recv):
    D = wt.shape[1]
    T = 512
    nh = lse.shape[0]
    L = Links(send, recv)
    at = positions()

    def lanes(r, s):
        return pl.ds(pl.multiple_of(at[r] * 256 + s * R, R), R)

    def loc(src, dst, i):
        c = pltpu.make_async_copy(src, dst, lsem.at[i])
        c.start()
        return c
    l_wo = loc(wo_h, wo, 0)
    l_m = [loc(m_h.at[block_at(r)], mv.at[block_at(r)], 1 + r) for r in range(4)]
    enter()
    l_qkv = loc(qkv_h, qkv, 6)
    l_att = loc(att_h, att, 7)
    y_x = L.to_chip(ysum, yr_o)
    y_x.start()
    h_far = L.to_core(csf, crf)
    h_near = L.to_core(csn, crn)
    attn_setup(segr, qside, kside, tri)
    l_wo.wait()

    def dout(r, c):
        pltpu.make_async_copy(m_h.at[block(r)], mv.at[block(r)], lsem.at[1 + r]).wait()
        me = lax.axis_index('model')
        pos = 2 * lax.rem(me // 2 + r // 2, 2) + lax.rem(me + r, 2)
        doall[:, block(pos)] = nt(wo[...], mv[block(r), :]).astype(BF)
        return c
    lax.fori_loop(0, len(l_m), dout, 0)
    l_wt = loc(wt_h, wt, 5)
    l_qkv.wait()
    l_att.wait()
    pairs(nh, lambda h, j: attn_head_bwd(h, dh, qkv, att, doall, lse, qside, kside, tri, gsc.at[j], dqkv))
    o_dqkv = loc(dqkv, dqkv_h, 8)
    l_wt.wait()

    def parts(far, near, to_far, to_near):
        rows = [block(at[r]) for r in (far, near)]

        def body(q):
            v = tn(jnp.concatenate([dqkv[:, w] for w in rows], 1), wt[:, q])
            to_far[:, q] = v[:256].astype(to_far.dtype)
            to_near[:, q] = v[256:].astype(to_near.dtype)
        tiles(D, T, body)

    def add_into(ref, got):
        def body(q):
            ref[q, :] = (ref[q, :].astype(F32) + got[q, :].astype(F32)).astype(ref.dtype)
        tiles(256, 32, body)

    parts(3, 1, csf, csn)
    h_far.start()
    h_near.start()
    parts(2, 0, hx_o, hn_o)
    h_far.wait_recv()
    add_into(hx_o, crf)
    o_hx = loc(hx_o, hx_h, 9)
    h_near.wait_recv()
    add_into(hn_o, crn)
    o_hn = loc(hn_o, hn_h, 10)
    for c in (o_dqkv, o_hx, o_hn):
        c.wait()
    y_x.wait_recv()
    for c in (y_x, h_far, h_near):
        c.wait_send()


def back_call(segr, qkv, att, lse, ysum, wt, wo, m_all):
    S, D = m_all.shape
    nh = lse.shape[0]
    dh = wo.shape[0] // nh
    V = pl.BlockSpec(memory_space=pltpu.VMEM)
    H = pl.BlockSpec(memory_space=pl.ANY)
    sd = jax.ShapeDtypeStruct
    quarter = pltpu.VMEM((256, D), BF)
    return pl.pallas_call(
        functools.partial(back_kernel, dh),
        in_specs=[V] * 2 + [H] * 6,
        out_specs=[H] * 4,
        out_shape=[sd(ysum.shape, BF), sd(ysum.shape, BF), sd(ysum.shape, BF), sd(qkv.shape, BF)],
        scratch_shapes=[pltpu.VMEM(qkv.shape, BF), pltpu.VMEM(att.shape, BF), pltpu.VMEM(qkv.shape, BF), quarter, quarter,
                        pltpu.VMEM(wt.shape, BF), pltpu.VMEM(wo.shape, BF), pltpu.VMEM((S, D), BF),
                        pltpu.VMEM(att.shape, BF), pltpu.VMEM((2, 2, S, dh), F32)]
        + [quarter] * 4 + [pltpu.VMEM((16, S), F32), pltpu.VMEM((16, S), F32), pltpu.VMEM((BLK, BLK), F32),
                           pltpu.SemaphoreType.DMA((11,)), pltpu.SemaphoreType.DMA((3,)), pltpu.SemaphoreType.DMA((3,))],
        name="back",
        cost_estimate=pl.CostEstimate(flops=int(3e10), bytes_accessed=30 << 20, transcendentals=nh * S * S // 2),
        compiler_params=pltpu.CompilerParams(collective_id=1, has_side_effects=True, vmem_limit_bytes=66900000),
    )(segr, lse, qkv, att, ysum, wt, wo, m_all)


def grads_kernel(dqkv_h, att_h, mid_h, ynear_h, yr_h, a_h, m_h, act_h, g_h, gu_h, gd_h, y_h, gq_o, go_o, gd_o, gu_o, dqkv, att, mid_ref, ynear, yr, y_o, av, mv, act, gv, guv, gdv, st, lsem, ssem):
    at = positions()
    early = pl.ds(0, EARLY * 256)
    late = (act.shape[1] // 256) - EARLY

    def loc(src, dst, i):
        c = pltpu.make_async_copy(src, dst, lsem.at[i])
        c.start()
        return c
    l_a = loc(a_h, av, 0)
    l_dqkv = loc(dqkv_h, dqkv, 11)
    l_m = [loc(m_h.at[block_at(r)], mv.at[block(at[r])], 1 + r) for r in range(4)]
    l_att = loc(att_h, att, 12)
    l_y = [loc(p, q, 13 + i) for i, (p, q) in enumerate(((mid_h, mid_ref), (ynear_h, ynear), (yr_h, yr)))]
    l_act = loc(act_h, act, 5)
    l_gv = loc(g_h, gv, 6)
    l_gu = loc(gu_h, guv, 7)
    l_gd = loc(gd_h.at[early], gdv, 8)

    def yout(q):
        v = ynear[q, :].astype(F32) + yr[q, :].astype(F32)
        y_o[q, :] = (mid_ref[q, :].astype(F32) + v.astype(BF).astype(F32)).astype(BF)
    l_a.wait()
    l_dqkv.wait()
    grad_blocks(dqkv, av, gq_o, st, ssem, False, 0, dqkv.shape[0] // 256)
    for c in l_m + l_y + [l_att, l_gu]:
        c.wait()
    tiles(256, 32, yout)
    s_y = loc(y_o, y_h, 16)
    s_gu = loc(guv, gu_o, 9)
    grad_blocks(att, mv, go_o, st, ssem, False, 0, att.shape[0] // 256)
    l_act.wait()
    l_gv.wait()
    l_gd.wait()
    s_gd = loc(gdv, gd_o.at[early], 10)
    grad_blocks(act, gv, gd_o, st, ssem, True, EARLY, EARLY + late, EARLY)
    for c in (s_y, s_gu, s_gd):
        c.wait()


def grads_call(dqkv, att, mid, ynear, yr, a_all, m_all, act, g_all, gu, gd):
    D = a_all.shape[1]
    H = pl.BlockSpec(memory_space=pl.ANY)
    sd = jax.ShapeDtypeStruct
    full = pltpu.VMEM(a_all.shape, BF)
    rows = dqkv.shape[0] + att.shape[0]
    return pl.pallas_call(
        grads_kernel,
        in_specs=[H] * 11,
        out_specs=[H] * 5,
        out_shape=[sd(mid.shape, BF), sd((dqkv.shape[0], D), BF), sd((att.shape[0], D), BF), sd(gd.shape, BF), sd(gu.shape, BF)],
        scratch_shapes=[pltpu.VMEM(v.shape, BF) for v in (dqkv, att, mid, mid, mid, mid)] + [full, full, pltpu.VMEM(act.shape, BF), full, pltpu.VMEM(gu.shape, BF), pltpu.VMEM((EARLY * 256, D), BF), pltpu.VMEM((2, 256, D), BF),
                        pltpu.SemaphoreType.DMA((17,)), pltpu.SemaphoreType.DMA((2,))],
        name="grads",
        cost_estimate=pl.CostEstimate(flops=3 * rows * D * a_all.shape[0], bytes_accessed=60 << 20, transcendentals=0),
        compiler_params=pltpu.CompilerParams(vmem_limit_bytes=66900000),
    )(dqkv, att, mid, ynear, yr, a_all, m_all, act, g_all, gu, gd)


def tail_kernel(x_ref, g_ref, hn, hr, m_ref, dg2_ref, dx_o, dg_o):
    da = (hn[...].astype(F32) + hr[...].astype(F32)).astype(BF).astype(F32)
    h, rstd = norm_stats(x_ref[...].astype(F32))
    v = da * row_of(g_ref)
    dx = rstd * (v - jnp.mean(v, **ROWS) - h * jnp.mean(v * h, **ROWS))
    dx_o[...] = (m_ref[...].astype(F32) + dx).astype(BF)
    s = jnp.sum(da * h, **COLS)
    i = pl.program_id(0)

    @pl.when(i == 0)
    def _():
        dg_o[...] = jnp.concatenate([s, dg2_ref[...]], 0)

    @pl.when(i > 0)
    def _():
        dg_o[0:1, :] += s


def tail_call(x, g1, hn, hr, m_all, dg2):
    n, D = x.shape
    blk = pl.BlockSpec((128, D), lambda i: (i, 0))
    whole = lambda r: pl.BlockSpec((r, D), lambda i: (0, 0))
    sd = jax.ShapeDtypeStruct
    return pl.pallas_call(
        tail_kernel, grid=(n // 128,),
        in_specs=[blk, pl.BlockSpec((D,), lambda i: (0,))] + [blk] * 3 + [whole(1)],
        out_specs=[blk, whole(2)],
        out_shape=[sd((n, D), BF), sd((2, D), F32)],
        name="tail",
        cost_estimate=pl.CostEstimate(flops=20 * n * D, bytes_accessed=14 * n * D, transcendentals=n),
    )(x, g1, hn, hr, m_all, dg2)


def swap(v, k):
    return lax.ppermute(v, 'model', [(i, i ^ k) for i in range(4)])


def local_layer(hidden_in, seg_ids, gain_attn, w_qkv, w_out, gain_mlp, w_up, w_down, grad_out):
    hidden, nh, _, dh = w_qkv.shape
    wt = w_qkv.transpose(1, 2, 3, 0).reshape(nh * 3 * dh, hidden)
    wo = w_out.reshape(nh * dh, hidden)
    x = hidden_in[0]
    d_g2, lse, mid, qkv, att, ysum, ynear, a_all, g_all, act, m_all, gw_up, gw_down = front_call(x, gain_attn, gain_mlp, seg_ids, wt, wo, w_up, w_down, grad_out[0], nh)
    yr, hx, hn, dqkv = back_call(seg_ids, qkv, att, lse, ysum, wt, wo, m_all)
    hr = swap(hx, 2)
    y, gq, go, gw_down, gw_up = grads_call(dqkv, att, mid, ynear, yr, a_all, m_all, act, g_all, gw_up, gw_down)
    hr, y, gq, go, gw_down, gw_up = lax.optimization_barrier((hr, y, gq, go, gw_down, gw_up))
    dx, dg = tail_call(x, gain_attn, hn, hr, m_all, d_g2)
    others = [swap(dg, k) for k in (2, 3, 1)]
    dg = ((dg + others[2]) + (others[0] + others[1])).astype(BF)
    gq = gq.reshape(nh, 3, dh, hidden).transpose(3, 0, 1, 2)
    return y[None], dx[None], gq, go.reshape(nh, dh, hidden), gw_up, gw_down, dg[0], dg[1]


def solution(mesh):
    act_spec = P('data', 'model', None)
    in_specs = (act_spec, P('data', None), P(), P(None, 'model', None, None), P('model', None, None), P(), P(None, 'model'), P('model', None), act_spec)
    out_specs = (act_spec, act_spec, P('data', 'model', None, None), P(('data', 'model'), None, None), P('data', 'model'), P(('data', 'model'), None), P('data'), P('data'))
    return jax.shard_map(local_layer, mesh=mesh, in_specs=in_specs, out_specs=out_specs, check_vma=False)
```
